256 devices in a mesh: row: 8 (over x, core), col: 32 (over y, z).
Axes of the slice: x: 4, y: 4, z: 8, core: 2. Of those that a mesh axis runs over, the one named last changes fastest.
Arguments:
- basis_raw: float32 [37, 384, 4096], P(None, 'row', 'col'), may hold values from -4 to 4
- krylov_raw: float32 [4, 37, 34], replicated, may hold values from -6 to 6
- stiffness: float32 [384, 4096], P('row', 'col'), may hold values from -0.4 to 0.4
- rotation: float32 [384, 4096], P('row', 'col'), may hold values from -0.2 to 0.2
Outputs:
- new_columns: float32 [3, 384, 4096], P(None, 'row', 'col')
- coefficients: float32 [4, 40, 37], replicated
- hessenberg: float32 [3, 37], replicated
- gram: float32 [5, 40, 5, 40], replicated
- new_images: float32 [3, 384, 4096], P(None, 'row', 'col')
The draws below stay inside these ranges and needn't reach their ends.
All inputs are finite; a program needn't handle non-finite values.
Results may differ from the reference program's by a relative error of at most 0.001.
Values sent between devices are 32-bit elements; how exact they have to be, the bound alone decides.
A program may use at most 64 MiB of HBM per device.

```python
import math
import jax
import jax.numpy as jnp
from jax import lax

K = 40
STEPS = 3
R = 37
KRYLOV = 34
NX = 384
NY = 4096


def draw_basis_raw(key, part):
    subkeys = jax.random.split(jax.random.fold_in(key, 17), 7)
    mode_count = R
    row_rate = jax.random.uniform(subkeys[0], (mode_count,), jnp.float32, 0.05, 3.0)
    col_rate = jax.random.uniform(subkeys[1], (mode_count,), jnp.float32, 0.05, 3.0)
    row_phase = jax.random.uniform(subkeys[2], (mode_count,), jnp.float32, 0.0, 2.0 * math.pi)
    col_phase = jax.random.uniform(subkeys[3], (mode_count,), jnp.float32, 0.0, 2.0 * math.pi)
    row_place = jnp.arange(NX, dtype=jnp.float32)
    col_place = jnp.arange(NY, dtype=jnp.float32)
    row_wave = jnp.cos(row_rate[:, None] * row_place[None, :] + row_phase[:, None])
    col_wave = jnp.cos(col_rate[:, None] * col_place[None, :] + col_phase[:, None])
    mixing = jax.random.uniform(subkeys[4], (R, mode_count), jnp.float32, -1.0, 1.0) * (2.0 / math.sqrt(mode_count))
    jitter = jax.random.uniform(subkeys[6], (R, NX, NY), jnp.float32, -0.3, 0.3)
    scaled_rows = mixing[:, :, None] * row_wave[None, :, :]
    smooth = jnp.einsum('rmx,my->rxy', scaled_rows, col_wave, precision=lax.Precision.HIGHEST)
    return jnp.clip(smooth + jitter, -4.0, 4.0)


def block_levels(rng, dims, cuts, smallest, high):
    factor_of, own = 1.0, jax.random.fold_in(rng, 6)
    for dim, shards_of in cuts:
        heights = jnp.exp(jax.random.uniform(jax.random.fold_in(own, dim), (shards_of,), jnp.float32, smallest / len(cuts), high / len(cuts)))
        factor_of = factor_of * jnp.repeat(heights, dims[dim] // shards_of).reshape([-1 if axis == dim else 1 for axis in range(len(dims))])
    return factor_of


def centred(own_key, extent, deviation, bound, held_as=jnp.bfloat16):
    array = jax.random.normal(own_key, extent, jnp.float32) * deviation
    return jnp.minimum(jnp.maximum(array, -bound), bound).astype(held_as)


def setup_inputs(seed: int = 0) -> dict:
    splits = jax.random.split(jax.random.key(seed), 5)
    basis_raw = draw_basis_raw(jax.random.fold_in(splits[4], 71), 0)
    krylov_raw = centred(splits[1], (4, R, KRYLOV), 1.0, 6.0, jnp.float32)
    stiffness = jnp.clip(jax.random.uniform(splits[2], (NX, NY), jnp.float32, -0.4, 0.4) * block_levels(splits[2], (NX, NY), ((0, 8), (1, 32)), -0.4, 0.0), -0.4, 0.4)
    rotation = jnp.clip(jax.random.uniform(splits[3], (NX, NY), jnp.float32, -0.2, 0.2) * block_levels(splits[3], (NX, NY), ((0, 8), (1, 32)), -0.4, 0.0), -0.2, 0.2)
    return {"basis_raw": basis_raw, "krylov_raw": krylov_raw, "stiffness": stiffness, "rotation": rotation}


COUPLING = 0.2
EPSILON = 1e-06
GRAM_SHIFT = 0.05
HIGHEST = lax.Precision.HIGHEST

def apply_core(border, diagonal, spin_field):
    middle = border[..., 1:-1, 1:-1]
    left_cells = border[..., 1:-1, :-2]
    right_cells = border[..., 1:-1, 2:]
    upper_cells = border[..., :-2, 1:-1]
    lower_cells = border[..., 2:, 1:-1]
    return diagonal * middle - COUPLING * (upper_cells + lower_cells + left_cells + right_cells) + spin_field * (right_cells - left_cells)

def lower_inverse(matrix):
    factor = jnp.linalg.cholesky(matrix)
    identity = jnp.eye(matrix.shape[0], dtype=matrix.dtype)
    return lax.linalg.triangular_solve(factor, identity, left_side=True, lower=True)

def reference(basis_raw, krylov_raw, stiffness, rotation):
    grid_total = NX * NY
    inverse_total = 1.0 / grid_total
    flat_raw = basis_raw.reshape(R, grid_total)
    raw_gram = jnp.dot(flat_raw, flat_raw.T, precision=HIGHEST) * inverse_total
    shifted = raw_gram + GRAM_SHIFT * jnp.eye(R, dtype=raw_gram.dtype)
    prepared = jnp.dot(lower_inverse(shifted), flat_raw, precision=HIGHEST)
    basis_rows = jnp.concatenate([prepared, jnp.zeros((STEPS, grid_total), prepared.dtype)], 0)
    krylov_flat = krylov_raw.reshape(4 * R, KRYLOV)
    krylov_ortho = jnp.dot(krylov_flat, lower_inverse(jnp.dot(krylov_flat.T, krylov_flat, precision=HIGHEST)).T, precision=HIGHEST)
    krylov_width = KRYLOV + STEPS
    krylov_rows = jnp.pad(krylov_ortho.reshape(4, R, KRYLOV), ((0, 0), (0, STEPS), (0, STEPS)))

    def operate(source):
        padding = [(0, 0)] * (source.ndim - 2) + [(1, 1), (1, 1)]
        return apply_core(jnp.pad(source, padding), stiffness, rotation)
    hessen_rows = []
    for turn_index in range(STEPS):
        column = KRYLOV + turn_index
        new_row = R + turn_index
        latest = krylov_rows[:, :, column - 1]
        components = jnp.dot(latest, basis_rows, precision=HIGHEST).reshape(4, NX, NY)
        section_four = components[3]
        section_three = components[2] + 2.0 * operate(section_four)
        section_two = components[1] + 2.0 * operate(section_three) - section_four
        section_one = components[0] + 2.0 * operate(section_two) - section_three
        summed = operate(section_one) - section_two
        target = (0.5 * components[2] - 0.5 * summed).reshape(grid_total)
        first_coef = jnp.dot(basis_rows, target, precision=HIGHEST) * inverse_total
        residual_one = target - jnp.dot(first_coef, basis_rows, precision=HIGHEST)
        second_coef = jnp.dot(basis_rows, residual_one, precision=HIGHEST) * inverse_total
        residual_two = residual_one - jnp.dot(second_coef, basis_rows, precision=HIGHEST)
        new_norm = jnp.sqrt(jnp.sum(residual_two * residual_two) * inverse_total + EPSILON)
        basis_rows = basis_rows.at[new_row].set(residual_two / new_norm)
        unit_row = (jnp.arange(K) == new_row).astype(basis_rows.dtype)
        expanded = jnp.stack([latest[1], 0.5 * (latest[0] + latest[2]), 0.5 * (latest[1] + latest[3]), first_coef + second_coef + new_norm * unit_row]).reshape(4 * K)
        matrix_view = krylov_rows.reshape(4 * K, krylov_width)
        first_proj = jnp.dot(expanded, matrix_view, precision=HIGHEST)
        ortho_one = expanded - jnp.dot(matrix_view, first_proj, precision=HIGHEST)
        second_proj = jnp.dot(ortho_one, matrix_view, precision=HIGHEST)
        ortho_two = ortho_one - jnp.dot(matrix_view, second_proj, precision=HIGHEST)
        krylov_norm = jnp.sqrt(jnp.sum(ortho_two * ortho_two) + EPSILON)
        krylov_rows = krylov_rows.at[:, :, column].set((ortho_two / krylov_norm).reshape(4, K))
        unit_column = (jnp.arange(krylov_width) == column).astype(krylov_rows.dtype)
        hessen_rows.append(first_proj + second_proj + krylov_norm * unit_column)
    new_columns = basis_rows[R:].reshape(STEPS, NX, NY)
    image_one = operate(new_columns)
    image_two = 2.0 * operate(image_one) - new_columns
    image_three = 2.0 * operate(image_two) - image_one
    new_images = 2.0 * operate(image_three) - image_two
    padded_basis = jnp.pad(basis_rows.reshape(K, NX, NY), ((0, 0), (4, 4), (0, 0)))
    diag_padded = jnp.pad(stiffness, ((4, 4), (0, 0)))
    spin_padded = jnp.pad(rotation, ((4, 4), (0, 0)))
    band_height = 32

    def row_apply(source, band_start, margin):
        out_rows = band_height + 2 * (margin - 1)
        diagonal = lax.dynamic_slice_in_dim(diag_padded, band_start + 5 - margin, out_rows, 0)
        spin_field = lax.dynamic_slice_in_dim(spin_padded, band_start + 5 - margin, out_rows, 0)
        result = apply_core(jnp.pad(source, ((0, 0), (0, 0), (1, 1))), diagonal, spin_field)
        row_global = band_start - (margin - 1) + jnp.arange(out_rows, dtype=jnp.int32)
        valid_rows = ((row_global >= 0) & (row_global < NX)).astype(result.dtype)
        return result * valid_rows[:, None]

    def crop_rows(source, margin):
        return source[:, margin:source.shape[1] - margin]

    def band_gram(gram_sum, band_start):
        order_zero = lax.dynamic_slice_in_dim(padded_basis, band_start, band_height + 8, 1)
        order_one = row_apply(order_zero, band_start, 4)
        order_two = 2.0 * row_apply(order_one, band_start, 3) - crop_rows(order_zero, 2)
        order_three = 2.0 * row_apply(order_two, band_start, 2) - crop_rows(order_one, 2)
        order_four = 2.0 * row_apply(order_three, band_start, 1) - crop_rows(order_two, 2)
        band_tile = jnp.concatenate([crop_rows(order_zero, 4), crop_rows(order_one, 3), crop_rows(order_two, 2), crop_rows(order_three, 1), order_four], 0).reshape(5 * K, band_height * NY)
        return (gram_sum + jnp.dot(band_tile, band_tile.T, precision=HIGHEST), None)
    band_starts = jnp.arange(NX // band_height, dtype=jnp.int32) * band_height
    gram_sum, _ = lax.scan(band_gram, jnp.zeros((5 * K, 5 * K), padded_basis.dtype), band_starts)
    gram = (gram_sum * inverse_total).reshape(5, K, 5, K)
    return (new_columns, krylov_rows, jnp.stack(hessen_rows), gram, new_images)
```

```python
import functools
import itertools

import jax
import jax.numpy as jnp
from jax import lax
from jax.experimental import pallas as pl
from jax.experimental.pallas import tpu as pltpu
from jax.sharding import Mesh
from jax.sharding import PartitionSpec as P

K = 40
STEPS = 3
R = 37
KRYLOV = 34
ORDERS = 5
FIELDS = ORDERS * K
COUPLING = 0.2
EPSILON = 1e-06
GRAM_SHIFT = 0.05
HIGHEST = lax.Precision.HIGHEST
AXES = ("x", "core", "y", "z")
ROW = ("x", "core")
COL = ("y", "z")
STAGES = (("x", "core"), ("y",), ("z",))
ROWS = 48
LANES = 128
GHOST = 4
F32 = jnp.float32


def dot(a, b, ca, cb):
    return lax.dot_general(
        a, b, (((ca,), (cb,)), ((), ())), precision=HIGHEST, preferred_element_type=F32
    )


def iota(shape, dim):
    return lax.broadcasted_iota(jnp.int32, shape, dim)


def offsets(sizes, axes):
    ranges = [range(sizes[a]) for a in axes]
    return [o for o in itertools.product(*ranges) if any(o)]


def place(sizes, axes):
    index = 0
    for a in axes:
        index = index * sizes[a] + lax.axis_index(a)
    return index


def peer_of(sizes, axes, off):
    return {a: lax.rem(lax.axis_index(a) + o, sizes[a]) for a, o in zip(axes, off)}


def linear(sizes, axes, coords):
    index = 0
    for a in axes:
        index = index * sizes[a] + coords[a]
    return index


def near(sizes, drow, dcol):
    rows = sizes["x"] * sizes["core"]
    cols = sizes["y"] * sizes["z"]
    r = lax.rem(place(sizes, ROW) + drow + rows, rows)
    c = lax.rem(place(sizes, COL) + dcol + cols, cols)
    return {
        "x": r // sizes["core"],
        "core": lax.rem(r, sizes["core"]),
        "y": c // sizes["z"],
        "z": lax.rem(c, sizes["z"]),
    }


def full(coords):
    return tuple(coords.get(a, lax.axis_index(a)) for a in AXES)


SIDES = [(-1, 0), (1, 0), (0, -1), (0, 1), (-1, -1), (-1, 1), (1, -1), (1, 1)]


def forward_inverse(aug, count):
    sub = iota((K, LANES), 0)
    lane = iota((K, LANES), 1)

    def step(j, a):
        col = jnp.sum(jnp.where(lane == j, a, 0.0), axis=1, keepdims=True)
        row = jnp.sum(jnp.where(sub == j, a, 0.0), axis=0, keepdims=True)
        pivot = jnp.sum(jnp.where(iota((1, LANES), 1) == j, row, 0.0), axis=1, keepdims=True)
        factor = jnp.where(iota((K, 1), 0) > j, col / pivot, 0.0)
        return a - factor * row

    aug = lax.fori_loop(0, count, step, aug)
    diag = jnp.sum(jnp.where(lane == sub, aug, 0.0), axis=1, keepdims=True)
    scaled = aug * (1.0 / jnp.sqrt(diag))
    return jnp.where(lane < K, pltpu.roll(scaled, 64, 1), 0.0)


def augmented(a, shift, count):
    sub = iota((K, LANES), 0)
    lane = iota((K, LANES), 1)
    a = jnp.where((lane < count) & (sub < count), a, 0.0)
    a = a + jnp.where((lane == sub) & (sub < count), shift, 0.0)
    return a + jnp.where(((lane == sub) & (sub >= count)) | (lane == sub + 64), 1.0, 0.0)


def kernel(
    sizes, x_ref, kr_ref, st_ref, ro_ref,
    newc_ref, coef_ref, hess_ref, gram_ref, newi_ref,
    X, SD, T, CF, PL, PR, RRB, RLB, ACC, BIG, FULL, GS, LB, GB0, CB, MT, HS, KS,
    U0, PK, HT, HB, KRB, KLB, VB, DACC,
    slots_big, slots_small,
    hsend, hrecv, bsend, brecv, usend, urecv, ssend, srecv,
):
    nrow = sizes["x"] * sizes["core"]
    ncol = sizes["y"] * sizes["z"]
    my_row = place(sizes, ROW)
    my_col = place(sizes, COL)
    grid_rows = nrow * ROWS
    inverse_total = 1.0 / (grid_rows * ncol * LANES)
    stage_offsets = [offsets(sizes, axes) for axes in STAGES]
    pending = []

    barrier = pltpu.get_barrier_semaphore()
    count = 0
    for axes, offs in zip(STAGES, stage_offsets):
        for off in offs:
            pl.semaphore_signal(
                barrier, inc=1, device_id=full(peer_of(sizes, axes, off)),
                device_id_type=pl.DeviceIdType.MESH,
            )
            count += 1
    for side in SIDES:
        pl.semaphore_signal(
            barrier, inc=1, device_id=full(near(sizes, *side)),
            device_id_type=pl.DeviceIdType.MESH,
        )
        count += 1

    def send(src, dst, ssem, rsem, coords):
        copy = pltpu.make_async_remote_copy(
            src_ref=src, dst_ref=dst, send_sem=ssem, recv_sem=rsem,
            device_id=full(coords), device_id_type=pl.DeviceIdType.MESH,
        )
        copy.start()
        pending.append(copy)
        return copy

    def load_row(r, carry):
        X[0, r + GHOST, pl.ds(0, R), :] = x_ref[pl.ds(r, R, stride=ROWS), :]
        X[0, r + GHOST, pl.ds(R, 1), :] = st_ref[pl.ds(r, 1), :]
        X[0, r + GHOST, pl.ds(R + 1, 1), :] = ro_ref[pl.ds(r, 1), :]
        X[0, r + GHOST, pl.ds(R + 2, 1), :] = jnp.zeros((1, LANES), F32)
        return carry

    lax.fori_loop(0, ROWS, load_row, 0)
    lane_k = iota((K, LANES), 1)

    def pack(base, n, q):
        def body(i, carry):
            left, right = carry
            row = X[0, base + i, :, :]
            here = (lane_k >= 4 * i) & (lane_k < 4 * i + 4)
            left = jnp.where(here, pltpu.roll(row, 4 * i, 1), left)
            right = jnp.where(here, pltpu.roll(row, lax.rem(4 * i + 4, LANES), 1), right)
            return left, right

        zero = jnp.zeros((K, LANES), F32)
        left, right = lax.fori_loop(0, n, body, (zero, zero))
        PL[q, :, :] = left
        PR[q, :, :] = right

    pack(GHOST, 32, 0)
    pack(GHOST + 32, 16, 1)
    pl.semaphore_wait(barrier, count)

    halo = [
        send(X.at[0, pl.ds(GHOST, GHOST)], X.at[0, pl.ds(GHOST + ROWS, GHOST)], hsend.at[0], hrecv.at[0], near(sizes, -1, 0)),
        send(X.at[0, pl.ds(ROWS, GHOST)], X.at[0, pl.ds(0, GHOST)], hsend.at[1], hrecv.at[1], near(sizes, 1, 0)),
        send(PL, RRB.at[pl.ds(1, 2)], hsend.at[2], hrecv.at[2], near(sizes, 0, -1)),
        send(PR, RLB.at[pl.ds(1, 2)], hsend.at[3], hrecv.at[3], near(sizes, 0, 1)),
        send(PL.at[0], RRB.at[3], hsend.at[4], hrecv.at[4], near(sizes, -1, -1)),
        send(PR.at[0], RLB.at[3], hsend.at[5], hrecv.at[5], near(sizes, -1, 1)),
        send(PL.at[1], RRB.at[0], hsend.at[6], hrecv.at[6], near(sizes, 1, -1)),
        send(PR.at[1], RLB.at[0], hsend.at[7], hrecv.at[7], near(sizes, 1, 1)),
    ]

    KS[...] = jnp.zeros((256, LANES), F32)
    for j in range(4):
        KS[pl.ds(j * K, R), pl.ds(0, KRYLOV)] = kr_ref[j]
    pt = jnp.transpose(KS[...])[0:K, :]
    kgram = dot(pt, KS[...], 1, 0)
    kinv = forward_inverse(augmented(kgram, 0.0, KRYLOV), KRYLOV)
    MT[...] = jnp.zeros((LANES, 256), F32)
    MT[pl.ds(0, K), :] = dot(kinv[:, 0:K], pt, 1, 0)
    HS[...] = jnp.zeros((LANES, LANES), F32)
    LB[...] = jnp.zeros((256, 256), F32)
    GS[...] = jnp.zeros((256, 256), F32)
    BIG[...] = jnp.zeros((256, LANES), F32)
    CF[...] = jnp.zeros((10, 64, LANES), F32)
    for m in range(ORDERS):
        DACC[m, pl.ds(FIELDS, 56), :] = jnp.zeros((56, LANES), F32)

    for copy in halo:
        copy.wait_recv()
    for copy in halo[:2]:
        copy.wait_send()
        pending.remove(copy)

    lane1 = iota((1, LANES), 1)
    has_right = (my_col < ncol - 1).astype(F32)
    has_left = (my_col > 0).astype(F32)
    side_mask = jnp.where(lane1 < 4, has_right, jnp.where(lane1 >= 124, has_left, 0.0))
    sub_k = iota((K, LANES), 0)

    def order_zero(base, n, part, first):
        def body(i, carry):
            rho = base + i
            g = my_row * ROWS + rho - GHOST
            row_mask = ((g >= 0) & (g < grid_rows)).astype(F32)
            at = 4 * (first + i)
            right = pltpu.roll(RRB[part, :, :], lax.rem(LANES - at, LANES), 1)
            left = pltpu.roll(RLB[part, :, :], lax.rem(2 * LANES - 4 - at, LANES), 1)
            ms = side_mask * row_mask
            side = jnp.where(lane_k < 4, right, left) * ms
            mid = X[0, rho, :, :] * row_mask
            mc = jnp.ones((1, LANES), F32) * row_mask
            for half, (v, m) in enumerate(((mid, mc), (side, ms))):
                d = v[R : R + 1, :]
                s = v[R + 1 : R + 2, :]
                CF[5 * half, pl.ds(rho + 4, 1), :] = 2.0 * d * m
                CF[5 * half + 1, pl.ds(rho + 4, 1), :] = (2.0 * COUPLING) * m
                CF[5 * half + 2, pl.ds(rho + 4, 1), :] = 2.0 * (s - COUPLING) * m
                CF[5 * half + 3, pl.ds(rho + 4, 1), :] = 2.0 * (s + COUPLING) * m
                CF[5 * half + 4, pl.ds(rho + 4, 1), :] = m
            X[0, rho, :, :] = jnp.where(sub_k < R, mid, 0.0)
            SD[0, rho, :, :] = jnp.where(sub_k < R, side, 0.0)
            return carry

        lax.fori_loop(0, n, body, 0)

    order_zero(0, 4, 0, 12)
    order_zero(4, 32, 1, 0)
    order_zero(36, 16, 2, 0)
    order_zero(52, 4, 3, 0)

    def copy_zero(r, carry):
        T[pl.ds(pl.multiple_of(r * FIELDS, 8), K), :] = X[0, r + GHOST, :, :]
        return carry

    lax.fori_loop(0, ROWS, copy_zero, 0)

    def images(m):
        def body(i, carry):
            rho = m + i
            c = X[m - 1, rho, :, :]
            s = SD[m - 1, rho, :, :]
            cu = X[m - 1, rho - 1, :, :] + X[m - 1, rho + 1, :, :]
            cl, sl = pltpu.roll(c, 1, 1), pltpu.roll(s, 1, 1)
            cr, sr = pltpu.roll(c, 127, 1), pltpu.roll(s, 127, 1)

            def row(kind):
                return CF[kind, pl.ds(rho + 4, 1), :]

            left = jnp.where(lane_k == 0, sl, cl)
            right = jnp.where(lane_k == 127, sr, cr)
            new = row(0) * c - row(1) * cu + row(2) * right - row(3) * left
            new = 0.5 * new if m == 1 else new - X[m - 2, rho, :, :]
            if m < 4:
                X[m, rho, :, :] = new
                su = SD[m - 1, rho - 1, :, :] + SD[m - 1, rho + 1, :, :]
                left = jnp.where(lane_k == 0, cl, sl)
                right = jnp.where(lane_k == 127, cr, sr)
                side = row(5) * s - row(6) * su + row(7) * right - row(8) * left
                SD[m, rho, :, :] = 0.5 * side if m == 1 else side - SD[m - 2, rho, :, :]

                @pl.when((rho >= GHOST) & (rho < GHOST + ROWS))
                def _():
                    at = pl.multiple_of((rho - GHOST) * FIELDS + m * K, 8)
                    T[pl.ds(at, K), :] = new
            else:
                at = pl.multiple_of((rho - GHOST) * FIELDS + m * K, 8)
                T[pl.ds(at, K), :] = new
            return carry

        lax.fori_loop(0, ROWS + 8 - 2 * m, body, 0)

    for m in range(1, ORDERS):
        images(m)

    ACC[...] = jnp.zeros((FIELDS, 256), F32)

    def gram_rows(g, carry):
        a = jnp.concatenate(
            [T[pl.ds(pl.multiple_of((4 * g + k) * FIELDS, 8), FIELDS), :] for k in range(4)], axis=1
        )
        ACC[:, pl.ds(0, FIELDS)] += dot(a, a, 1, 1)
        return carry

    lax.fori_loop(0, ROWS // 4, gram_rows, 0)

    def strip(ref, a, shift):
        v = ref[pl.ds(a * K, K), :]
        return pltpu.roll(v, shift % 256, 1) if shift % 256 else v

    lane_n = iota((K, LANES), 1)
    last = lane_n >= 80
    BIG[pl.ds(0, K), :] = strip(ACC, 0, 0)[:, 0:LANES]
    BIG[pl.ds(K, K), :] = strip(ACC, 1, -40)[:, 0:LANES]
    BIG[pl.ds(2 * K, K), :] = strip(ACC, 2, -80)[:, 0:LANES]
    BIG[pl.ds(3 * K, K), :] = jnp.where(last, strip(ACC, 4, -80)[:, 0:LANES], strip(ACC, 0, -120)[:, 0:LANES])
    BIG[pl.ds(4 * K, K), :] = jnp.where(last, strip(ACC, 1, -80)[:, 0:LANES], strip(ACC, 3, -120)[:, 0:LANES])

    chunk = 256 // nrow
    own = pl.ds(pl.multiple_of(my_row * chunk, 8), chunk)

    def chunk_of(coords):
        return pl.ds(pl.multiple_of(linear(sizes, ROW, coords) * chunk, 8), chunk)

    sem = 0
    for stage, (axes, offs) in enumerate(zip(STAGES, stage_offsets)):
        me = place(sizes, axes)
        box = slots_big[stage]
        if stage == 0:
            box[me] = BIG[own, :]
        copies = []
        for off in offs:
            to = peer_of(sizes, axes, off)
            src = BIG.at[chunk_of(to)] if stage == 0 else box.at[me]
            copies.append(send(src, box.at[me], bsend.at[sem], brecv.at[sem], to))
            sem += 1
        for copy in copies:
            copy.wait_recv()
        total = box[0]
        for i in range(1, len(offs) + 1):
            total = total + box[i]
        if stage + 1 < len(STAGES):
            slots_big[stage + 1][place(sizes, STAGES[stage + 1])] = total
        else:
            FULL[own, :] = total * inverse_total
    copies = []
    for off in stage_offsets[0]:
        to = peer_of(sizes, ROW, off)
        copies.append(send(FULL.at[own], FULL.at[own], bsend.at[sem], brecv.at[sem], to))
        sem += 1
    for copy in copies:
        copy.wait_recv()

    lane_w = iota((K, 256), 1)

    def wide(a):
        v = FULL[pl.ds(a * K, K), :]
        return jnp.concatenate([jnp.where(lane_n < 120, v, 0.0), jnp.zeros((K, LANES), F32)], axis=1)

    g3, g4 = wide(3), wide(4)

    def between(v, lo, hi):
        return jnp.where((lane_w >= lo) & (lane_w < hi), v, 0.0)

    GS[pl.ds(0, K), :] = wide(0) + between(pltpu.roll(g3, 120, 1), 120, 200)
    GS[pl.ds(K, K), :] = pltpu.roll(wide(1), 40, 1) + between(pltpu.roll(g4, 80, 1), 160, 200)
    GS[pl.ds(2 * K, K), :] = pltpu.roll(wide(2), 80, 1)
    GS[pl.ds(3 * K, K), :] = between(pltpu.roll(g4, 120, 1), 120, 200)
    GS[pl.ds(4 * K, K), :] = between(pltpu.roll(g3, 80, 1), 160, 200)
    mirrored = jnp.transpose(GS[...])
    for a in range(1, ORDERS):
        GS[pl.ds(a * K, K), :] = jnp.where(
            lane_w >= a * K, GS[pl.ds(a * K, K), :], mirrored[a * K : (a + 1) * K, :]
        )

    finv = forward_inverse(augmented(GS[pl.ds(0, K), pl.ds(0, LANES)], GRAM_SHIFT, R), R)
    finv = jnp.where(sub_k < R, finv, 0.0)
    finv_wide = jnp.concatenate([finv, jnp.zeros((K, LANES), F32)], axis=1)
    for a in range(ORDERS):
        LB[pl.ds(a * K, K), :] = pltpu.roll(finv_wide, a * K, 1) if a else finv_wide
    square = (iota((LANES, LANES), 0) < K) & (iota((LANES, LANES), 1) < K)
    small = jnp.where(square, LB[pl.ds(0, LANES), pl.ds(0, LANES)], 0.0)
    GB0[...] = dot(dot(LB[...], GS[:, pl.ds(0, LANES)], 1, 0), small, 1, 1)

    lane_r = iota((1, 256), 1)
    lane8 = iota((8, 256), 1)
    sub8 = iota((8, 256), 0)
    tile_mask = iota((64, LANES), 1)

    for s in range(STEPS):
        column = KRYLOV + s
        r = R + s
        latest = MT[pl.ds(column - 1, 1), :]

        def moved(shift):
            return pltpu.roll(latest, shift % 256, 1)

        cw = jnp.where(lane_r < K, 0.5 * moved(-80), -0.5 * moved(40))
        cw = jnp.where(lane_r < FIELDS, cw, 0.0)
        cw = jnp.broadcast_to(cw, (8, 256))
        h1 = dot(cw, GB0[...], 1, 0)
        h = 2.0 * h1 - dot(h1, GB0[pl.ds(0, LANES), :], 1, 0)
        h_wide = jnp.concatenate([h, jnp.zeros((8, LANES), F32)], axis=1)
        raw = dot(cw - h_wide, LB[...], 1, 0)
        raw_col = jnp.transpose(raw)[0:FIELDS, 0:1]
        CB[...] = jnp.broadcast_to(raw_col, (FIELDS, LANES))

        def combine(i, carry):
            for k in range(8):
                at = pl.multiple_of((8 * i + k) * FIELDS, 8)
                value = jnp.sum(CB[...] * T[pl.ds(at, FIELDS), :], axis=0, keepdims=True)
                U0[s, pl.ds(8 * i + k, 1), :] = value
            return carry

        lax.fori_loop(0, ROWS // 8, combine, 0)

        lane_t = iota((8, LANES), 1)
        packed = jnp.zeros((8, LANES), F32)
        for q in range(6):
            tile = U0[s, pl.ds(8 * q, 8), :]
            packed = jnp.where(
                (lane_t >= 4 * q) & (lane_t < 4 * q + 4), pltpu.roll(tile, 4 * q, 1) if q else tile, packed
            )
            packed = jnp.where(
                (lane_t >= 64 + 4 * q) & (lane_t < 68 + 4 * q), pltpu.roll(tile, 68 + 4 * q, 1), packed
            )
        PK[s, :, :] = packed
        edge = [
            send(U0.at[s, pl.ds(0, 8)], HB.at[s], usend.at[s, 0], urecv.at[s, 0], near(sizes, -1, 0)),
            send(U0.at[s, pl.ds(40, 8)], HT.at[s], usend.at[s, 1], urecv.at[s, 1], near(sizes, 1, 0)),
            send(PK.at[s], KRB.at[s, 1], usend.at[s, 2], urecv.at[s, 2], near(sizes, 0, -1)),
            send(PK.at[s], KLB.at[s, 1], usend.at[s, 3], urecv.at[s, 3], near(sizes, 0, 1)),
            send(PK.at[s], KRB.at[s, 2], usend.at[s, 4], urecv.at[s, 4], near(sizes, -1, -1)),
            send(PK.at[s], KLB.at[s, 2], usend.at[s, 5], urecv.at[s, 5], near(sizes, -1, 1)),
            send(PK.at[s], KRB.at[s, 0], usend.at[s, 6], urecv.at[s, 6], near(sizes, 1, -1)),
            send(PK.at[s], KLB.at[s, 0], usend.at[s, 7], urecv.at[s, 7], near(sizes, 1, 1)),
        ]

        h_row = h_wide[0:1, :]
        e = jnp.where(lane_r < K, moved(-40), 0.5 * (moved(40) + moved(-40)))
        e = jnp.where(lane_r < 3 * K, e, pltpu.roll(h_row, 3 * K, 1))
        e = jnp.where(lane_r < 4 * K, e, 0.0)
        mt = MT[pl.ds(0, K), :]
        g1 = jnp.sum(mt * e, axis=1, keepdims=True)
        e1 = e - jnp.sum(mt * g1, axis=0, keepdims=True)
        g2 = jnp.sum(mt * e1, axis=1, keepdims=True)
        e2 = e1 - jnp.sum(mt * g2, axis=0, keepdims=True)
        e2_square = jnp.sum(e2 * e2, axis=1, keepdims=True)

        for copy in edge:
            copy.wait_recv()

        mids = jnp.concatenate([HT[s], U0[s], HB[s]], axis=0) * CF[4]
        sides = []
        for j in range(8):
            part = 0 if j == 0 else (2 if j == 7 else 1)
            q = 5 if j == 0 else (0 if j == 7 else j - 1)
            rt = KRB[s, part]
            lf = pltpu.roll(KLB[s, part], 60 - 4 * q, 1)
            rt = pltpu.roll(rt, LANES - 4 * q, 1) if q else rt
            sides.append(jnp.where(lane_t < 4, rt, lf))
        sds = jnp.concatenate(sides, axis=0) * CF[9]

        def twice_s(c, v):
            cl, sl = pltpu.roll(c, 1, 1), pltpu.roll(v, 1, 1)
            cr, sr = pltpu.roll(c, 127, 1), pltpu.roll(v, 127, 1)
            cu = pltpu.roll(c, 1, 0) + pltpu.roll(c, 63, 0)
            su = pltpu.roll(v, 1, 0) + pltpu.roll(v, 63, 0)
            lo, hi = tile_mask == 0, tile_mask == 127
            mid = CF[0] * c - CF[1] * cu + CF[2] * jnp.where(hi, sr, cr) - CF[3] * jnp.where(lo, sl, cl)
            side = CF[5] * v - CF[6] * su + CF[7] * jnp.where(hi, cr, sr) - CF[8] * jnp.where(lo, cl, sl)
            return mid, side

        before = (mids, sds)
        now = twice_s(*before)
        now = (0.5 * now[0], 0.5 * now[1])
        orders = [before[0], now[0]]
        for m in range(2, ORDERS):
            nxt = twice_s(*now)
            before, now = now, (nxt[0] - before[0], nxt[1] - before[1])
            orders.append(now[0])
        for m in range(ORDERS):
            VB[m, :, :] = orders[m][8:56, :]
            T[pl.ds(m * K + r, ROWS, stride=FIELDS), :] = orders[m][8:56, :]

        for a in range(ORDERS):
            def products(i, accs):
                at = pl.multiple_of(i * FIELDS + a * K, 8)
                t = T[pl.ds(at, K), :]
                return tuple(acc + t * VB[m, pl.ds(i, 1), :] for m, acc in enumerate(accs))

            accs = lax.fori_loop(
                0, ROWS, products, tuple(jnp.zeros((K, LANES), F32) for _ in range(ORDERS))
            )
            for m in range(ORDERS):
                DACC[m, pl.ds(a * K, K), :] = accs[m]
        d = jnp.zeros((8, 256), F32)
        for m in range(ORDERS):
            pick = (iota((8, LANES), 0) == m).astype(F32)
            d = d + dot(pick, DACC[m], 1, 1)

        total = d
        sem = 0
        for stage, (axes, offs) in enumerate(zip(STAGES, stage_offsets)):
            me = place(sizes, axes)
            box = slots_small[stage].at[s]
            box[me] = total
            copies = []
            for off in offs:
                copies.append(
                    send(box.at[me], box.at[me], ssend.at[s, sem], srecv.at[s, sem], peer_of(sizes, axes, off))
                )
                sem += 1
            for copy in copies:
                copy.wait_recv()
            total = box[0]
            for i in range(1, len(offs) + 1):
                total = total + box[i]
        d = total * inverse_total

        nn = jnp.sum(jnp.where(lane_r == r, d[0:1, :], 0.0), axis=1, keepdims=True)
        beta = jnp.sqrt(nn + EPSILON)
        ib = 1.0 / beta
        eta = jnp.sqrt(e2_square + beta * beta + EPSILON)
        MT[pl.ds(column, 1), :] = (e2 + jnp.where(lane_r == 3 * K + r, beta, 0.0)) / eta
        sub_col = iota((K, 1), 0)
        g = g1 + g2 + jnp.where(sub_col == column, eta, 0.0)
        lane_h = iota((K, LANES), 1)
        HS[pl.ds(0, K), :] = jnp.where(lane_h == s, g, HS[pl.ds(0, K), :])
        newc_ref[s, :, :] = VB[0] * ib
        newi_ref[s, :, :] = VB[4] * ib
        for m in range(ORDERS):
            at = m * K + r
            LB[pl.ds(at, 1), :] = jnp.where(lane_r == at, ib, 0.0)
            GS[pl.ds(at, 1), :] = d[m : m + 1, :]
        if s + 1 < STEPS:
            db = dot(d, LB[...], 1, 1) * ib
            dcol = jnp.transpose(db)[:, 0:1]
            lane_g = iota((256, LANES), 1)
            GB0[...] = jnp.where(lane_g == r, dcol, GB0[...])
            for m in range(ORDERS):
                GB0[pl.ds(m * K + r, 1), :] = jnp.where(lane1 < K, db[m : m + 1, 0:LANES], 0.0)

    mirrored = jnp.transpose(GS[...])
    field = lane_w
    for a in range(1, ORDERS):
        field = field - jnp.where(lane_w >= a * K, K, 0)
    age_col = jnp.maximum(field - (R - 1), 0)
    age_row = jnp.maximum(iota((K, 256), 0) - (R - 1), 0)
    for a in range(ORDERS):
        GS[pl.ds(a * K, K), :] = jnp.where(
            age_row >= age_col, GS[pl.ds(a * K, K), :], mirrored[a * K : (a + 1) * K, :]
        )
    gram = dot(dot(LB[...], GS[...], 1, 0), LB[...], 1, 1)
    gram_ref[...] = gram[0:FIELDS, 0:FIELDS]
    mcol = jnp.transpose(MT[...])
    for j in range(4):
        coef_ref[j, :, :] = mcol[j * K : (j + 1) * K, 0 : KRYLOV + STEPS]
    hess_ref[...] = jnp.transpose(HS[...])[0:STEPS, 0 : KRYLOV + STEPS]

    for copy in pending:
        copy.wait_send()


def local(sizes, basis_raw, krylov_raw, stiffness, rotation):
    width = KRYLOV + STEPS
    nrow = sizes["x"] * sizes["core"]
    counts = []
    for axes in STAGES:
        n = 1
        for a in axes:
            n *= sizes[a]
        counts.append(n)
    chunk = 256 // nrow
    big_copies = sum(n - 1 for n in counts) + counts[0] - 1
    small_copies = sum(n - 1 for n in counts)
    vmem = lambda *shape: pltpu.VMEM(shape, F32)
    dma = lambda *shape: pltpu.SemaphoreType.DMA(shape)
    scratch = [
        vmem(4, ROWS + 8, K, LANES), vmem(4, ROWS + 8, K, LANES), vmem(ROWS * FIELDS, LANES),
        vmem(10, 64, LANES), vmem(2, K, LANES), vmem(2, K, LANES), vmem(4, K, LANES), vmem(4, K, LANES),
        vmem(FIELDS, 256), vmem(256, LANES), vmem(256, LANES), vmem(256, 256), vmem(256, 256),
        vmem(256, LANES), vmem(FIELDS, LANES), vmem(LANES, 256), vmem(LANES, LANES), vmem(256, LANES),
        vmem(STEPS, ROWS, LANES), vmem(STEPS, 8, LANES), vmem(STEPS, 8, LANES), vmem(STEPS, 8, LANES),
        vmem(STEPS, 3, 8, LANES), vmem(STEPS, 3, 8, LANES), vmem(ORDERS, ROWS, LANES),
        vmem(ORDERS, 256, LANES),
        [vmem(n, chunk, LANES) for n in counts],
        [vmem(STEPS, n, 8, 256) for n in counts],
        dma(8), dma(8), dma(big_copies), dma(big_copies),
        dma(STEPS, 8), dma(STEPS, 8), dma(STEPS, small_copies), dma(STEPS, small_copies),
    ]
    shape = lambda *dims: jax.ShapeDtypeStruct(dims, F32)
    new_columns, coefficients, hessenberg, gram, new_images = pl.pallas_call(
        functools.partial(kernel, sizes),
        out_shape=[
            shape(STEPS, ROWS, LANES), shape(4, K, width), shape(STEPS, width),
            shape(FIELDS, FIELDS), shape(STEPS, ROWS, LANES),
        ],
        in_specs=[pl.BlockSpec(memory_space=pltpu.VMEM)] * 4,
        out_specs=[pl.BlockSpec(memory_space=pltpu.VMEM)] * 5,
        scratch_shapes=scratch,
        compiler_params=pltpu.CompilerParams(
            collective_id=0, has_side_effects=True, vmem_limit_bytes=48 * 1024 * 1024
        ),
    )(basis_raw.reshape(R * ROWS, LANES), krylov_raw, stiffness, rotation)
    return new_columns, coefficients, hessenberg, gram.reshape(ORDERS, K, ORDERS, K), new_images


def solution(mesh):
    cores = 2
    columns = mesh.devices.shape[1]
    depth = 8 if columns % 8 == 0 else 2
    sizes = {
        "x": mesh.devices.shape[0] // cores, "core": cores,
        "y": columns // depth, "z": depth,
    }
    split = Mesh(mesh.devices.reshape(*(sizes[a] for a in AXES)), AXES)
    return jax.shard_map(
        functools.partial(local, sizes),
        mesh=split,
        in_specs=(P(None, ROW, COL), P(), P(ROW, COL), P(ROW, COL)),
        out_specs=(P(None, ROW, COL), P(), P(), P(), P(None, ROW, COL)),
        check_vma=False,
    )
```

```python
import functools
import itertools

import jax
import jax.numpy as jnp
from jax import lax
from jax.experimental import pallas as pl
from jax.experimental.pallas import tpu as pltpu
from jax.sharding import Mesh
from jax.sharding import PartitionSpec as P

K = 40
STEPS = 3
R = 37
KRYLOV = 34
ORDERS = 5
FIELDS = ORDERS * K
COUPLING = 0.2
EPSILON = 1e-06
GRAM_SHIFT = 0.05
HIGHEST = lax.Precision.HIGHEST
AXES = ("x", "core", "y", "z")
ROW = ("x", "core")
COL = ("y", "z")
STAGES = (("x", "core"), ("y",), ("z",))
ROWS = 48
LANES = 128
GHOST = 4
PADDED = 208
GROUP = 8
F32 = jnp.float32


def dot(a, b, ca, cb):
    return lax.dot_general(
        a, b, (((ca,), (cb,)), ((), ())), precision=HIGHEST, preferred_element_type=F32
    )


def iota(shape, dim):
    return lax.broadcasted_iota(jnp.int32, shape, dim)


def offsets(sizes, axes):
    ranges = [range(sizes[a]) for a in axes]
    return [o for o in itertools.product(*ranges) if any(o)]


def place(sizes, axes):
    index = 0
    for a in axes:
        index = index * sizes[a] + lax.axis_index(a)
    return index


def peer_of(sizes, axes, off):
    return {a: lax.rem(lax.axis_index(a) + o, sizes[a]) for a, o in zip(axes, off)}


def linear(sizes, axes, coords):
    index = 0
    for a in axes:
        index = index * sizes[a] + coords[a]
    return index


def near(sizes, drow, dcol):
    rows = sizes["x"] * sizes["core"]
    cols = sizes["y"] * sizes["z"]
    r = lax.rem(place(sizes, ROW) + drow + rows, rows)
    c = lax.rem(place(sizes, COL) + dcol + cols, cols)
    return {
        "x": r // sizes["core"],
        "core": lax.rem(r, sizes["core"]),
        "y": c // sizes["z"],
        "z": lax.rem(c, sizes["z"]),
    }


def full(coords):
    return tuple(coords.get(a, lax.axis_index(a)) for a in AXES)


SIDES = [(-1, 0), (1, 0), (0, -1), (0, 1), (-1, -1), (-1, 1), (1, -1), (1, 1)]


def forward_inverse(a, count, block=4):
    sub = iota((K, LANES), 0)
    lane = iota((K, LANES), 1)
    for first in range(0, count, block):
        pivots = range(first, min(first + block, count))
        cols = [jnp.broadcast_to(a[:, j : j + 1], (K, LANES)) for j in pivots]
        rows = [a[j : j + 1, :] for j in pivots]
        for p, j in enumerate(pivots):
            inverse = 1.0 / cols[p][j : j + 1, :]
            factor = jnp.where(sub > j, cols[p] * inverse, 0.0)
            for q in range(p + 1, len(pivots)):
                cols[q] = cols[q] - factor * cols[q][j : j + 1, :]
                rows[q] = rows[q] - factor[pivots[q] : pivots[q] + 1, :] * rows[p]
            a = a - factor * rows[p]
    diag = jnp.sum(jnp.where(lane == sub, a, 0.0), axis=1, keepdims=True)
    scaled = a * (1.0 / jnp.sqrt(diag))
    return jnp.where(lane < K, pltpu.roll(scaled, 64, 1), 0.0)


def augmented(a, shift, count):
    sub = iota((K, LANES), 0)
    lane = iota((K, LANES), 1)
    a = jnp.where((lane < count) & (sub < count), a, 0.0)
    a = a + jnp.where((lane == sub) & (sub < count), shift, 0.0)
    return a + jnp.where(((lane == sub) & (sub >= count)) | (lane == sub + 64), 1.0, 0.0)


def kernel(
    sizes, x_ref, kr_ref, st_ref, ro_ref,
    newc_ref, coef_ref, hess_ref, gram_ref, newi_ref,
    X, SD, CF, PL, PR, RRB, RLB, AHL, ACC, BIG, FULL, GS, LB, GB0, CB, MT, HS, KS,
    U0, PK, HT, HB, KRB, KLB, VB, VW, UV, DN,
    slots_big, slots_small,
    hsend, hrecv, bsend, brecv, usend, urecv, ssend, srecv,
):
    nrow = sizes["x"] * sizes["core"]
    ncol = sizes["y"] * sizes["z"]
    my_row = place(sizes, ROW)
    my_col = place(sizes, COL)
    grid_rows = nrow * ROWS
    inverse_total = 1.0 / (grid_rows * ncol * LANES)
    stage_offsets = [offsets(sizes, axes) for axes in STAGES]
    pending = []

    barrier = pltpu.get_barrier_semaphore()
    count = 0
    for axes, offs in zip(STAGES, stage_offsets):
        for off in offs:
            pl.semaphore_signal(
                barrier, inc=1, device_id=full(peer_of(sizes, axes, off)),
                device_id_type=pl.DeviceIdType.MESH,
            )
            count += 1
    for side in SIDES:
        pl.semaphore_signal(
            barrier, inc=1, device_id=full(near(sizes, *side)),
            device_id_type=pl.DeviceIdType.MESH,
        )
        count += 1

    def send(src, dst, ssem, rsem, coords):
        copy = pltpu.make_async_remote_copy(
            src_ref=src, dst_ref=dst, send_sem=ssem, recv_sem=rsem,
            device_id=full(coords), device_id_type=pl.DeviceIdType.MESH,
        )
        copy.start()
        pending.append(copy)
        return copy

    def load_rows(i, carry):
        for k in range(4):
            r = 4 * i + k
            at = pl.multiple_of((r + GHOST) * K, 8)
            X[0][pl.ds(at, R), :] = x_ref[pl.ds(r, R, stride=ROWS), :]
            X[0][pl.ds(at + R, 1), :] = st_ref[pl.ds(r, 1), :]
            X[0][pl.ds(at + R + 1, 1), :] = ro_ref[pl.ds(r, 1), :]
            X[0][pl.ds(at + R + 2, 1), :] = jnp.zeros((1, LANES), F32)
        return carry

    lax.fori_loop(0, ROWS // 4, load_rows, 0)
    lane_k = iota((K, LANES), 1)

    def line(rho):
        return pl.ds(pl.multiple_of(rho * K, 8), K)

    def pack(base, n, q):
        def body(b, carry):
            left, right = carry
            for k in range(8):
                i = 8 * b + k
                row = X[0][line(base + i), :]
                here = (lane_k >= 4 * i) & (lane_k < 4 * i + 4)
                left = jnp.where(here, pltpu.roll(row, 4 * i, 1), left)
                right = jnp.where(here, pltpu.roll(row, lax.rem(4 * i + 4, LANES), 1), right)
            return left, right

        zero = jnp.zeros((K, LANES), F32)
        left, right = lax.fori_loop(0, n // 8, body, (zero, zero))
        PL[q, :, :] = left
        PR[q, :, :] = right

    pack(GHOST, 32, 0)
    pack(GHOST + 32, 16, 1)
    pl.semaphore_wait(barrier, count)

    halo = [
        send(X[0].at[pl.ds(GHOST * K, GHOST * K)], X[0].at[pl.ds((GHOST + ROWS) * K, GHOST * K)], hsend.at[0], hrecv.at[0], near(sizes, -1, 0)),
        send(X[0].at[pl.ds(ROWS * K, GHOST * K)], X[0].at[pl.ds(0, GHOST * K)], hsend.at[1], hrecv.at[1], near(sizes, 1, 0)),
        send(PL, RRB.at[pl.ds(1, 2)], hsend.at[2], hrecv.at[2], near(sizes, 0, -1)),
        send(PR, RLB.at[pl.ds(1, 2)], hsend.at[3], hrecv.at[3], near(sizes, 0, 1)),
        send(PL.at[0], RRB.at[3], hsend.at[4], hrecv.at[4], near(sizes, -1, -1)),
        send(PR.at[0], RLB.at[3], hsend.at[5], hrecv.at[5], near(sizes, -1, 1)),
        send(PL.at[1], RRB.at[0], hsend.at[6], hrecv.at[6], near(sizes, 1, -1)),
        send(PR.at[1], RLB.at[0], hsend.at[7], hrecv.at[7], near(sizes, 1, 1)),
    ]

    KS[...] = jnp.zeros((256, LANES), F32)
    for j in range(4):
        KS[pl.ds(j * K, R), pl.ds(0, KRYLOV)] = kr_ref[j]
    pt = jnp.transpose(KS[...])[0:K, :]
    kgram = dot(pt, KS[...], 1, 0)
    kinv = forward_inverse(augmented(kgram, 0.0, KRYLOV), KRYLOV)
    MT[...] = jnp.zeros((LANES, 256), F32)
    MT[pl.ds(0, K), :] = dot(kinv[:, 0:K], pt, 1, 0)
    HS[...] = jnp.zeros((LANES, LANES), F32)
    LB[...] = jnp.zeros((256, 256), F32)
    GS[...] = jnp.zeros((256, 256), F32)
    BIG[...] = jnp.zeros((256, LANES), F32)
    CF[...] = jnp.zeros((10, 64, LANES), F32)
    VW[...] = jnp.zeros((ROWS * 8, LANES), F32)
    UV[...] = jnp.zeros((ROWS * 16, LANES), F32)

    for copy in halo:
        copy.wait_recv()
    for copy in halo[:2]:
        copy.wait_send()
        pending.remove(copy)

    lane1 = iota((1, LANES), 1)
    has_right = (my_col < ncol - 1).astype(F32)
    has_left = (my_col > 0).astype(F32)
    side_mask = jnp.where(lane1 < 4, has_right, jnp.where(lane1 >= 124, has_left, 0.0))
    sub_k = iota((K, LANES), 0)

    def order_zero(base, n, part, first):
        def body(b, carry):
            stores = []
            for k in range(4):
                i = 4 * b + k
                rho = base + i
                g = my_row * ROWS + rho - GHOST
                row_mask = ((g >= 0) & (g < grid_rows)).astype(F32)
                at = 4 * (first + i)
                right = pltpu.roll(RRB[part, :, :], lax.rem(LANES - at, LANES), 1)
                left = pltpu.roll(RLB[part, :, :], lax.rem(2 * LANES - 4 - at, LANES), 1)
                ms = side_mask * row_mask
                side = jnp.where(lane_k < 4, right, left) * ms
                mid = X[0][line(rho), :] * row_mask
                mc = jnp.ones((1, LANES), F32) * row_mask
                stores.append((rho, (mid, mc), (side, ms)))
            for rho, mid, side in stores:
                for half, (v, m) in enumerate((mid, side)):
                    d = v[R : R + 1, :]
                    s = v[R + 1 : R + 2, :]
                    CF[5 * half, pl.ds(rho + 4, 1), :] = 2.0 * d * m
                    CF[5 * half + 1, pl.ds(rho + 4, 1), :] = (2.0 * COUPLING) * m
                    CF[5 * half + 2, pl.ds(rho + 4, 1), :] = 2.0 * (s - COUPLING) * m
                    CF[5 * half + 3, pl.ds(rho + 4, 1), :] = 2.0 * (s + COUPLING) * m
                    CF[5 * half + 4, pl.ds(rho + 4, 1), :] = m
                X[0][line(rho), :] = jnp.where(sub_k < R, mid[0], 0.0)
                SD[0][line(rho), :] = jnp.where(sub_k < R, side[0], 0.0)
            return carry

        lax.fori_loop(0, n // 4, body, 0)

    order_zero(0, 4, 0, 12)
    order_zero(4, 32, 1, 0)
    order_zero(36, 16, 2, 0)
    order_zero(52, 4, 3, 0)

    def images(m, n):
        def body(b, carry):
            mids, sides = [], []
            for k in range(n):
                rho = m + n * b + k
                c = X[m - 1][line(rho), :]
                s = SD[m - 1][line(rho), :]
                cu = X[m - 1][line(rho - 1), :] + X[m - 1][line(rho + 1), :]
                cl, sl = pltpu.roll(c, 1, 1), pltpu.roll(s, 1, 1)
                cr, sr = pltpu.roll(c, 127, 1), pltpu.roll(s, 127, 1)

                def row(kind):
                    return CF[kind, pl.ds(rho + 4, 1), :]

                left = jnp.where(lane_k == 0, sl, cl)
                right = jnp.where(lane_k == 127, sr, cr)
                new = row(0) * c - row(1) * cu + row(2) * right - row(3) * left
                mids.append(0.5 * new if m == 1 else new - X[m - 2][line(rho), :])
                if m < 4:
                    su = SD[m - 1][line(rho - 1), :] + SD[m - 1][line(rho + 1), :]
                    left = jnp.where(lane_k == 0, cl, sl)
                    right = jnp.where(lane_k == 127, cr, sr)
                    side = row(5) * s - row(6) * su + row(7) * right - row(8) * left
                    sides.append(0.5 * side if m == 1 else side - SD[m - 2][line(rho), :])
            for k in range(n):
                rho = m + n * b + k
                X[m][line(rho), :] = mids[k]
                if m < 4:
                    SD[m][line(rho), :] = sides[k]
            return carry

        lax.fori_loop(0, (ROWS + 8 - 2 * m) // n, body, 0)

    for m, n in zip(range(1, ORDERS), (6, 4, 5, 6)):
        images(m, n)

    ACC[...] = jnp.zeros((256 + PADDED, 256), F32)
    AHL[pl.ds(PADDED, 256 - PADDED), :] = jnp.zeros((256 - PADDED, ROWS * LANES), jnp.bfloat16)

    def lines(first, n):
        blank = [jnp.zeros((PADDED - FIELDS, LANES), F32)]
        return jnp.concatenate(
            [
                jnp.concatenate([X[m][line(first + k + GHOST), :] for m in range(ORDERS)] + blank, axis=0)
                for k in range(n)
            ],
            axis=1,
        )

    def bdot(a, b):
        return lax.dot_general(a, b, (((1,), (1,)), ((), ())), preferred_element_type=F32)

    def gram_rows(g, carry):
        for part in range(4):
            a = lines(GROUP * g + 2 * part, 2)
            hi = a.astype(jnp.bfloat16)
            at = pl.ds(pl.multiple_of((GROUP * g + 2 * part) * LANES, LANES), 2 * LANES)
            AHL[pl.ds(0, PADDED), at] = hi
            AHL[pl.ds(256, PADDED), at] = (a - hi.astype(F32)).astype(jnp.bfloat16)
        at = pl.ds(pl.multiple_of(GROUP * g * LANES, LANES), GROUP * LANES)
        ACC[:, pl.ds(0, PADDED)] += bdot(AHL[:, at], AHL[pl.ds(0, PADDED), at])
        return carry

    lax.fori_loop(0, ROWS // GROUP, gram_rows, 0)
    cross = jnp.concatenate([ACC[pl.ds(256, PADDED), :], jnp.zeros((256 - PADDED, 256), F32)], axis=0)
    ACC[pl.ds(0, PADDED), :] = ACC[pl.ds(0, PADDED), :] + cross[0:PADDED, :] + jnp.transpose(cross)[0:PADDED, :]

    def strip(ref, a, shift):
        v = ref[pl.ds(a * K, K), :]
        return pltpu.roll(v, shift % 256, 1) if shift % 256 else v

    lane_n = iota((K, LANES), 1)
    last = lane_n >= 80
    BIG[pl.ds(0, K), :] = strip(ACC, 0, 0)[:, 0:LANES]
    BIG[pl.ds(K, K), :] = strip(ACC, 1, -40)[:, 0:LANES]
    BIG[pl.ds(2 * K, K), :] = strip(ACC, 2, -80)[:, 0:LANES]
    BIG[pl.ds(3 * K, K), :] = jnp.where(last, strip(ACC, 4, -80)[:, 0:LANES], strip(ACC, 0, -120)[:, 0:LANES])
    BIG[pl.ds(4 * K, K), :] = jnp.where(last, strip(ACC, 1, -80)[:, 0:LANES], strip(ACC, 3, -120)[:, 0:LANES])

    chunk = 256 // nrow
    own = pl.ds(pl.multiple_of(my_row * chunk, 8), chunk)

    def chunk_of(coords):
        return pl.ds(pl.multiple_of(linear(sizes, ROW, coords) * chunk, 8), chunk)

    sem = 0
    for stage, (axes, offs) in enumerate(zip(STAGES, stage_offsets)):
        me = place(sizes, axes)
        box = slots_big[stage]
        if stage == 0:
            box[me] = BIG[own, :]
        copies = []
        for off in offs:
            to = peer_of(sizes, axes, off)
            src = BIG.at[chunk_of(to)] if stage == 0 else box.at[me]
            copies.append(send(src, box.at[me], bsend.at[sem], brecv.at[sem], to))
            sem += 1
        for copy in copies:
            copy.wait_recv()
        total = box[0]
        for i in range(1, len(offs) + 1):
            total = total + box[i]
        if stage + 1 < len(STAGES):
            slots_big[stage + 1][place(sizes, STAGES[stage + 1])] = total
        else:
            FULL[own, :] = total * inverse_total
    copies = []
    for off in stage_offsets[0]:
        to = peer_of(sizes, ROW, off)
        copies.append(send(FULL.at[own], FULL.at[own], bsend.at[sem], brecv.at[sem], to))
        sem += 1
    for copy in copies:
        copy.wait_recv()

    lane_w = iota((K, 256), 1)

    def wide(a):
        v = FULL[pl.ds(a * K, K), :]
        return jnp.concatenate([jnp.where(lane_n < 120, v, 0.0), jnp.zeros((K, LANES), F32)], axis=1)

    g3, g4 = wide(3), wide(4)

    def between(v, lo, hi):
        return jnp.where((lane_w >= lo) & (lane_w < hi), v, 0.0)

    GS[pl.ds(0, K), :] = wide(0) + between(pltpu.roll(g3, 120, 1), 120, 200)
    GS[pl.ds(K, K), :] = pltpu.roll(wide(1), 40, 1) + between(pltpu.roll(g4, 80, 1), 160, 200)
    GS[pl.ds(2 * K, K), :] = pltpu.roll(wide(2), 80, 1)
    GS[pl.ds(3 * K, K), :] = between(pltpu.roll(g4, 120, 1), 120, 200)
    GS[pl.ds(4 * K, K), :] = between(pltpu.roll(g3, 80, 1), 160, 200)
    mirrored = jnp.transpose(GS[...])
    for a in range(1, ORDERS):
        GS[pl.ds(a * K, K), :] = jnp.where(
            lane_w >= a * K, GS[pl.ds(a * K, K), :], mirrored[a * K : (a + 1) * K, :]
        )

    finv = forward_inverse(augmented(GS[pl.ds(0, K), pl.ds(0, LANES)], GRAM_SHIFT, R), R)
    finv = jnp.where(sub_k < R, finv, 0.0)
    finv_wide = jnp.concatenate([finv, jnp.zeros((K, LANES), F32)], axis=1)
    for a in range(ORDERS):
        LB[pl.ds(a * K, K), :] = pltpu.roll(finv_wide, a * K, 1) if a else finv_wide
    square = (iota((LANES, LANES), 0) < K) & (iota((LANES, LANES), 1) < K)
    small = jnp.where(square, LB[pl.ds(0, LANES), pl.ds(0, LANES)], 0.0)
    GB0[...] = dot(dot(LB[...], GS[:, pl.ds(0, LANES)], 1, 0), small, 1, 1)

    lane_r = iota((1, 256), 1)
    lane8 = iota((8, 256), 1)
    sub8 = iota((8, 256), 0)
    tile_mask = iota((64, LANES), 1)

    for s in range(STEPS):
        column = KRYLOV + s
        r = R + s
        latest = MT[pl.ds(column - 1, 1), :]

        def moved(shift):
            return pltpu.roll(latest, shift % 256, 1)

        cw = jnp.where(lane_r < K, 0.5 * moved(-80), -0.5 * moved(40))
        cw = jnp.where(lane_r < FIELDS, cw, 0.0)
        cw = jnp.broadcast_to(cw, (8, 256))
        h1 = dot(cw, GB0[...], 1, 0)
        h = 2.0 * h1 - dot(h1, GB0[pl.ds(0, LANES), :], 1, 0)
        h_wide = jnp.concatenate([h, jnp.zeros((8, LANES), F32)], axis=1)
        raw = dot(cw - h_wide, LB[...], 1, 0)
        raw_col = jnp.transpose(raw)[0 : FIELDS + 16, 0:1]
        CB[...] = jnp.broadcast_to(raw_col, (FIELDS + 16, LANES))

        def combine(i, carry):
            for k in range(8):
                rho = 8 * i + k + GHOST
                value = CB[pl.ds(0, K), :] * X[0][line(rho), :]
                for m in range(1, ORDERS):
                    value = value + CB[pl.ds(m * K, K), :] * X[m][line(rho), :]
                value = jnp.sum(value, axis=0, keepdims=True)
                if s:
                    at = pl.multiple_of(16 * (8 * i + k), 8)
                    older = CB[pl.ds(FIELDS, 16), :] * UV[pl.ds(at, 16), :]
                    value = value + jnp.sum(older, axis=0, keepdims=True)
                U0[s, pl.ds(8 * i + k, 1), :] = value
            return carry

        lax.fori_loop(0, ROWS // 8, combine, 0)

        lane_t = iota((8, LANES), 1)
        packed = jnp.zeros((8, LANES), F32)
        for q in range(6):
            tile = U0[s, pl.ds(8 * q, 8), :]
            packed = jnp.where(
                (lane_t >= 4 * q) & (lane_t < 4 * q + 4), pltpu.roll(tile, 4 * q, 1) if q else tile, packed
            )
            packed = jnp.where(
                (lane_t >= 64 + 4 * q) & (lane_t < 68 + 4 * q), pltpu.roll(tile, 68 + 4 * q, 1), packed
            )
        PK[s, :, :] = packed
        edge = [
            send(U0.at[s, pl.ds(0, 8)], HB.at[s], usend.at[s, 0], urecv.at[s, 0], near(sizes, -1, 0)),
            send(U0.at[s, pl.ds(40, 8)], HT.at[s], usend.at[s, 1], urecv.at[s, 1], near(sizes, 1, 0)),
            send(PK.at[s], KRB.at[s, 1], usend.at[s, 2], urecv.at[s, 2], near(sizes, 0, -1)),
            send(PK.at[s], KLB.at[s, 1], usend.at[s, 3], urecv.at[s, 3], near(sizes, 0, 1)),
            send(PK.at[s], KRB.at[s, 2], usend.at[s, 4], urecv.at[s, 4], near(sizes, -1, -1)),
            send(PK.at[s], KLB.at[s, 2], usend.at[s, 5], urecv.at[s, 5], near(sizes, -1, 1)),
            send(PK.at[s], KRB.at[s, 0], usend.at[s, 6], urecv.at[s, 6], near(sizes, 1, -1)),
            send(PK.at[s], KLB.at[s, 0], usend.at[s, 7], urecv.at[s, 7], near(sizes, 1, 1)),
        ]

        h_row = h_wide[0:1, :]
        e = jnp.where(lane_r < K, moved(-40), 0.5 * (moved(40) + moved(-40)))
        e = jnp.where(lane_r < 3 * K, e, pltpu.roll(h_row, 3 * K, 1))
        e = jnp.where(lane_r < 4 * K, e, 0.0)
        mt = MT[pl.ds(0, K), :]
        g1 = jnp.sum(mt * e, axis=1, keepdims=True)
        e1 = e - jnp.sum(mt * g1, axis=0, keepdims=True)
        g2 = jnp.sum(mt * e1, axis=1, keepdims=True)
        e2 = e1 - jnp.sum(mt * g2, axis=0, keepdims=True)
        e2_square = jnp.sum(e2 * e2, axis=1, keepdims=True)

        for copy in edge:
            copy.wait_recv()

        mids = jnp.concatenate([HT[s], U0[s], HB[s]], axis=0) * CF[4]
        sides = []
        for j in range(8):
            part = 0 if j == 0 else (2 if j == 7 else 1)
            q = 5 if j == 0 else (0 if j == 7 else j - 1)
            rt = KRB[s, part]
            lf = pltpu.roll(KLB[s, part], 60 - 4 * q, 1)
            rt = pltpu.roll(rt, LANES - 4 * q, 1) if q else rt
            sides.append(jnp.where(lane_t < 4, rt, lf))
        sds = jnp.concatenate(sides, axis=0) * CF[9]

        def twice_s(c, v):
            cl, sl = pltpu.roll(c, 1, 1), pltpu.roll(v, 1, 1)
            cr, sr = pltpu.roll(c, 127, 1), pltpu.roll(v, 127, 1)
            cu = pltpu.roll(c, 1, 0) + pltpu.roll(c, 63, 0)
            su = pltpu.roll(v, 1, 0) + pltpu.roll(v, 63, 0)
            lo, hi = tile_mask == 0, tile_mask == 127
            mid = CF[0] * c - CF[1] * cu + CF[2] * jnp.where(hi, sr, cr) - CF[3] * jnp.where(lo, sl, cl)
            side = CF[5] * v - CF[6] * su + CF[7] * jnp.where(hi, cr, sr) - CF[8] * jnp.where(lo, cl, sl)
            return mid, side

        before = (mids, sds)
        now = twice_s(*before)
        now = (0.5 * now[0], 0.5 * now[1])
        orders = [before[0], now[0]]
        for m in range(2, ORDERS):
            nxt = twice_s(*now)
            before, now = now, (nxt[0] - before[0], nxt[1] - before[1])
            orders.append(now[0])
        for m in range(ORDERS):
            VB[m, :, :] = orders[m][8:56, :]
            VW[pl.ds(m, ROWS, stride=8), :] = orders[m][8:56, :]
            UV[pl.ds(5 * s + m, ROWS, stride=16), :] = orders[m][8:56, :]

        v = jnp.concatenate([VW[pl.ds(8 * k, 8), :] for k in range(ROWS)], axis=1)
        w = jnp.concatenate([UV[pl.ds(16 * k, 16), :] for k in range(ROWS)], axis=1)
        v_hi = v.astype(jnp.bfloat16).astype(F32)
        w_hi = w.astype(jnp.bfloat16).astype(F32)
        v = jnp.concatenate([v_hi, v - v_hi], axis=0).astype(jnp.bfloat16)
        w = jnp.concatenate([w_hi, w - w_hi], axis=0).astype(jnp.bfloat16)
        old = bdot(v, AHL[...])
        new = bdot(v, w)
        new = new[0:8, :] + new[8:16, :]
        DN[...] = jnp.zeros((8, 256), F32)
        DN[:, pl.ds(FIELDS, 16)] = new[:, 0:16] + new[:, 16:32]
        old = old[0:8, :] + old[8:16, :]
        d = old[:, 0:256] + jnp.concatenate([old[:, 256:], jnp.zeros((8, 256 - PADDED), F32)], axis=1)
        d = jnp.where(lane8 < FIELDS, d, 0.0)
        d = d + DN[...]

        total = d
        sem = 0
        for stage, (axes, offs) in enumerate(zip(STAGES, stage_offsets)):
            me = place(sizes, axes)
            box = slots_small[stage].at[s]
            box[me] = total
            copies = []
            for off in offs:
                copies.append(
                    send(box.at[me], box.at[me], ssend.at[s, sem], srecv.at[s, sem], peer_of(sizes, axes, off))
                )
                sem += 1
            for copy in copies:
                copy.wait_recv()
            total = box[0]
            for i in range(1, len(offs) + 1):
                total = total + box[i]
        d = total * inverse_total

        nn = jnp.sum(jnp.where(lane_r == FIELDS + 5 * s, d[0:1, :], 0.0), axis=1, keepdims=True)
        beta = jnp.sqrt(nn + EPSILON)
        ib = 1.0 / beta
        eta = jnp.sqrt(e2_square + beta * beta + EPSILON)
        MT[pl.ds(column, 1), :] = (e2 + jnp.where(lane_r == 3 * K + r, beta, 0.0)) / eta
        sub_col = iota((K, 1), 0)
        g = g1 + g2 + jnp.where(sub_col == column, eta, 0.0)
        lane_h = iota((K, LANES), 1)
        HS[pl.ds(0, K), :] = jnp.where(lane_h == s, g, HS[pl.ds(0, K), :])
        newc_ref[s, :, :] = VB[0] * ib
        newi_ref[s, :, :] = VB[4] * ib
        for m in range(ORDERS):
            at = m * K + r
            LB[pl.ds(at, 1), :] = jnp.where(lane_r == FIELDS + 5 * s + m, ib, 0.0)
            GS[pl.ds(FIELDS + 5 * s + m, 1), :] = d[m : m + 1, :]
        if s + 1 < STEPS:
            db = dot(d, LB[...], 1, 1) * ib
            dcol = jnp.transpose(db)[:, 0:1]
            lane_g = iota((256, LANES), 1)
            GB0[...] = jnp.where(lane_g == r, dcol, GB0[...])
            for m in range(ORDERS):
                GB0[pl.ds(m * K + r, 1), :] = jnp.where(lane1 < K, db[m : m + 1, 0:LANES], 0.0)

    mirrored = jnp.transpose(GS[...])
    def age(index):
        return sum(((index >= FIELDS + 5 * t).astype(jnp.int32) for t in range(1, STEPS)), (index >= FIELDS).astype(jnp.int32))

    whole_row = age(iota((256, 256), 0))
    whole_col = age(iota((256, 256), 1))
    GS[...] = jnp.where(whole_row >= whole_col, GS[...], mirrored)
    gram = dot(dot(LB[...], GS[...], 1, 0), LB[...], 1, 1)
    gram_ref[...] = gram[0:FIELDS, 0:FIELDS]
    mcol = jnp.transpose(MT[...])
    for j in range(4):
        coef_ref[j, :, :] = mcol[j * K : (j + 1) * K, 0 : KRYLOV + STEPS]
    hess_ref[...] = jnp.transpose(HS[...])[0:STEPS, 0 : KRYLOV + STEPS]

    for copy in pending:
        copy.wait_send()


def local(sizes, basis_raw, krylov_raw, stiffness, rotation):
    width = KRYLOV + STEPS
    nrow = sizes["x"] * sizes["core"]
    counts = []
    for axes in STAGES:
        n = 1
        for a in axes:
            n *= sizes[a]
        counts.append(n)
    chunk = 256 // nrow
    big_copies = sum(n - 1 for n in counts) + counts[0] - 1
    small_copies = sum(n - 1 for n in counts)
    vmem = lambda *shape: pltpu.VMEM(shape, F32)
    half = lambda *shape: pltpu.VMEM(shape, jnp.bfloat16)
    dma = lambda *shape: pltpu.SemaphoreType.DMA(shape)
    scratch = [
        [vmem((ROWS + 8) * K, LANES) for _ in range(ORDERS)],
        [vmem((ROWS + 8) * K, LANES) for _ in range(ORDERS - 1)],
        vmem(10, 64, LANES), vmem(2, K, LANES), vmem(2, K, LANES), vmem(4, K, LANES), vmem(4, K, LANES),
        half(256 + PADDED, ROWS * LANES), vmem(256 + PADDED, 256), vmem(256, LANES), vmem(256, LANES), vmem(256, 256), vmem(256, 256),
        vmem(256, LANES), vmem(FIELDS + 16, LANES), vmem(LANES, 256), vmem(LANES, LANES), vmem(256, LANES),
        vmem(STEPS, ROWS, LANES), vmem(STEPS, 8, LANES), vmem(STEPS, 8, LANES), vmem(STEPS, 8, LANES),
        vmem(STEPS, 3, 8, LANES), vmem(STEPS, 3, 8, LANES), vmem(ORDERS, ROWS, LANES),
        vmem(ROWS * 8, LANES), vmem(ROWS * 16, LANES), vmem(8, 256),
        [vmem(n, chunk, LANES) for n in counts],
        [vmem(STEPS, n, 8, 256) for n in counts],
        dma(8), dma(8), dma(big_copies), dma(big_copies),
        dma(STEPS, 8), dma(STEPS, 8), dma(STEPS, small_copies), dma(STEPS, small_copies),
    ]
    shape = lambda *dims: jax.ShapeDtypeStruct(dims, F32)
    new_columns, coefficients, hessenberg, gram, new_images = pl.pallas_call(
        functools.partial(kernel, sizes),
        out_shape=[
            shape(STEPS, ROWS, LANES), shape(4, K, width), shape(STEPS, width),
            shape(FIELDS, FIELDS), shape(STEPS, ROWS, LANES),
        ],
        in_specs=[pl.BlockSpec(memory_space=pltpu.VMEM)] * 4,
        out_specs=[pl.BlockSpec(memory_space=pltpu.VMEM)] * 5,
        scratch_shapes=scratch,
        compiler_params=pltpu.CompilerParams(
            collective_id=0, has_side_effects=True, vmem_limit_bytes=48 * 1024 * 1024
        ),
    )(basis_raw.reshape(R * ROWS, LANES), krylov_raw, stiffness, rotation)
    return new_columns, coefficients, hessenberg, gram.reshape(ORDERS, K, ORDERS, K), new_images


def solution(mesh):
    cores = 2
    columns = mesh.devices.shape[1]
    depth = 8 if columns % 8 == 0 else 2
    sizes = {
        "x": mesh.devices.shape[0] // cores, "core": cores,
        "y": columns // depth, "z": depth,
    }
    split = Mesh(mesh.devices.reshape(*(sizes[a] for a in AXES)), AXES)
    return jax.shard_map(
        functools.partial(local, sizes),
        mesh=split,
        in_specs=(P(None, ROW, COL), P(), P(ROW, COL), P(ROW, COL)),
        out_specs=(P(None, ROW, COL), P(), P(), P(), P(None, ROW, COL)),
        check_vma=False,
    )
```

```python
import functools
import itertools

import jax
import jax.numpy as jnp
from jax import lax
from jax.experimental import pallas as pl
from jax.experimental.pallas import tpu as pltpu
from jax.sharding import Mesh
from jax.sharding import PartitionSpec as P

K = 40
STEPS = 3
R = 37
KRYLOV = 34
ORDERS = 5
FIELDS = ORDERS * K
COUPLING = 0.2
EPSILON = 1e-06
GRAM_SHIFT = 0.05
HIGHEST = lax.Precision.HIGHEST
AXES = ("x", "core", "y", "z")
ROW = ("x", "core")
COL = ("y", "z")
STAGES = (("x", "core"), ("y",), ("z",))
ROWS = 48
LANES = 128
GHOST = 4
PADDED = 208
GROUP = 8
FIRST = 128
SECOND = 192
F32 = jnp.float32


def dot(a, b, ca, cb):
    return lax.dot_general(
        a, b, (((ca,), (cb,)), ((), ())), precision=HIGHEST, preferred_element_type=F32
    )


def dot3(a, b, ca, cb):
    return lax.dot_general(
        a, b, (((ca,), (cb,)), ((), ())), precision=lax.Precision.HIGH, preferred_element_type=F32
    )


def iota(shape, dim):
    return lax.broadcasted_iota(jnp.int32, shape, dim)


def offsets(sizes, axes):
    ranges = [range(sizes[a]) for a in axes]
    return [o for o in itertools.product(*ranges) if any(o)]


def place(sizes, axes):
    index = 0
    for a in axes:
        index = index * sizes[a] + lax.axis_index(a)
    return index


def peer_of(sizes, axes, off):
    return {a: lax.rem(lax.axis_index(a) + o, sizes[a]) for a, o in zip(axes, off)}


def linear(sizes, axes, coords):
    index = 0
    for a in axes:
        index = index * sizes[a] + coords[a]
    return index


def near(sizes, drow, dcol):
    rows = sizes["x"] * sizes["core"]
    cols = sizes["y"] * sizes["z"]
    r = lax.rem(place(sizes, ROW) + drow + rows, rows)
    c = lax.rem(place(sizes, COL) + dcol + cols, cols)
    return {
        "x": r // sizes["core"],
        "core": lax.rem(r, sizes["core"]),
        "y": c // sizes["z"],
        "z": lax.rem(c, sizes["z"]),
    }


def full(coords):
    return tuple(coords.get(a, lax.axis_index(a)) for a in AXES)


SIDES = [(-1, 0), (1, 0), (0, -1), (0, 1), (-1, -1), (-1, 1), (1, -1), (1, 1)]


def forward_inverse(a, count, block=4):
    sub = iota((K, LANES), 0)
    lane = iota((K, LANES), 1)
    for first in range(0, count, block):
        pivots = range(first, min(first + block, count))
        cols = [jnp.broadcast_to(a[:, j : j + 1], (K, LANES)) for j in pivots]
        rows = [a[j : j + 1, :] for j in pivots]
        for p, j in enumerate(pivots):
            inverse = 1.0 / cols[p][j : j + 1, :]
            factor = jnp.where(sub > j, cols[p] * inverse, 0.0)
            for q in range(p + 1, len(pivots)):
                cols[q] = cols[q] - factor * cols[q][j : j + 1, :]
                rows[q] = rows[q] - factor[pivots[q] : pivots[q] + 1, :] * rows[p]
            a = a - factor * rows[p]
    diag = jnp.sum(jnp.where(lane == sub, a, 0.0), axis=1, keepdims=True)
    scaled = a * (1.0 / jnp.sqrt(diag))
    return jnp.where(lane < K, pltpu.roll(scaled, 64, 1), 0.0)


def augmented(a, shift, count):
    sub = iota((K, LANES), 0)
    lane = iota((K, LANES), 1)
    a = jnp.where((lane < count) & (sub < count), a, 0.0)
    a = a + jnp.where((lane == sub) & (sub < count), shift, 0.0)
    return a + jnp.where(((lane == sub) & (sub >= count)) | (lane == sub + 64), 1.0, 0.0)


def kernel(
    sizes, x_hbm, kr_hbm, st_hbm, ro_hbm,
    newc_ref, coef_ref, hess_ref, gram_ref, newi_ref,
    x_ref, kr_ref, st_ref, ro_ref, in_sem,
    X, SD, CF, PL, PR, RRB, RLB, AHL, ACC, AC0, BIG, FULL, BIG2, FULL2, GS, GC, LB, GB0, CB, MT, HS, KS,
    U0, PK, HT, HB, KRB, KLB, VB, VW, UV, DN,
    slots_big, slots_two, slots_small, slots_last, slots_late,
    hsend, hrecv, bsend, brecv, csend, crecv, usend, urecv, ssend, srecv, lsend, lrecv,
):
    nrow = sizes["x"] * sizes["core"]
    ncol = sizes["y"] * sizes["z"]
    my_row = place(sizes, ROW)
    my_col = place(sizes, COL)
    grid_rows = nrow * ROWS
    inverse_total = 1.0 / (grid_rows * ncol * LANES)
    stage_offsets = [offsets(sizes, axes) for axes in STAGES]
    pending = []

    loads = [
        pltpu.make_async_copy(src, dst, in_sem.at[i])
        for i, (src, dst) in enumerate(
            ((x_hbm, x_ref), (st_hbm, st_ref), (ro_hbm, ro_ref), (kr_hbm, kr_ref))
        )
    ]
    for copy in loads:
        copy.start()

    barrier = pltpu.get_barrier_semaphore()
    count = 0
    for axes, offs in zip(STAGES, stage_offsets):
        for off in offs:
            pl.semaphore_signal(
                barrier, inc=1, device_id=full(peer_of(sizes, axes, off)),
                device_id_type=pl.DeviceIdType.MESH,
            )
            count += 1
    for side in SIDES:
        pl.semaphore_signal(
            barrier, inc=1, device_id=full(near(sizes, *side)),
            device_id_type=pl.DeviceIdType.MESH,
        )
        count += 1

    def send(src, dst, ssem, rsem, coords):
        copy = pltpu.make_async_remote_copy(
            src_ref=src, dst_ref=dst, send_sem=ssem, recv_sem=rsem,
            device_id=full(coords), device_id_type=pl.DeviceIdType.MESH,
        )
        copy.start()
        pending.append(copy)
        return copy

    def load_rows(i, carry):
        for k in range(4):
            r = 4 * i + k
            at = pl.multiple_of((r + GHOST) * K, 8)
            X[0][pl.ds(at, R), :] = x_ref[pl.ds(r, R, stride=ROWS), :]
            X[0][pl.ds(at + R, 1), :] = st_ref[pl.ds(r, 1), :]
            X[0][pl.ds(at + R + 1, 1), :] = ro_ref[pl.ds(r, 1), :]
            X[0][pl.ds(at + R + 2, 1), :] = jnp.zeros((1, LANES), F32)
        return carry

    for copy in loads[:3]:
        copy.wait()
    lax.fori_loop(0, ROWS // 4, load_rows, 0)
    lane_k = iota((K, LANES), 1)

    def line(rho):
        return pl.ds(pl.multiple_of(rho * K, 8), K)

    def pack(base, n, q):
        def body(b, carry):
            left, right = carry
            for k in range(8):
                i = 8 * b + k
                row = X[0][line(base + i), :]
                here = (lane_k >= 4 * i) & (lane_k < 4 * i + 4)
                left = jnp.where(here, pltpu.roll(row, 4 * i, 1), left)
                right = jnp.where(here, pltpu.roll(row, lax.rem(4 * i + 4, LANES), 1), right)
            return left, right

        zero = jnp.zeros((K, LANES), F32)
        left, right = lax.fori_loop(0, n // 8, body, (zero, zero))
        PL[q, :, :] = left
        PR[q, :, :] = right

    pack(GHOST, 32, 0)
    pack(GHOST + 32, 16, 1)
    pl.semaphore_wait(barrier, count)

    halo = [
        send(X[0].at[pl.ds(GHOST * K, GHOST * K)], X[0].at[pl.ds((GHOST + ROWS) * K, GHOST * K)], hsend.at[0], hrecv.at[0], near(sizes, -1, 0)),
        send(X[0].at[pl.ds(ROWS * K, GHOST * K)], X[0].at[pl.ds(0, GHOST * K)], hsend.at[1], hrecv.at[1], near(sizes, 1, 0)),
        send(PL, RRB.at[pl.ds(1, 2)], hsend.at[2], hrecv.at[2], near(sizes, 0, -1)),
        send(PR, RLB.at[pl.ds(1, 2)], hsend.at[3], hrecv.at[3], near(sizes, 0, 1)),
        send(PL.at[0], RRB.at[3], hsend.at[4], hrecv.at[4], near(sizes, -1, -1)),
        send(PR.at[0], RLB.at[3], hsend.at[5], hrecv.at[5], near(sizes, -1, 1)),
        send(PL.at[1], RRB.at[0], hsend.at[6], hrecv.at[6], near(sizes, 1, -1)),
        send(PR.at[1], RLB.at[0], hsend.at[7], hrecv.at[7], near(sizes, 1, 1)),
    ]

    loads[3].wait()
    KS[...] = jnp.zeros((K, 256), F32)
    for j in range(4):
        KS[pl.ds(0, KRYLOV), pl.ds(j * K, R)] = kr_ref[:, j, :]
    pt = KS[...]
    kgram = dot(pt, pt, 1, 1)
    kgram = jnp.concatenate([kgram, jnp.zeros((K, LANES - K), F32)], axis=1)
    kinv = forward_inverse(augmented(kgram, 0.0, KRYLOV), KRYLOV)
    MT[...] = jnp.zeros((LANES, 256), F32)
    MT[pl.ds(0, K), :] = dot(kinv[:, 0:K], pt, 1, 0)
    HS[...] = jnp.zeros((LANES, LANES), F32)
    LB[...] = jnp.zeros((256, 256), F32)
    GS[...] = jnp.zeros((256, 256), F32)
    BIG[...] = jnp.zeros((FIRST, LANES), F32)
    BIG2[...] = jnp.zeros((SECOND, LANES), F32)
    CF[...] = jnp.zeros((10, 64, LANES), F32)
    VW[...] = jnp.zeros((ROWS * 8, LANES), F32)
    UV[...] = jnp.zeros((ROWS * 24, LANES), F32)

    for copy in halo:
        copy.wait_recv()
    for copy in halo[:2]:
        copy.wait_send()
        pending.remove(copy)

    lane1 = iota((1, LANES), 1)
    has_right = (my_col < ncol - 1).astype(F32)
    has_left = (my_col > 0).astype(F32)
    side_mask = jnp.where(lane1 < 4, has_right, jnp.where(lane1 >= 124, has_left, 0.0))
    sub_k = iota((K, LANES), 0)

    def order_zero(base, n, part, first):
        def body(b, carry):
            stores = []
            for k in range(4):
                i = 4 * b + k
                rho = base + i
                g = my_row * ROWS + rho - GHOST
                row_mask = ((g >= 0) & (g < grid_rows)).astype(F32)
                at = 4 * (first + i)
                right = pltpu.roll(RRB[part, :, :], lax.rem(LANES - at, LANES), 1)
                left = pltpu.roll(RLB[part, :, :], lax.rem(2 * LANES - 4 - at, LANES), 1)
                ms = side_mask * row_mask
                side = jnp.where(lane_k < 4, right, left) * ms
                mid = X[0][line(rho), :] * row_mask
                mc = jnp.ones((1, LANES), F32) * row_mask
                stores.append((rho, (mid, mc), (side, ms)))
            for rho, mid, side in stores:
                for half, (v, m) in enumerate((mid, side)):
                    d = v[R : R + 1, :]
                    s = v[R + 1 : R + 2, :]
                    CF[5 * half, pl.ds(rho + 4, 1), :] = 2.0 * d * m
                    CF[5 * half + 1, pl.ds(rho + 4, 1), :] = (2.0 * COUPLING) * m
                    CF[5 * half + 2, pl.ds(rho + 4, 1), :] = 2.0 * (s - COUPLING) * m
                    CF[5 * half + 3, pl.ds(rho + 4, 1), :] = 2.0 * (s + COUPLING) * m
                    CF[5 * half + 4, pl.ds(rho + 4, 1), :] = m
                X[0][line(rho), :] = jnp.where(sub_k < R, mid[0], 0.0)
                SD[0][line(rho), :] = jnp.where(sub_k < R, side[0], 0.0)
            return carry

        lax.fori_loop(0, n // 4, body, 0)

    order_zero(0, 4, 0, 12)
    order_zero(4, 32, 1, 0)
    order_zero(36, 16, 2, 0)
    order_zero(52, 4, 3, 0)

    def images(m, n):
        def body(b, carry):
            mids, sides = [], []
            for k in range(n):
                rho = m + n * b + k
                c = X[m - 1][line(rho), :]
                s = SD[m - 1][line(rho), :]
                cu = X[m - 1][line(rho - 1), :] + X[m - 1][line(rho + 1), :]
                cl, sl = pltpu.roll(c, 1, 1), pltpu.roll(s, 1, 1)
                cr, sr = pltpu.roll(c, 127, 1), pltpu.roll(s, 127, 1)

                def row(kind):
                    return CF[kind, pl.ds(rho + 4, 1), :]

                left = jnp.where(lane_k == 0, sl, cl)
                right = jnp.where(lane_k == 127, sr, cr)
                new = row(0) * c - row(1) * cu + row(2) * right - row(3) * left
                mids.append(0.5 * new if m == 1 else new - X[m - 2][line(rho), :])
                if m < 4:
                    su = SD[m - 1][line(rho - 1), :] + SD[m - 1][line(rho + 1), :]
                    left = jnp.where(lane_k == 0, cl, sl)
                    right = jnp.where(lane_k == 127, cr, sr)
                    side = row(5) * s - row(6) * su + row(7) * right - row(8) * left
                    sides.append(0.5 * side if m == 1 else side - SD[m - 2][line(rho), :])
            for k in range(n):
                rho = m + n * b + k
                X[m][line(rho), :] = mids[k]
                if m < 4:
                    SD[m][line(rho), :] = sides[k]
            return carry

        lax.fori_loop(0, (ROWS + 8 - 2 * m) // n, body, 0)

    for m, n in zip(range(1, ORDERS), (6, 4, 5, 6)):
        images(m, n)

    AC0[...] = jnp.zeros((96, 512), F32)
    AHL[pl.ds(PADDED, 256 - PADDED), :] = jnp.zeros((256 - PADDED, ROWS * LANES), jnp.bfloat16)

    def lines(first, n):
        blank = [jnp.zeros((PADDED - FIELDS, LANES), F32)]
        return jnp.concatenate(
            [
                jnp.concatenate([X[m][line(first + k + GHOST), :] for m in range(ORDERS)] + blank, axis=0)
                for k in range(n)
            ],
            axis=1,
        )

    def bdot(a, b):
        return lax.dot_general(a, b, (((1,), (1,)), ((), ())), preferred_element_type=F32)

    def split_rows(g):
        for part in range(GROUP // 2):
            a = lines(GROUP * g + 2 * part, 2)
            hi = a.astype(jnp.bfloat16)
            at = pl.ds(pl.multiple_of((GROUP * g + 2 * part) * LANES, LANES), 2 * LANES)
            AHL[pl.ds(0, PADDED), at] = hi
            AHL[pl.ds(256, PADDED), at] = (a - hi.astype(F32)).astype(jnp.bfloat16)

    def gram_rows(g):
        at = pl.ds(pl.multiple_of(GROUP * g * LANES, LANES), GROUP * LANES)
        first = jnp.concatenate([AHL[pl.ds(0, 48), at], AHL[pl.ds(256, 48), at]], axis=0)
        return bdot(first, AHL[:, at])

    def gram_step(g, carry):
        part = gram_rows(g - 1)
        split_rows(g)
        AC0[:, pl.ds(0, 256 + PADDED)] += part
        return carry

    split_rows(0)
    lax.fori_loop(1, ROWS // GROUP, gram_step, 0)
    AC0[:, pl.ds(0, 256 + PADDED)] += gram_rows(ROWS // GROUP - 1)
    top = AC0[pl.ds(0, K), pl.ds(0, 256)] + AC0[pl.ds(48, K), pl.ds(0, 256)] + AC0[pl.ds(0, K), pl.ds(256, 256)]
    lane_w = iota((K, 256), 1)
    top = jnp.where(lane_w < FIELDS, top, 0.0)
    BIG[pl.ds(0, K), :] = top[:, 0:LANES]
    BIG[pl.ds(K, K), :] = top[:, LANES:]

    class Reduction:
        def __init__(self, big, whole, boxes, total_rows, send_sems, recv_sems):
            self.big, self.whole, self.boxes = big, whole, boxes
            self.chunk = total_rows // nrow
            self.send_sems, self.recv_sems, self.sem = send_sems, recv_sems, 0
            self.own = pl.ds(pl.multiple_of(my_row * self.chunk, 8), self.chunk)
            self.copies = []

        def emit(self, src, dst, to):
            self.copies.append(send(src, dst, self.send_sems.at[self.sem], self.recv_sems.at[self.sem], to))
            self.sem += 1

        def arrived(self):
            for copy in self.copies:
                copy.wait_recv()
            self.copies = []

        def start(self, stage):
            me = place(sizes, STAGES[stage])
            box = self.boxes[stage]
            if stage == 0:
                box[me] = self.big[self.own, :]
            for off in stage_offsets[stage]:
                to = peer_of(sizes, STAGES[stage], off)
                if stage == 0:
                    at = pl.multiple_of(linear(sizes, ROW, to) * self.chunk, 8)
                    self.emit(self.big.at[pl.ds(at, self.chunk)], box.at[me], to)
                else:
                    self.emit(box.at[me], box.at[me], to)

        def finish(self, stage):
            self.arrived()
            box = self.boxes[stage]
            total = box[0]
            for i in range(1, len(stage_offsets[stage]) + 1):
                total = total + box[i]
            if stage + 1 < len(STAGES):
                self.boxes[stage + 1][place(sizes, STAGES[stage + 1])] = total
            else:
                self.whole[self.own, :] = total * inverse_total

        def gather(self):
            for off in stage_offsets[0]:
                self.emit(self.whole.at[self.own], self.whole.at[self.own], peer_of(sizes, ROW, off))

    class Sum:
        def __init__(self, boxes, send_sems, recv_sems):
            self.boxes, self.send_sems, self.recv_sems, self.sem = boxes, send_sems, recv_sems, 0

        def start(self, stage, value):
            me = place(sizes, STAGES[stage])
            box = self.boxes[stage]
            box[me] = value
            self.copies = []
            for off in stage_offsets[stage]:
                to = peer_of(sizes, STAGES[stage], off)
                sems = self.send_sems.at[self.sem], self.recv_sems.at[self.sem]
                self.copies.append(send(box.at[me], box.at[me], *sems, to))
                self.sem += 1

        def finish(self, stage):
            for copy in self.copies:
                copy.wait_recv()
            box = self.boxes[stage]
            total = box[0]
            for i in range(1, len(stage_offsets[stage]) + 1):
                total = total + box[i]
            return total

    one = Reduction(BIG, FULL, slots_big, FIRST, bsend, brecv)
    two = Reduction(BIG2, FULL2, slots_two, SECOND, csend, crecv)
    one.start(0)

    ACC[...] = jnp.zeros((256 + PADDED, 256), F32)

    def gram_rest(g, carry):
        at = pl.ds(pl.multiple_of(GROUP * g * LANES, LANES), GROUP * LANES)
        ACC[:, pl.ds(0, PADDED)] += bdot(AHL[:, at], AHL[pl.ds(0, PADDED), at])
        return carry

    lax.fori_loop(0, ROWS // GROUP, gram_rest, 0)
    cross = jnp.concatenate([ACC[pl.ds(256, PADDED), :], jnp.zeros((256 - PADDED, 256), F32)], axis=0)
    ACC[pl.ds(0, PADDED), :] = ACC[pl.ds(0, PADDED), :] + cross[0:PADDED, :] + jnp.transpose(cross)[0:PADDED, :]

    def strip(a, shift):
        return pltpu.roll(ACC[pl.ds(a * K, K), :], shift % 256, 1)[:, 0:LANES]

    lane_n = iota((K, LANES), 1)
    BIG2[pl.ds(0, K), :] = strip(1, -40)
    BIG2[pl.ds(K, K), :] = strip(2, -80)
    BIG2[pl.ds(2 * K, K), :] = jnp.where(lane_n >= 80, strip(4, -80), strip(3, -120))
    BIG2[pl.ds(3 * K, K), :] = strip(1, -160)

    for stage in range(3):
        one.finish(stage)
        if stage < 2:
            one.start(stage + 1)
    one.gather()
    one.arrived()
    two.start(0)

    GS[pl.ds(0, K), pl.ds(0, LANES)] = FULL[pl.ds(0, K), :]
    GS[pl.ds(0, K), pl.ds(LANES, LANES)] = FULL[pl.ds(K, K), :]
    GC[...] = jnp.transpose(GS[pl.ds(0, LANES), :])

    def assemble_rest():
        def wide(a):
            v = FULL2[pl.ds(a * K, K), :]
            return jnp.concatenate([v, jnp.zeros((K, LANES), F32)], axis=1)

        def moved(v, shift, lo, hi):
            return jnp.where((lane_w >= lo) & (lane_w < hi), pltpu.roll(v, shift, 1), 0.0)

        GS[pl.ds(K, K), :] = moved(wide(0), 40, 40, 160) + moved(wide(3), 160, 160, 200)
        GS[pl.ds(2 * K, K), :] = moved(wide(1), 80, 80, 200)
        GS[pl.ds(3 * K, K), :] = moved(wide(2), 120, 120, 200)
        GS[pl.ds(4 * K, K), :] = moved(wide(2), 80, 160, 200)
        mirrored = jnp.transpose(GS[...])
        for a in range(1, ORDERS):
            GS[pl.ds(a * K, K), :] = jnp.where(
                lane_w >= a * K, GS[pl.ds(a * K, K), :], mirrored[a * K : (a + 1) * K, :]
            )

    finv = forward_inverse(augmented(GS[pl.ds(0, K), pl.ds(0, LANES)], GRAM_SHIFT, R), R)
    finv = jnp.where(sub_k < R, finv, 0.0)
    finv_wide = jnp.concatenate([finv, jnp.zeros((K, LANES), F32)], axis=1)
    for a in range(ORDERS):
        LB[pl.ds(a * K, K), :] = pltpu.roll(finv_wide, a * K, 1) if a else finv_wide
    square = (iota((LANES, LANES), 0) < K) & (iota((LANES, LANES), 1) < K)
    small = jnp.where(square, LB[pl.ds(0, LANES), pl.ds(0, LANES)], 0.0)
    GB0[...] = dot3(dot3(LB[...], GC[...], 1, 0), small, 1, 1)

    lane_r = iota((1, 256), 1)
    lane8 = iota((8, 256), 1)
    late = [Sum([b.at[s] for b in slots_late], lsend.at[s], lrecv.at[s]) for s in range(STEPS - 1)]

    def paired():
        v = jnp.concatenate([VW[pl.ds(8 * k, 8), :] for k in range(ROWS)], axis=1)
        v_hi = v.astype(jnp.bfloat16).astype(F32)
        return jnp.concatenate([v_hi, v - v_hi], axis=0).astype(jnp.bfloat16)

    def with_old(v):
        old = bdot(v, AHL[...])
        old = old[0:8, :] + old[8:16, :]
        d = old[:, 0:256] + jnp.concatenate([old[:, 256:], jnp.zeros((8, 256 - PADDED), F32)], axis=1)
        return jnp.where(lane8 < FIELDS, d, 0.0)

    def with_first(v):
        first = jnp.concatenate([AHL[pl.ds(0, 48), :], AHL[pl.ds(256, 48), :]], axis=0)
        part = bdot(v, first)
        return part[0:8, 0:K] + part[8:16, 0:K] + part[0:8, 48 : 48 + K]

    def with_new(v):
        w = jnp.concatenate([UV[pl.ds(24 * k, 24), :] for k in range(ROWS)], axis=1)
        w_hi = w.astype(jnp.bfloat16).astype(F32)
        w = jnp.concatenate([w_hi, w - w_hi], axis=0).astype(jnp.bfloat16)
        new = bdot(v, w)
        new = new[0:8, :] + new[8:16, :]
        return new[:, 0:24] + new[:, 24:48]

    def keep_late(s, total):
        rows = pl.ds(FIELDS + 8 * s, 8)
        GS[rows, :] = GS[rows, :] + total * inverse_total
    sub8 = iota((8, 256), 0)
    tile_mask = iota((64, LANES), 1)

    for s in range(STEPS):
        column = KRYLOV + s
        r = R + s
        latest = MT[pl.ds(column - 1, 1), :]

        def moved(shift):
            return pltpu.roll(latest, shift % 256, 1)

        cw = jnp.where(lane_r < K, 0.5 * moved(-80), -0.5 * moved(40))
        cw = jnp.where(lane_r < FIELDS, cw, 0.0)
        cw = jnp.broadcast_to(cw, (8, 256))
        h1 = dot3(cw, GB0[...], 1, 0)
        h = 2.0 * h1 - dot3(h1, GB0[pl.ds(0, LANES), :], 1, 0)
        h_wide = jnp.concatenate([h, jnp.zeros((8, LANES), F32)], axis=1)
        raw = dot3(cw - h_wide, LB[...], 1, 0)
        raw_col = jnp.transpose(raw)[0 : FIELDS + 24, 0:1]
        CB[...] = jnp.broadcast_to(raw_col, (FIELDS + 24, LANES))

        def combine(i, carry):
            for k in range(8):
                rho = 8 * i + k + GHOST
                value = CB[pl.ds(0, K), :] * X[0][line(rho), :]
                for m in range(1, ORDERS):
                    value = value + CB[pl.ds(m * K, K), :] * X[m][line(rho), :]
                value = jnp.sum(value, axis=0, keepdims=True)
                if s:
                    at = pl.multiple_of(24 * (8 * i + k), 8)
                    older = CB[pl.ds(FIELDS, 16), :] * UV[pl.ds(at, 16), :]
                    value = value + jnp.sum(older, axis=0, keepdims=True)
                U0[s, pl.ds(8 * i + k, 1), :] = value
            return carry

        lax.fori_loop(0, ROWS // 8, combine, 0)

        lane_t = iota((8, LANES), 1)
        sub_t = iota((8, LANES), 0)
        packed = jnp.zeros((8, LANES), F32)
        for q in range(6):
            tile = U0[s, pl.ds(8 * q, 8), :]
            packed = jnp.where(
                (lane_t >= 4 * q) & (lane_t < 4 * q + 4), pltpu.roll(tile, 4 * q, 1) if q else tile, packed
            )
            packed = jnp.where(
                (lane_t >= 64 + 4 * q) & (lane_t < 68 + 4 * q), pltpu.roll(tile, 68 + 4 * q, 1), packed
            )
        PK[s, :, :] = packed
        edge = [
            send(U0.at[s, pl.ds(0, 8)], HB.at[s], usend.at[s, 0], urecv.at[s, 0], near(sizes, -1, 0)),
            send(U0.at[s, pl.ds(40, 8)], HT.at[s], usend.at[s, 1], urecv.at[s, 1], near(sizes, 1, 0)),
            send(PK.at[s], KRB.at[s, 1], usend.at[s, 2], urecv.at[s, 2], near(sizes, 0, -1)),
            send(PK.at[s], KLB.at[s, 1], usend.at[s, 3], urecv.at[s, 3], near(sizes, 0, 1)),
            send(PK.at[s], KRB.at[s, 2], usend.at[s, 4], urecv.at[s, 4], near(sizes, -1, -1)),
            send(PK.at[s], KLB.at[s, 2], usend.at[s, 5], urecv.at[s, 5], near(sizes, -1, 1)),
            send(PK.at[s], KRB.at[s, 0], usend.at[s, 6], urecv.at[s, 6], near(sizes, 1, -1)),
            send(PK.at[s], KLB.at[s, 0], usend.at[s, 7], urecv.at[s, 7], near(sizes, 1, 1)),
        ]

        if s + 1 < STEPS:
            VW[pl.ds(0, ROWS, stride=8), :] = U0[s]
            d_old = with_old(paired())
        h_row = h_wide[0:1, :]
        e = jnp.where(lane_r < K, moved(-40), 0.5 * (moved(40) + moved(-40)))
        e = jnp.where(lane_r < 3 * K, e, pltpu.roll(h_row, 3 * K, 1))
        e = jnp.where(lane_r < 4 * K, e, 0.0)
        mt = MT[pl.ds(0, K), :]
        g1 = jnp.sum(mt * e, axis=1, keepdims=True)
        e1 = e - jnp.sum(mt * g1, axis=0, keepdims=True)
        g2 = jnp.sum(mt * e1, axis=1, keepdims=True)
        e2 = e1 - jnp.sum(mt * g2, axis=0, keepdims=True)
        e2_square = jnp.sum(e2 * e2, axis=1, keepdims=True)

        if s == 0:
            two.finish(0)
            two.start(1)
        if s == 1:
            two.finish(2)
            two.gather()
            late[0].start(1, late[0].finish(0))
        if s == 2:
            keep_late(0, late[0].finish(2))
            late[1].start(1, late[1].finish(0))
        for copy in edge:
            copy.wait_recv()

        mids = jnp.concatenate([HT[s], U0[s], HB[s]], axis=0) * CF[4]
        sides = []
        for j in range(8):
            part = 0 if j == 0 else (2 if j == 7 else 1)
            q = 5 if j == 0 else (0 if j == 7 else j - 1)
            rt = KRB[s, part]
            lf = pltpu.roll(KLB[s, part], 60 - 4 * q, 1)
            rt = pltpu.roll(rt, LANES - 4 * q, 1) if q else rt
            sides.append(jnp.where(lane_t < 4, rt, lf))
        sds = jnp.concatenate(sides, axis=0) * CF[9]

        def twice_s(c, v):
            cl, sl = pltpu.roll(c, 1, 1), pltpu.roll(v, 1, 1)
            cr, sr = pltpu.roll(c, 127, 1), pltpu.roll(v, 127, 1)
            cu = pltpu.roll(c, 1, 0) + pltpu.roll(c, 63, 0)
            su = pltpu.roll(v, 1, 0) + pltpu.roll(v, 63, 0)
            lo, hi = tile_mask == 0, tile_mask == 127
            mid = CF[0] * c - CF[1] * cu + CF[2] * jnp.where(hi, sr, cr) - CF[3] * jnp.where(lo, sl, cl)
            side = CF[5] * v - CF[6] * su + CF[7] * jnp.where(hi, cr, sr) - CF[8] * jnp.where(lo, cl, sl)
            return mid, side

        before = (mids, sds)
        now = twice_s(*before)
        now = (0.5 * now[0], 0.5 * now[1])
        orders = [before[0], now[0]]
        for m in range(2, ORDERS):
            nxt = twice_s(*now)
            before, now = now, (nxt[0] - before[0], nxt[1] - before[1])
            orders.append(now[0])
        for m in range(ORDERS):
            VB[m, :, :] = orders[m][8:56, :]
            VW[pl.ds(m, ROWS, stride=8), :] = orders[m][8:56, :]
            UV[pl.ds(8 * s + m, ROWS, stride=24), :] = orders[m][8:56, :]

        v = paired()
        if s + 1 < STEPS:
            total_sum = Sum([b.at[s] for b in slots_small], ssend.at[s], srecv.at[s])
            DN[...] = jnp.zeros((8, 256), F32)
            DN[:, pl.ds(0, K)] = with_first(v)
            DN[:, pl.ds(72, 24)] = with_new(v)
            low = pltpu.roll(DN[:, pl.ds(0, LANES)], 1, 0)
            wide_row = d_old[0:1, :]
            packed_new = jnp.where((lane_t >= 72) & (lane_t < 96), DN[0:1, pl.ds(0, LANES)], wide_row[:, LANES:])
            value = jnp.where(sub_t == 0, wide_row[:, 0:LANES], jnp.where(sub_t == 1, packed_new, low))
        else:
            total_sum = Sum(slots_last, ssend.at[s], srecv.at[s])
            DN[...] = with_old(v)
            DN[:, pl.ds(FIELDS, 24)] = with_new(v)
            value = DN[...]
        for stage in range(3):
            total_sum.start(stage, value)
            if stage == 0 and s + 1 < STEPS:
                rest = jnp.where((lane8 >= K) & (sub8 >= 1) & (sub8 < ORDERS), with_old(v), 0.0)
            if s == 0 and stage == 2:
                two.finish(1)
                two.start(2)
                late[0].start(0, rest)
            if s == 1 and stage == 0:
                two.arrived()
                assemble_rest()
            if s == 1 and stage == 2:
                late[0].start(2, late[0].finish(1))
                late[1].start(0, rest)
            if s == 2 and stage == 2:
                late[1].start(2, late[1].finish(1))
            value = total_sum.finish(stage)
        if s + 1 < STEPS:
            up = pltpu.roll(value, 7, 0)
            mid = (lane_t >= 72) & (lane_t < 96)
            left = jnp.where(sub_t == 0, value, jnp.where(lane_t < K, up, 0.0))
            right = jnp.where((sub_t == 0) | mid, up, 0.0)
            value = jnp.concatenate([left, right], axis=1)
        d = value * inverse_total
        d = jnp.where(sub8 < ORDERS, d, 0.0)

        nn = jnp.sum(jnp.where(lane_r == FIELDS + 8 * s, d[0:1, :], 0.0), axis=1, keepdims=True)
        beta = jnp.sqrt(nn + EPSILON)
        ib = 1.0 / beta
        eta = jnp.sqrt(e2_square + beta * beta + EPSILON)
        MT[pl.ds(column, 1), :] = (e2 + jnp.where(lane_r == 3 * K + r, beta, 0.0)) / eta
        sub_col = iota((K, 1), 0)
        g = g1 + g2 + jnp.where(sub_col == column, eta, 0.0)
        lane_h = iota((K, LANES), 1)
        HS[pl.ds(0, K), :] = jnp.where(lane_h == s, g, HS[pl.ds(0, K), :])
        newc_ref[s, :, :] = VB[0] * ib
        newi_ref[s, :, :] = VB[4] * ib
        for m in range(ORDERS):
            at = m * K + r
            LB[pl.ds(at, 1), :] = jnp.where(lane_r == FIELDS + 8 * s + m, ib, 0.0)
        GS[pl.ds(FIELDS + 8 * s, 8), :] = d
        if s + 1 < STEPS:
            db = dot3(d, LB[...], 1, 1) * ib
            dcol = jnp.transpose(db)[:, 0:1]
            lane_g = iota((256, LANES), 1)
            GB0[...] = jnp.where(lane_g == r, dcol, GB0[...])
            for m in range(ORDERS):
                GB0[pl.ds(m * K + r, 1), :] = jnp.where(lane1 < K, db[m : m + 1, 0:LANES], 0.0)

    keep_late(1, late[1].finish(2))
    mirrored = jnp.transpose(GS[...])
    def age(index):
        return sum(((index >= FIELDS + 8 * t).astype(jnp.int32) for t in range(1, STEPS)), (index >= FIELDS).astype(jnp.int32))

    whole_row = age(iota((256, 256), 0))
    whole_col = age(iota((256, 256), 1))
    GS[...] = jnp.where(whole_row >= whole_col, GS[...], mirrored)
    gram = dot3(dot3(LB[...], GS[...], 1, 0), LB[...], 1, 1)
    for a in range(ORDERS):
        for b in range(ORDERS):
            gram_ref[a, b, :, :] = gram[a * K : (a + 1) * K, b * K : (b + 1) * K]
    for j in range(4):
        coef_ref[:, j, :] = MT[pl.ds(0, KRYLOV + STEPS), pl.ds(j * K, K)]
    hess_ref[...] = jnp.transpose(HS[...])[0:STEPS, 0 : KRYLOV + STEPS]

    for copy in pending:
        copy.wait_send()


def handed_out(*refs):
    sources, targets, sems = refs[:5], refs[5:10], refs[10]
    copies = [pltpu.make_async_copy(a, b, sems.at[i]) for i, (a, b) in enumerate(zip(sources, targets))]
    for copy in copies:
        copy.start()
    for copy in copies:
        copy.wait()


def local(sizes, basis_raw, krylov_raw, stiffness, rotation):
    width = KRYLOV + STEPS
    nrow = sizes["x"] * sizes["core"]
    counts = []
    for axes in STAGES:
        n = 1
        for a in axes:
            n *= sizes[a]
        counts.append(n)
    big_copies = sum(n - 1 for n in counts) + counts[0] - 1
    small_copies = sum(n - 1 for n in counts)
    vmem = lambda *shape: pltpu.VMEM(shape, F32)
    half = lambda *shape: pltpu.VMEM(shape, jnp.bfloat16)
    dma = lambda *shape: pltpu.SemaphoreType.DMA(shape)
    scratch = [
        vmem(R * ROWS, LANES), vmem(KRYLOV, 4, R), vmem(ROWS, LANES), vmem(ROWS, LANES), dma(4),
        [vmem((ROWS + 8) * K, LANES) for _ in range(ORDERS)],
        [vmem((ROWS + 8) * K, LANES) for _ in range(ORDERS - 1)],
        vmem(10, 64, LANES), vmem(2, K, LANES), vmem(2, K, LANES), vmem(4, K, LANES), vmem(4, K, LANES),
        half(256 + PADDED, ROWS * LANES), vmem(256 + PADDED, 256), vmem(96, 512),
        vmem(FIRST, LANES), vmem(FIRST, LANES), vmem(SECOND, LANES), vmem(SECOND, LANES),
        vmem(256, 256), vmem(256, LANES), vmem(256, 256),
        vmem(256, LANES), vmem(FIELDS + 24, LANES), vmem(LANES, 256), vmem(LANES, LANES), vmem(K, 256),
        vmem(STEPS, ROWS, LANES), vmem(STEPS, 8, LANES), vmem(STEPS, 8, LANES), vmem(STEPS, 8, LANES),
        vmem(STEPS, 3, 8, LANES), vmem(STEPS, 3, 8, LANES), vmem(ORDERS, ROWS, LANES),
        vmem(ROWS * 8, LANES), vmem(ROWS * 24, LANES), vmem(8, 256),
        [vmem(n, FIRST // nrow, LANES) for n in counts],
        [vmem(n, SECOND // nrow, LANES) for n in counts],
        [vmem(STEPS - 1, n, 8, LANES) for n in counts],
        [vmem(n, 8, 256) for n in counts],
        [vmem(STEPS - 1, n, 8, 256) for n in counts],
        dma(8), dma(8), dma(big_copies), dma(big_copies), dma(big_copies), dma(big_copies),
        dma(STEPS, 8), dma(STEPS, 8), dma(STEPS, small_copies), dma(STEPS, small_copies),
        dma(STEPS - 1, small_copies), dma(STEPS - 1, small_copies),
    ]
    shape = lambda *dims: jax.ShapeDtypeStruct(dims, F32)
    shapes = [
        shape(STEPS, ROWS, LANES), shape(width, 4, K), shape(STEPS, width),
        shape(ORDERS, ORDERS, K, K), shape(STEPS, ROWS, LANES),
    ]
    results = pl.pallas_call(
        functools.partial(kernel, sizes),
        out_shape=shapes,
        in_specs=[pl.BlockSpec(memory_space=pltpu.HBM)] * 4,
        out_specs=[pl.BlockSpec(memory_space=pltpu.VMEM)] * 5,
        scratch_shapes=scratch,
        compiler_params=pltpu.CompilerParams(
            collective_id=0, has_side_effects=True, vmem_limit_bytes=55_000_000
        ),
    )(
        basis_raw.reshape(R * ROWS, LANES), jnp.transpose(krylov_raw, (2, 0, 1)),
        stiffness, rotation,
    )
    new_columns, coefficients, hessenberg, gram, new_images = pl.pallas_call(
        handed_out,
        out_shape=shapes,
        in_specs=[pl.BlockSpec(memory_space=pltpu.VMEM)] * 5,
        out_specs=[pl.BlockSpec(memory_space=pltpu.HBM)] * 5,
        scratch_shapes=[pltpu.SemaphoreType.DMA((5,))],
        compiler_params=pltpu.CompilerParams(vmem_limit_bytes=2 * 1024 * 1024),
    )(*results)
    return (
        new_columns, jnp.transpose(coefficients, (1, 2, 0)), hessenberg,
        jnp.transpose(gram, (0, 2, 1, 3)), new_images,
    )


def solution(mesh):
    cores = 2
    columns = mesh.devices.shape[1]
    depth = 8 if columns % 8 == 0 else 2
    sizes = {
        "x": mesh.devices.shape[0] // cores, "core": cores,
        "y": columns // depth, "z": depth,
    }
    split = Mesh(mesh.devices.reshape(*(sizes[a] for a in AXES)), AXES)
    return jax.shard_map(
        functools.partial(local, sizes),
        mesh=split,
        in_specs=(P(None, ROW, COL), P(), P(ROW, COL), P(ROW, COL)),
        out_specs=(P(None, ROW, COL), P(), P(), P(), P(None, ROW, COL)),
        check_vma=False,
    )
```

```python
import functools
import itertools

import jax
import jax.numpy as jnp
from jax import lax
from jax.experimental import pallas as pl
from jax.experimental.pallas import tpu as pltpu
from jax.sharding import Mesh
from jax.sharding import PartitionSpec as P

K = 40
STEPS = 3
R = 37
KRYLOV = 34
ORDERS = 5
FIELDS = ORDERS * K
COUPLING = 0.2
EPSILON = 1e-06
GRAM_SHIFT = 0.05
HIGHEST = lax.Precision.HIGHEST
AXES = ("x", "core", "y", "z")
ROW = ("x", "core")
COL = ("y", "z")
STAGES = (("x", "core"), ("y",), ("z",))
ROWS = 48
LANES = 128
GHOST = 4
PADDED = 208
GROUP = 8
FIRST = 128
SECOND = 192
CENTRE = pl.ds(GHOST * LANES, ROWS * LANES)
F32 = jnp.float32


def dot(a, b, ca, cb):
    return lax.dot_general(
        a, b, (((ca,), (cb,)), ((), ())), precision=HIGHEST, preferred_element_type=F32
    )


def dot3(a, b, ca, cb):
    return lax.dot_general(
        a, b, (((ca,), (cb,)), ((), ())), precision=lax.Precision.HIGH, preferred_element_type=F32
    )


def iota(shape, dim):
    return lax.broadcasted_iota(jnp.int32, shape, dim)


def offsets(sizes, axes):
    ranges = [range(sizes[a]) for a in axes]
    return [o for o in itertools.product(*ranges) if any(o)]


def place(sizes, axes):
    index = 0
    for a in axes:
        index = index * sizes[a] + lax.axis_index(a)
    return index


def peer_of(sizes, axes, off):
    return {a: lax.rem(lax.axis_index(a) + o, sizes[a]) for a, o in zip(axes, off)}


def linear(sizes, axes, coords):
    index = 0
    for a in axes:
        index = index * sizes[a] + coords[a]
    return index


def near(sizes, drow, dcol):
    rows = sizes["x"] * sizes["core"]
    cols = sizes["y"] * sizes["z"]
    r = lax.rem(place(sizes, ROW) + drow + rows, rows)
    c = lax.rem(place(sizes, COL) + dcol + cols, cols)
    return {
        "x": r // sizes["core"],
        "core": lax.rem(r, sizes["core"]),
        "y": c // sizes["z"],
        "z": lax.rem(c, sizes["z"]),
    }


def full(coords):
    return tuple(coords.get(a, lax.axis_index(a)) for a in AXES)


SIDES = [(-1, 0), (1, 0), (0, -1), (0, 1), (-1, -1), (-1, 1), (1, -1), (1, 1)]


def forward_inverse(a, count, block=4):
    sub = iota((K, LANES), 0)
    lane = iota((K, LANES), 1)
    for first in range(0, count, block):
        pivots = range(first, min(first + block, count))
        cols = [jnp.broadcast_to(a[:, j : j + 1], (K, LANES)) for j in pivots]
        rows = [a[j : j + 1, :] for j in pivots]
        for p, j in enumerate(pivots):
            inverse = 1.0 / cols[p][j : j + 1, :]
            factor = jnp.where(sub > j, cols[p] * inverse, 0.0)
            for q in range(p + 1, len(pivots)):
                cols[q] = cols[q] - factor * cols[q][j : j + 1, :]
                rows[q] = rows[q] - factor[pivots[q] : pivots[q] + 1, :] * rows[p]
            a = a - factor * rows[p]
    diag = jnp.sum(jnp.where(lane == sub, a, 0.0), axis=1, keepdims=True)
    scaled = a * (1.0 / jnp.sqrt(diag))
    return jnp.where(lane < K, pltpu.roll(scaled, 64, 1), 0.0)


def augmented(a, shift, count):
    sub = iota((K, LANES), 0)
    lane = iota((K, LANES), 1)
    a = jnp.where((lane < count) & (sub < count), a, 0.0)
    a = a + jnp.where((lane == sub) & (sub < count), shift, 0.0)
    return a + jnp.where(((lane == sub) & (sub >= count)) | (lane == sub + 64), 1.0, 0.0)


def kernel(
    sizes, x_hbm, small_ref,
    newc_ref, coef_ref, hess_ref, gram_ref, newi_ref,
    x_ref, in_sem,
    X, SD, CF, PL, PR, RRB, RLB, AHL, ACC, AC0, BIG, FULL, BIG2, FULL2, GS, GC, LB, GB0, CB, MT, HS,
    U0, PK, HT, HB, KRB, KLB, VB, VW, UV, DN,
    slots_big, slots_two, slots_small, slots_last, slots_late, slots_early,
    hsend, hrecv, bsend, brecv, csend, crecv, usend, urecv, ssend, srecv, lsend, lrecv, esend, erecv,
):
    nrow = sizes["x"] * sizes["core"]
    ncol = sizes["y"] * sizes["z"]
    my_row = place(sizes, ROW)
    my_col = place(sizes, COL)
    grid_rows = nrow * ROWS
    inverse_total = 1.0 / (grid_rows * ncol * LANES)
    stage_offsets = [offsets(sizes, axes) for axes in STAGES]
    pending = []

    load = pltpu.make_async_copy(x_hbm, x_ref, in_sem.at[0])
    load.start()

    barrier = pltpu.get_barrier_semaphore()
    count = 0
    for axes, offs in zip(STAGES, stage_offsets):
        for off in offs:
            pl.semaphore_signal(
                barrier, inc=1, device_id=full(peer_of(sizes, axes, off)),
                device_id_type=pl.DeviceIdType.MESH,
            )
            count += 1
    for side in SIDES:
        pl.semaphore_signal(
            barrier, inc=1, device_id=full(near(sizes, *side)),
            device_id_type=pl.DeviceIdType.MESH,
        )
        count += 1

    def send(src, dst, ssem, rsem, coords):
        copy = pltpu.make_async_remote_copy(
            src_ref=src, dst_ref=dst, send_sem=ssem, recv_sem=rsem,
            device_id=full(coords), device_id_type=pl.DeviceIdType.MESH,
        )
        copy.start()
        pending.append(copy)
        return copy

    def load_rows(i, carry):
        for k in range(4):
            r = 4 * i + k
            at = pl.multiple_of((r + GHOST) * K, 8)
            X[0][pl.ds(at, R), :] = x_ref[pl.ds(r, R, stride=ROWS), :]
            X[0][pl.ds(at + R, 1), :] = small_ref[pl.ds(r, 1), :]
            X[0][pl.ds(at + R + 1, 1), :] = small_ref[pl.ds(ROWS + r, 1), :]
            X[0][pl.ds(at + R + 2, 1), :] = jnp.zeros((1, LANES), F32)
        return carry

    load.wait()
    lax.fori_loop(0, ROWS // 4, load_rows, 0)
    lane_k = iota((K, LANES), 1)

    def line(rho):
        return pl.ds(pl.multiple_of(rho * K, 8), K)

    def pack(base, n, q):
        def body(b, carry):
            left, right = carry
            for k in range(8):
                i = 8 * b + k
                row = X[0][line(base + i), :]
                here = (lane_k >= 4 * i) & (lane_k < 4 * i + 4)
                left = jnp.where(here, pltpu.roll(row, 4 * i, 1), left)
                right = jnp.where(here, pltpu.roll(row, lax.rem(4 * i + 4, LANES), 1), right)
            return left, right

        zero = jnp.zeros((K, LANES), F32)
        left, right = lax.fori_loop(0, n // 8, body, (zero, zero))
        PL[q, :, :] = left
        PR[q, :, :] = right

    pack(GHOST, 32, 0)
    pack(GHOST + 32, 16, 1)
    pl.semaphore_wait(barrier, count)

    halo = [
        send(X[0].at[pl.ds(GHOST * K, GHOST * K)], X[0].at[pl.ds((GHOST + ROWS) * K, GHOST * K)], hsend.at[0], hrecv.at[0], near(sizes, -1, 0)),
        send(X[0].at[pl.ds(ROWS * K, GHOST * K)], X[0].at[pl.ds(0, GHOST * K)], hsend.at[1], hrecv.at[1], near(sizes, 1, 0)),
        send(PL, RRB.at[pl.ds(1, 2)], hsend.at[2], hrecv.at[2], near(sizes, 0, -1)),
        send(PR, RLB.at[pl.ds(1, 2)], hsend.at[3], hrecv.at[3], near(sizes, 0, 1)),
        send(PL.at[0], RRB.at[3], hsend.at[4], hrecv.at[4], near(sizes, -1, -1)),
        send(PR.at[0], RLB.at[3], hsend.at[5], hrecv.at[5], near(sizes, -1, 1)),
        send(PL.at[1], RRB.at[0], hsend.at[6], hrecv.at[6], near(sizes, 1, -1)),
        send(PR.at[1], RLB.at[0], hsend.at[7], hrecv.at[7], near(sizes, 1, 1)),
    ]

    class Sum:
        def __init__(self, boxes, send_sems, recv_sems):
            self.boxes, self.send_sems, self.recv_sems, self.sem = boxes, send_sems, recv_sems, 0

        def start(self, stage, value):
            me = place(sizes, STAGES[stage])
            box = self.boxes[stage]
            box[me] = value
            self.copies = []
            for off in stage_offsets[stage]:
                to = peer_of(sizes, STAGES[stage], off)
                sems = self.send_sems.at[self.sem], self.recv_sems.at[self.sem]
                self.copies.append(send(box.at[me], box.at[me], *sems, to))
                self.sem += 1

        def finish(self, stage):
            for copy in self.copies:
                copy.wait_recv()
            box = self.boxes[stage]
            total = box[0]
            for i in range(1, len(stage_offsets[stage]) + 1):
                total = total + box[i]
            return total

    early = Sum(slots_early, esend, erecv)
    raw_lines = jnp.concatenate([X[0][line(r + GHOST), :] for r in range(ROWS)], axis=1)
    raw_part = jnp.concatenate([dot3(raw_lines, raw_lines, 1, 1), jnp.zeros((K, LANES - K), F32)], axis=1)
    early.start(0, raw_part)

    blank_half = jnp.zeros((KRYLOV, LANES), F32)
    pt = jnp.zeros((KRYLOV, 256), F32)
    for j in range(4):
        v = small_ref[pl.ds(2 * ROWS + j, KRYLOV, stride=4), :]
        v = jnp.concatenate([v, blank_half], axis=1)
        pt = pt + (pltpu.roll(v, j * K, 1) if j else v)
    pt = jnp.concatenate([pt, jnp.zeros((K - KRYLOV, 256), F32)], axis=0)
    kgram = dot(pt, pt, 1, 1)
    kgram = jnp.concatenate([kgram, jnp.zeros((K, LANES - K), F32)], axis=1)
    kinv = forward_inverse(augmented(kgram, 0.0, KRYLOV), KRYLOV)
    MT[...] = jnp.zeros((LANES, 256), F32)
    MT[pl.ds(0, K), :] = dot(kinv[:, 0:K], pt, 1, 0)
    HS[...] = jnp.zeros((LANES, LANES), F32)
    LB[...] = jnp.zeros((256, 256), F32)
    GS[...] = jnp.zeros((256, 256), F32)
    BIG[...] = jnp.zeros((FIRST, LANES), F32)
    BIG2[...] = jnp.zeros((SECOND, LANES), F32)
    CF[...] = jnp.zeros((10, 64, LANES), F32)
    AHL[pl.ds(PADDED, 256 - PADDED), :] = jnp.zeros((256 - PADDED, (ROWS + 8) * LANES), jnp.bfloat16)
    VW[...] = jnp.zeros((ROWS * 8, LANES), F32)
    UV[...] = jnp.zeros((ROWS * 24, LANES), F32)

    for copy in halo:
        copy.wait_recv()
    for copy in halo[:2]:
        copy.wait_send()
        pending.remove(copy)

    lane1 = iota((1, LANES), 1)
    has_right = (my_col < ncol - 1).astype(F32)
    has_left = (my_col > 0).astype(F32)
    side_mask = jnp.where(lane1 < 4, has_right, jnp.where(lane1 >= 124, has_left, 0.0))
    sub_k = iota((K, LANES), 0)

    def order_zero(base, n, part, first):
        def body(b, carry):
            stores = []
            for k in range(4):
                i = 4 * b + k
                rho = base + i
                g = my_row * ROWS + rho - GHOST
                row_mask = ((g >= 0) & (g < grid_rows)).astype(F32)
                at = 4 * (first + i)
                right = pltpu.roll(RRB[part, :, :], lax.rem(LANES - at, LANES), 1)
                left = pltpu.roll(RLB[part, :, :], lax.rem(2 * LANES - 4 - at, LANES), 1)
                ms = side_mask * row_mask
                side = jnp.where(lane_k < 4, right, left) * ms
                mid = X[0][line(rho), :] * row_mask
                mc = jnp.ones((1, LANES), F32) * row_mask
                stores.append((rho, (mid, mc), (side, ms)))
            for rho, mid, side in stores:
                for half, (v, m) in enumerate((mid, side)):
                    d = v[R : R + 1, :]
                    s = v[R + 1 : R + 2, :]
                    CF[5 * half, pl.ds(rho + 4, 1), :] = 2.0 * d * m
                    CF[5 * half + 1, pl.ds(rho + 4, 1), :] = (2.0 * COUPLING) * m
                    CF[5 * half + 2, pl.ds(rho + 4, 1), :] = 2.0 * (s - COUPLING) * m
                    CF[5 * half + 3, pl.ds(rho + 4, 1), :] = 2.0 * (s + COUPLING) * m
                    CF[5 * half + 4, pl.ds(rho + 4, 1), :] = m
                X[0][line(rho), :] = jnp.where(sub_k < R, mid[0], 0.0)
                SD[0][line(rho), :] = jnp.where(sub_k < R, side[0], 0.0)
            return carry

        lax.fori_loop(0, n // 4, body, 0)

    order_zero(0, 4, 0, 12)
    order_zero(4, 32, 1, 0)
    order_zero(36, 16, 2, 0)
    order_zero(52, 4, 3, 0)

    def split_tile(t, at, a):
        hi = a.astype(jnp.bfloat16)
        AHL[pl.ds(16 * t, 16), at] = hi
        AHL[pl.ds(256 + 16 * t, 16), at] = (a - hi.astype(F32)).astype(jnp.bfloat16)

    def images(m, n):
        def body(b, carry):
            mids, sides = [], []
            for k in range(n):
                rho = m + n * b + k
                c = X[m - 1][line(rho), :]
                s = SD[m - 1][line(rho), :]
                cu = X[m - 1][line(rho - 1), :] + X[m - 1][line(rho + 1), :]
                cl, sl = pltpu.roll(c, 1, 1), pltpu.roll(s, 1, 1)
                cr, sr = pltpu.roll(c, 127, 1), pltpu.roll(s, 127, 1)

                def row(kind):
                    return CF[kind, pl.ds(rho + 4, 1), :]

                left = jnp.where(lane_k == 0, sl, cl)
                right = jnp.where(lane_k == 127, sr, cr)
                new = row(0) * c - row(1) * cu + row(2) * right - row(3) * left
                mids.append(0.5 * new if m == 1 else new - X[m - 2][line(rho), :])
                if m < 4:
                    su = SD[m - 1][line(rho - 1), :] + SD[m - 1][line(rho + 1), :]
                    left = jnp.where(lane_k == 0, cl, sl)
                    right = jnp.where(lane_k == 127, cr, sr)
                    side = row(5) * s - row(6) * su + row(7) * right - row(8) * left
                    sides.append(0.5 * side if m == 1 else side - SD[m - 2][line(rho), :])
            for k in range(n):
                rho = m + n * b + k
                X[m][line(rho), :] = mids[k]
                if m < 4:
                    SD[m][line(rho), :] = sides[k]
                at = pl.ds(pl.multiple_of(rho * LANES, LANES), LANES)
                new = mids[k]
                if m in (1, 3):
                    ends = jnp.concatenate([X[m - 1][pl.ds(pl.multiple_of(rho * K + 32, 8), 8), :], new[0:8, :]], axis=0)
                    split_tile(5 * (m - 1) // 2 + 2, at, ends)
                    split_tile(5 * (m - 1) // 2 + 3, at, new[8:24, :])
                    split_tile(5 * (m - 1) // 2 + 4, at, new[24:40, :])
                else:
                    split_tile(5 * m // 2, at, new[0:16, :])
                    split_tile(5 * m // 2 + 1, at, new[16:32, :])
                if m == 4:
                    split_tile(12, at, jnp.concatenate([new[32:40, :], jnp.zeros((8, LANES), F32)], axis=0))
                if m == 1:
                    old = X[0][pl.ds(pl.multiple_of(rho * K, 8), 32), :]
                    split_tile(0, at, old[0:16, :])
                    split_tile(1, at, old[16:32, :])
            return carry

        lax.fori_loop(0, (ROWS + 8 - 2 * m) // n, body, 0)

    for m, n in zip(range(1, ORDERS), (3, 4, 5, 6)):
        images(m, n)
        if m == 2:
            early.start(1, early.finish(0))
        if m == 4:
            early.start(2, early.finish(1))


    def bdot(a, b):
        return lax.dot_general(a, b, (((1,), (1,)), ((), ())), preferred_element_type=F32)

    first_rows = jnp.concatenate([AHL[pl.ds(0, 48), CENTRE], AHL[pl.ds(256, 48), CENTRE]], axis=0)
    AC0[:, pl.ds(0, 256 + PADDED)] = bdot(first_rows, AHL[:, CENTRE])
    top = AC0[pl.ds(0, K), pl.ds(0, 256)] + AC0[pl.ds(48, K), pl.ds(0, 256)] + AC0[pl.ds(0, K), pl.ds(256, 256)]
    lane_w = iota((K, 256), 1)
    top = jnp.where(lane_w < FIELDS, top, 0.0)
    BIG[pl.ds(0, K), :] = top[:, 0:LANES]
    BIG[pl.ds(K, K), :] = top[:, LANES:]

    class Reduction:
        def __init__(self, big, whole, boxes, total_rows, send_sems, recv_sems):
            self.big, self.whole, self.boxes = big, whole, boxes
            self.chunk = total_rows // nrow
            self.send_sems, self.recv_sems, self.sem = send_sems, recv_sems, 0
            self.own = pl.ds(pl.multiple_of(my_row * self.chunk, 8), self.chunk)
            self.copies = []

        def emit(self, src, dst, to):
            self.copies.append(send(src, dst, self.send_sems.at[self.sem], self.recv_sems.at[self.sem], to))
            self.sem += 1

        def arrived(self):
            for copy in self.copies:
                copy.wait_recv()
            self.copies = []

        def start(self, stage):
            me = place(sizes, STAGES[stage])
            box = self.boxes[stage]
            if stage == 0:
                box[me] = self.big[self.own, :]
            for off in stage_offsets[stage]:
                to = peer_of(sizes, STAGES[stage], off)
                if stage == 0:
                    at = pl.multiple_of(linear(sizes, ROW, to) * self.chunk, 8)
                    self.emit(self.big.at[pl.ds(at, self.chunk)], box.at[me], to)
                else:
                    self.emit(box.at[me], box.at[me], to)

        def finish(self, stage):
            self.arrived()
            box = self.boxes[stage]
            total = box[0]
            for i in range(1, len(stage_offsets[stage]) + 1):
                total = total + box[i]
            if stage + 1 < len(STAGES):
                self.boxes[stage + 1][place(sizes, STAGES[stage + 1])] = total
            else:
                self.whole[self.own, :] = total * inverse_total

        def gather(self):
            for off in stage_offsets[0]:
                self.emit(self.whole.at[self.own], self.whole.at[self.own], peer_of(sizes, ROW, off))

    one = Reduction(BIG, FULL, slots_big, FIRST, bsend, brecv)
    two = Reduction(BIG2, FULL2, slots_two, SECOND, csend, crecv)
    one.start(0)

    ACC[...] = jnp.zeros((256 + PADDED, 256), F32)

    def gram_rest(g, carry):
        at = pl.ds(pl.multiple_of((GHOST + GROUP * g) * LANES, LANES), GROUP * LANES)
        ACC[:, pl.ds(0, PADDED)] += bdot(AHL[:, at], AHL[pl.ds(0, PADDED), at])
        return carry

    lax.fori_loop(0, ROWS // GROUP, gram_rest, 0)
    cross = jnp.concatenate([ACC[pl.ds(256, PADDED), :], jnp.zeros((256 - PADDED, 256), F32)], axis=0)
    ACC[pl.ds(0, PADDED), :] = ACC[pl.ds(0, PADDED), :] + cross[0:PADDED, :] + jnp.transpose(cross)[0:PADDED, :]

    def strip(a, shift):
        return pltpu.roll(ACC[pl.ds(a * K, K), :], shift % 256, 1)[:, 0:LANES]

    lane_n = iota((K, LANES), 1)
    BIG2[pl.ds(0, K), :] = strip(1, -40)
    BIG2[pl.ds(K, K), :] = strip(2, -80)
    BIG2[pl.ds(2 * K, K), :] = jnp.where(lane_n >= 80, strip(4, -80), strip(3, -120))
    BIG2[pl.ds(3 * K, K), :] = strip(1, -160)

    raw_gram = early.finish(2) * inverse_total
    for stage in range(3):
        one.finish(stage)
        if stage < 2:
            one.start(stage + 1)
        if stage == 0:
            finv = forward_inverse(augmented(raw_gram, GRAM_SHIFT, R), R)
            finv = jnp.where(sub_k < R, finv, 0.0)
            finv_wide = jnp.concatenate([finv, jnp.zeros((K, LANES), F32)], axis=1)
            for a in range(ORDERS):
                LB[pl.ds(a * K, K), :] = pltpu.roll(finv_wide, a * K, 1) if a else finv_wide
    one.gather()
    one.arrived()
    two.start(0)

    GS[pl.ds(0, K), pl.ds(0, LANES)] = FULL[pl.ds(0, K), :]
    GS[pl.ds(0, K), pl.ds(LANES, LANES)] = FULL[pl.ds(K, K), :]
    GC[...] = jnp.transpose(GS[pl.ds(0, LANES), :])

    def assemble_rest():
        def wide(a):
            v = FULL2[pl.ds(a * K, K), :]
            return jnp.concatenate([v, jnp.zeros((K, LANES), F32)], axis=1)

        def moved(v, shift, lo, hi):
            return jnp.where((lane_w >= lo) & (lane_w < hi), pltpu.roll(v, shift, 1), 0.0)

        GS[pl.ds(K, K), :] = moved(wide(0), 40, 40, 160) + moved(wide(3), 160, 160, 200)
        GS[pl.ds(2 * K, K), :] = moved(wide(1), 80, 80, 200)
        GS[pl.ds(3 * K, K), :] = moved(wide(2), 120, 120, 200)
        GS[pl.ds(4 * K, K), :] = moved(wide(2), 80, 160, 200)
        mirrored = jnp.transpose(GS[...])
        for a in range(1, ORDERS):
            GS[pl.ds(a * K, K), :] = jnp.where(
                lane_w >= a * K, GS[pl.ds(a * K, K), :], mirrored[a * K : (a + 1) * K, :]
            )

    square = (iota((LANES, LANES), 0) < K) & (iota((LANES, LANES), 1) < K)
    small = jnp.where(square, LB[pl.ds(0, LANES), pl.ds(0, LANES)], 0.0)
    GB0[...] = dot3(dot3(LB[...], GC[...], 1, 0), small, 1, 1)

    lane_r = iota((1, 256), 1)
    lane8 = iota((8, 256), 1)
    late = [Sum([b.at[s] for b in slots_late], lsend.at[s], lrecv.at[s]) for s in range(STEPS - 1)]

    def paired():
        v = jnp.concatenate([VW[pl.ds(8 * k, 8), :] for k in range(ROWS)], axis=1)
        v_hi = v.astype(jnp.bfloat16).astype(F32)
        return jnp.concatenate([v_hi, v - v_hi], axis=0).astype(jnp.bfloat16)

    def with_old(v):
        old = bdot(v, AHL[:, CENTRE])
        old = old[0:8, :] + old[8:16, :]
        d = old[:, 0:256] + jnp.concatenate([old[:, 256:], jnp.zeros((8, 256 - PADDED), F32)], axis=1)
        return jnp.where(lane8 < FIELDS, d, 0.0)

    def with_first(v):
        first = jnp.concatenate([AHL[pl.ds(0, 48), CENTRE], AHL[pl.ds(256, 48), CENTRE]], axis=0)
        part = bdot(v, first)
        return part[0:8, 0:K] + part[8:16, 0:K] + part[0:8, 48 : 48 + K]

    def with_new(v):
        w = jnp.concatenate([UV[pl.ds(24 * k, 24), :] for k in range(ROWS)], axis=1)
        w_hi = w.astype(jnp.bfloat16).astype(F32)
        w = jnp.concatenate([w_hi, w - w_hi], axis=0).astype(jnp.bfloat16)
        new = bdot(v, w)
        new = new[0:8, :] + new[8:16, :]
        return new[:, 0:24] + new[:, 24:48]

    def keep_late(s, total):
        rows = pl.ds(FIELDS + 8 * s, 8)
        GS[rows, :] = GS[rows, :] + total * inverse_total
    sub8 = iota((8, 256), 0)
    tile_mask = iota((64, LANES), 1)

    for s in range(STEPS):
        column = KRYLOV + s
        r = R + s
        latest = MT[pl.ds(column - 1, 1), :]

        def moved(shift):
            return pltpu.roll(latest, shift % 256, 1)

        cw = jnp.where(lane_r < K, 0.5 * moved(-80), -0.5 * moved(40))
        cw = jnp.where(lane_r < FIELDS, cw, 0.0)
        cw = jnp.broadcast_to(cw, (8, 256))
        h1 = dot3(cw, GB0[...], 1, 0)
        h = 2.0 * h1 - dot3(h1, GB0[pl.ds(0, LANES), :], 1, 0)
        h_wide = jnp.concatenate([h, jnp.zeros((8, LANES), F32)], axis=1)
        raw = dot3(cw - h_wide, LB[...], 1, 0)
        raw_col = jnp.transpose(raw)[0 : FIELDS + 24, 0:1]
        CB[...] = jnp.broadcast_to(raw_col, (FIELDS + 24, LANES))

        def combine(i, carry):
            for k in range(8):
                rho = 8 * i + k + GHOST
                value = CB[pl.ds(0, K), :] * X[0][line(rho), :]
                for m in range(1, ORDERS):
                    value = value + CB[pl.ds(m * K, K), :] * X[m][line(rho), :]
                value = jnp.sum(value, axis=0, keepdims=True)
                if s:
                    at = pl.multiple_of(24 * (8 * i + k), 8)
                    older = CB[pl.ds(FIELDS, 16), :] * UV[pl.ds(at, 16), :]
                    value = value + jnp.sum(older, axis=0, keepdims=True)
                U0[s, pl.ds(8 * i + k, 1), :] = value
            return carry

        lax.fori_loop(0, ROWS // 8, combine, 0)

        lane_t = iota((8, LANES), 1)
        sub_t = iota((8, LANES), 0)
        packed = jnp.zeros((8, LANES), F32)
        for q in range(6):
            tile = U0[s, pl.ds(8 * q, 8), :]
            packed = jnp.where(
                (lane_t >= 4 * q) & (lane_t < 4 * q + 4), pltpu.roll(tile, 4 * q, 1) if q else tile, packed
            )
            packed = jnp.where(
                (lane_t >= 64 + 4 * q) & (lane_t < 68 + 4 * q), pltpu.roll(tile, 68 + 4 * q, 1), packed
            )
        PK[s, :, :] = packed
        edge = [
            send(U0.at[s, pl.ds(0, 8)], HB.at[s], usend.at[s, 0], urecv.at[s, 0], near(sizes, -1, 0)),
            send(U0.at[s, pl.ds(40, 8)], HT.at[s], usend.at[s, 1], urecv.at[s, 1], near(sizes, 1, 0)),
            send(PK.at[s], KRB.at[s, 1], usend.at[s, 2], urecv.at[s, 2], near(sizes, 0, -1)),
            send(PK.at[s], KLB.at[s, 1], usend.at[s, 3], urecv.at[s, 3], near(sizes, 0, 1)),
            send(PK.at[s], KRB.at[s, 2], usend.at[s, 4], urecv.at[s, 4], near(sizes, -1, -1)),
            send(PK.at[s], KLB.at[s, 2], usend.at[s, 5], urecv.at[s, 5], near(sizes, -1, 1)),
            send(PK.at[s], KRB.at[s, 0], usend.at[s, 6], urecv.at[s, 6], near(sizes, 1, -1)),
            send(PK.at[s], KLB.at[s, 0], usend.at[s, 7], urecv.at[s, 7], near(sizes, 1, 1)),
        ]

        if s + 1 < STEPS:
            VW[pl.ds(0, ROWS, stride=8), :] = U0[s]
            d_old = with_old(paired())
        h_row = h_wide[0:1, :]
        e = jnp.where(lane_r < K, moved(-40), 0.5 * (moved(40) + moved(-40)))
        e = jnp.where(lane_r < 3 * K, e, pltpu.roll(h_row, 3 * K, 1))
        e = jnp.where(lane_r < 4 * K, e, 0.0)
        mt = MT[pl.ds(0, K), :]
        g1 = jnp.sum(mt * e, axis=1, keepdims=True)
        e1 = e - jnp.sum(mt * g1, axis=0, keepdims=True)
        g2 = jnp.sum(mt * e1, axis=1, keepdims=True)
        e2 = e1 - jnp.sum(mt * g2, axis=0, keepdims=True)
        e2_square = jnp.sum(e2 * e2, axis=1, keepdims=True)

        if s == 0:
            two.finish(0)
            two.start(1)
        if s == 1:
            two.finish(2)
            two.gather()
            late[0].start(1, late[0].finish(0))
        if s == 2:
            keep_late(0, late[0].finish(2))
            late[1].start(1, late[1].finish(0))
        for copy in edge:
            copy.wait_recv()

        mids = jnp.concatenate([HT[s], U0[s], HB[s]], axis=0) * CF[4]
        sides = []
        for j in range(8):
            part = 0 if j == 0 else (2 if j == 7 else 1)
            q = 5 if j == 0 else (0 if j == 7 else j - 1)
            rt = KRB[s, part]
            lf = pltpu.roll(KLB[s, part], 60 - 4 * q, 1)
            rt = pltpu.roll(rt, LANES - 4 * q, 1) if q else rt
            sides.append(jnp.where(lane_t < 4, rt, lf))
        sds = jnp.concatenate(sides, axis=0) * CF[9]

        def twice_s(c, v):
            cl, sl = pltpu.roll(c, 1, 1), pltpu.roll(v, 1, 1)
            cr, sr = pltpu.roll(c, 127, 1), pltpu.roll(v, 127, 1)
            cu = pltpu.roll(c, 1, 0) + pltpu.roll(c, 63, 0)
            su = pltpu.roll(v, 1, 0) + pltpu.roll(v, 63, 0)
            lo, hi = tile_mask == 0, tile_mask == 127
            mid = CF[0] * c - CF[1] * cu + CF[2] * jnp.where(hi, sr, cr) - CF[3] * jnp.where(lo, sl, cl)
            side = CF[5] * v - CF[6] * su + CF[7] * jnp.where(hi, cr, sr) - CF[8] * jnp.where(lo, cl, sl)
            return mid, side

        before = (mids, sds)
        now = twice_s(*before)
        now = (0.5 * now[0], 0.5 * now[1])
        orders = [before[0], now[0]]
        for m in range(2, ORDERS):
            nxt = twice_s(*now)
            before, now = now, (nxt[0] - before[0], nxt[1] - before[1])
            orders.append(now[0])
        for m in range(ORDERS):
            VB[m, :, :] = orders[m][8:56, :]
            VW[pl.ds(m, ROWS, stride=8), :] = orders[m][8:56, :]
            UV[pl.ds(8 * s + m, ROWS, stride=24), :] = orders[m][8:56, :]

        v = paired()
        if s + 1 < STEPS:
            total_sum = Sum([b.at[s] for b in slots_small], ssend.at[s], srecv.at[s])
            DN[...] = jnp.zeros((8, 256), F32)
            DN[:, pl.ds(0, K)] = with_first(v)
            DN[:, pl.ds(72, 24)] = with_new(v)
            low = pltpu.roll(DN[:, pl.ds(0, LANES)], 1, 0)
            wide_row = d_old[0:1, :]
            packed_new = jnp.where((lane_t >= 72) & (lane_t < 96), DN[0:1, pl.ds(0, LANES)], wide_row[:, LANES:])
            value = jnp.where(sub_t == 0, wide_row[:, 0:LANES], jnp.where(sub_t == 1, packed_new, low))
        else:
            total_sum = Sum(slots_last, ssend.at[s], srecv.at[s])
            DN[...] = with_old(v)
            DN[:, pl.ds(FIELDS, 24)] = with_new(v)
            value = DN[...]
        for stage in range(3):
            total_sum.start(stage, value)
            if stage == 0 and s + 1 < STEPS:
                rest = jnp.where((lane8 >= K) & (sub8 >= 1) & (sub8 < ORDERS), with_old(v), 0.0)
            if s == 0 and stage == 2:
                two.finish(1)
                two.start(2)
                late[0].start(0, rest)
            if s == 1 and stage == 0:
                two.arrived()
                assemble_rest()
            if s == 1 and stage == 2:
                late[0].start(2, late[0].finish(1))
                late[1].start(0, rest)
            if s == 2 and stage == 2:
                late[1].start(2, late[1].finish(1))
            value = total_sum.finish(stage)
        if s + 1 < STEPS:
            up = pltpu.roll(value, 7, 0)
            mid = (lane_t >= 72) & (lane_t < 96)
            left = jnp.where(sub_t == 0, value, jnp.where(lane_t < K, up, 0.0))
            right = jnp.where((sub_t == 0) | mid, up, 0.0)
            value = jnp.concatenate([left, right], axis=1)
        d = value * inverse_total
        d = jnp.where(sub8 < ORDERS, d, 0.0)

        nn = jnp.sum(jnp.where(lane_r == FIELDS + 8 * s, d[0:1, :], 0.0), axis=1, keepdims=True)
        beta = jnp.sqrt(nn + EPSILON)
        ib = 1.0 / beta
        eta = jnp.sqrt(e2_square + beta * beta + EPSILON)
        MT[pl.ds(column, 1), :] = (e2 + jnp.where(lane_r == 3 * K + r, beta, 0.0)) / eta
        sub_col = iota((K, 1), 0)
        g = g1 + g2 + jnp.where(sub_col == column, eta, 0.0)
        lane_h = iota((K, LANES), 1)
        HS[pl.ds(0, K), :] = jnp.where(lane_h == s, g, HS[pl.ds(0, K), :])
        newc_ref[s, :, :] = VB[0] * ib
        newi_ref[s, :, :] = VB[4] * ib
        for m in range(ORDERS):
            at = m * K + r
            LB[pl.ds(at, 1), :] = jnp.where(lane_r == FIELDS + 8 * s + m, ib, 0.0)
        GS[pl.ds(FIELDS + 8 * s, 8), :] = d
        if s + 1 < STEPS:
            db = dot3(d, LB[...], 1, 1) * ib
            dcol = jnp.transpose(db)[:, 0:1]
            lane_g = iota((256, LANES), 1)
            GB0[...] = jnp.where(lane_g == r, dcol, GB0[...])
            for m in range(ORDERS):
                GB0[pl.ds(m * K + r, 1), :] = jnp.where(lane1 < K, db[m : m + 1, 0:LANES], 0.0)

    keep_late(1, late[1].finish(2))
    mirrored = jnp.transpose(GS[...])
    def age(index):
        return sum(((index >= FIELDS + 8 * t).astype(jnp.int32) for t in range(1, STEPS)), (index >= FIELDS).astype(jnp.int32))

    whole_row = age(iota((256, 256), 0))
    whole_col = age(iota((256, 256), 1))
    GS[...] = jnp.where(whole_row >= whole_col, GS[...], mirrored)
    gram = dot3(dot3(LB[...], GS[...], 1, 0), LB[...], 1, 1)
    for a in range(ORDERS):
        for b in range(ORDERS):
            gram_ref[a, b, :, :] = gram[a * K : (a + 1) * K, b * K : (b + 1) * K]
    for j in range(4):
        coef_ref[:, j, :] = MT[pl.ds(0, KRYLOV + STEPS), pl.ds(j * K, K)]
    hess_ref[...] = jnp.transpose(HS[...])[0:STEPS, 0 : KRYLOV + STEPS]

    for copy in pending:
        copy.wait_send()


def handed_out(*refs):
    sources, targets, sems = refs[:5], refs[5:10], refs[10]
    copies = [pltpu.make_async_copy(a, b, sems.at[i]) for i, (a, b) in enumerate(zip(sources, targets))]
    for copy in copies:
        copy.start()
    for copy in copies:
        copy.wait()


def local(sizes, basis_raw, krylov_raw, stiffness, rotation):
    width = KRYLOV + STEPS
    nrow = sizes["x"] * sizes["core"]
    counts = []
    for axes in STAGES:
        n = 1
        for a in axes:
            n *= sizes[a]
        counts.append(n)
    big_copies = sum(n - 1 for n in counts) + counts[0] - 1
    small_copies = sum(n - 1 for n in counts)
    vmem = lambda *shape: pltpu.VMEM(shape, F32)
    half = lambda *shape: pltpu.VMEM(shape, jnp.bfloat16)
    dma = lambda *shape: pltpu.SemaphoreType.DMA(shape)
    scratch = [
        vmem(R * ROWS, LANES), dma(1),
        [vmem((ROWS + 8) * K, LANES) for _ in range(ORDERS)],
        [vmem((ROWS + 8) * K, LANES) for _ in range(ORDERS - 1)],
        vmem(10, 64, LANES), vmem(2, K, LANES), vmem(2, K, LANES), vmem(4, K, LANES), vmem(4, K, LANES),
        half(256 + PADDED, (ROWS + 8) * LANES), vmem(256 + PADDED, 256), vmem(96, 512),
        vmem(FIRST, LANES), vmem(FIRST, LANES), vmem(SECOND, LANES), vmem(SECOND, LANES),
        vmem(256, 256), vmem(256, LANES), vmem(256, 256),
        vmem(256, LANES), vmem(FIELDS + 24, LANES), vmem(LANES, 256), vmem(LANES, LANES),
        vmem(STEPS, ROWS, LANES), vmem(STEPS, 8, LANES), vmem(STEPS, 8, LANES), vmem(STEPS, 8, LANES),
        vmem(STEPS, 3, 8, LANES), vmem(STEPS, 3, 8, LANES), vmem(ORDERS, ROWS, LANES),
        vmem(ROWS * 8, LANES), vmem(ROWS * 24, LANES), vmem(8, 256),
        [vmem(n, FIRST // nrow, LANES) for n in counts],
        [vmem(n, SECOND // nrow, LANES) for n in counts],
        [vmem(STEPS - 1, n, 8, LANES) for n in counts],
        [vmem(n, 8, 256) for n in counts],
        [vmem(STEPS - 1, n, 8, 256) for n in counts],
        [vmem(n, K, LANES) for n in counts],
        dma(8), dma(8), dma(big_copies), dma(big_copies), dma(big_copies), dma(big_copies),
        dma(STEPS, 8), dma(STEPS, 8), dma(STEPS, small_copies), dma(STEPS, small_copies),
        dma(STEPS - 1, small_copies), dma(STEPS - 1, small_copies),
        dma(small_copies), dma(small_copies),
    ]
    shape = lambda *dims: jax.ShapeDtypeStruct(dims, F32)
    shapes = [
        shape(STEPS, ROWS, LANES), shape(width, 4, K), shape(STEPS, width),
        shape(ORDERS, ORDERS, K, K), shape(STEPS, ROWS, LANES),
    ]
    krylov_lines = jnp.transpose(krylov_raw, (2, 0, 1)).reshape(4 * KRYLOV, R)
    krylov_lines = jnp.pad(krylov_lines, ((0, 0), (0, LANES - R)))
    small = jnp.concatenate([stiffness, rotation, krylov_lines], axis=0)
    results = pl.pallas_call(
        functools.partial(kernel, sizes),
        out_shape=shapes,
        in_specs=[pl.BlockSpec(memory_space=pltpu.HBM), pl.BlockSpec(memory_space=pltpu.VMEM)],
        out_specs=[pl.BlockSpec(memory_space=pltpu.VMEM)] * 5,
        scratch_shapes=scratch,
        compiler_params=pltpu.CompilerParams(
            collective_id=0, has_side_effects=True, vmem_limit_bytes=55_000_000
        ),
    )(
        basis_raw.reshape(R * ROWS, LANES), small,
    )
    new_columns, coefficients, hessenberg, gram, new_images = pl.pallas_call(
        handed_out,
        out_shape=shapes,
        in_specs=[pl.BlockSpec(memory_space=pltpu.VMEM)] * 5,
        out_specs=[pl.BlockSpec(memory_space=pltpu.HBM)] * 5,
        scratch_shapes=[pltpu.SemaphoreType.DMA((5,))],
        compiler_params=pltpu.CompilerParams(vmem_limit_bytes=2 * 1024 * 1024),
    )(*results)
    return (
        new_columns, jnp.transpose(coefficients, (1, 2, 0)), hessenberg,
        jnp.transpose(gram, (0, 2, 1, 3)), new_images,
    )


def solution(mesh):
    cores = 2
    columns = mesh.devices.shape[1]
    depth = 8 if columns % 8 == 0 else 2
    sizes = {
        "x": mesh.devices.shape[0] // cores, "core": cores,
        "y": columns // depth, "z": depth,
    }
    split = Mesh(mesh.devices.reshape(*(sizes[a] for a in AXES)), AXES)
    return jax.shard_map(
        functools.partial(local, sizes),
        mesh=split,
        in_specs=(P(None, ROW, COL), P(), P(ROW, COL), P(ROW, COL)),
        out_specs=(P(None, ROW, COL), P(), P(), P(), P(None, ROW, COL)),
        check_vma=False,
    )
```

```python
import functools
import itertools

import jax
import jax.numpy as jnp
from jax import lax
from jax.experimental import pallas as pl
from jax.experimental.pallas import tpu as pltpu
from jax.sharding import Mesh
from jax.sharding import PartitionSpec as P

K = 40
STEPS = 3
R = 37
KRYLOV = 34
ORDERS = 5
FIELDS = ORDERS * K
COUPLING = 0.2
EPSILON = 1e-06
GRAM_SHIFT = 0.05
HIGHEST = lax.Precision.HIGHEST
AXES = ("x", "core", "y", "z")
ROW = ("x", "core")
COL = ("y", "z")
STAGES = (("x", "core"), ("y",), ("z",))
ROWS = 48
LANES = 128
GHOST = 4
PADDED = 208
GROUP = 8
FIRST = 64
SECOND = 192
CENTRE = pl.ds(GHOST * LANES, ROWS * LANES)
F32 = jnp.float32


def dot(a, b, ca, cb):
    return lax.dot_general(
        a, b, (((ca,), (cb,)), ((), ())), precision=HIGHEST, preferred_element_type=F32
    )


def dot3(a, b, ca, cb):
    return lax.dot_general(
        a, b, (((ca,), (cb,)), ((), ())), precision=lax.Precision.HIGH, preferred_element_type=F32
    )


def iota(shape, dim):
    return lax.broadcasted_iota(jnp.int32, shape, dim)


def offsets(sizes, axes):
    ranges = [range(sizes[a]) for a in axes]
    return [o for o in itertools.product(*ranges) if any(o)]


def place(sizes, axes):
    index = 0
    for a in axes:
        index = index * sizes[a] + lax.axis_index(a)
    return index


def peer_of(sizes, axes, off):
    return {a: lax.rem(lax.axis_index(a) + o, sizes[a]) for a, o in zip(axes, off)}


def linear(sizes, axes, coords):
    index = 0
    for a in axes:
        index = index * sizes[a] + coords[a]
    return index


def near(sizes, drow, dcol):
    rows = sizes["x"] * sizes["core"]
    cols = sizes["y"] * sizes["z"]
    r = lax.rem(place(sizes, ROW) + drow + rows, rows)
    c = lax.rem(place(sizes, COL) + dcol + cols, cols)
    return {
        "x": r // sizes["core"],
        "core": lax.rem(r, sizes["core"]),
        "y": c // sizes["z"],
        "z": lax.rem(c, sizes["z"]),
    }


def full(coords):
    return tuple(coords.get(a, lax.axis_index(a)) for a in AXES)


SIDES = [(-1, 0), (1, 0), (0, -1), (0, 1), (-1, -1), (-1, 1), (1, -1), (1, 1)]


def forward_inverse(a, count, block=4):
    sub = iota((K, LANES), 0)
    lane = iota((K, LANES), 1)
    for first in range(0, count, block):
        pivots = range(first, min(first + block, count))
        cols = [jnp.broadcast_to(a[:, j : j + 1], (K, LANES)) for j in pivots]
        rows = [a[j : j + 1, :] for j in pivots]
        for p, j in enumerate(pivots):
            inverse = 1.0 / cols[p][j : j + 1, :]
            factor = jnp.where(sub > j, cols[p] * inverse, 0.0)
            for q in range(p + 1, len(pivots)):
                cols[q] = cols[q] - factor * cols[q][j : j + 1, :]
                rows[q] = rows[q] - factor[pivots[q] : pivots[q] + 1, :] * rows[p]
            a = a - factor * rows[p]
    diag = jnp.sum(jnp.where(lane == sub, a, 0.0), axis=1, keepdims=True)
    scaled = a * (1.0 / jnp.sqrt(diag))
    return jnp.where(lane < K, pltpu.roll(scaled, 64, 1), 0.0)


def augmented(a, shift, count):
    sub = iota((K, LANES), 0)
    lane = iota((K, LANES), 1)
    a = jnp.where((lane < count) & (sub < count), a, 0.0)
    a = a + jnp.where((lane == sub) & (sub < count), shift, 0.0)
    return a + jnp.where(((lane == sub) & (sub >= count)) | (lane == sub + 64), 1.0, 0.0)


def kernel(
    sizes, x_hbm, small_ref,
    newc_ref, coef_ref, hess_ref, gram_ref, newi_ref,
    x_ref, in_sem,
    X, SD, CF, PL, PR, RRB, RLB, AHL, ACC, AC0, BIG, FULL, BIG2, FULL2, GS, GC, LB, GB0, CB, MT, HS,
    U0, PK, HT, HB, KRB, KLB, VB, VW, UV, DN,
    slots_big, slots_two, slots_small, slots_last, slots_late, slots_early,
    hsend, hrecv, bsend, brecv, csend, crecv, usend, urecv, ssend, srecv, lsend, lrecv, esend, erecv,
):
    nrow = sizes["x"] * sizes["core"]
    ncol = sizes["y"] * sizes["z"]
    my_row = place(sizes, ROW)
    my_col = place(sizes, COL)
    grid_rows = nrow * ROWS
    inverse_total = 1.0 / (grid_rows * ncol * LANES)
    stage_offsets = [offsets(sizes, axes) for axes in STAGES]
    pending = []

    load = pltpu.make_async_copy(x_hbm, x_ref, in_sem.at[0])
    load.start()

    barrier = pltpu.get_barrier_semaphore()
    count = 0
    for axes, offs in zip(STAGES, stage_offsets):
        for off in offs:
            pl.semaphore_signal(
                barrier, inc=1, device_id=full(peer_of(sizes, axes, off)),
                device_id_type=pl.DeviceIdType.MESH,
            )
            count += 1
    for side in SIDES:
        pl.semaphore_signal(
            barrier, inc=1, device_id=full(near(sizes, *side)),
            device_id_type=pl.DeviceIdType.MESH,
        )
        count += 1

    def send(src, dst, ssem, rsem, coords):
        copy = pltpu.make_async_remote_copy(
            src_ref=src, dst_ref=dst, send_sem=ssem, recv_sem=rsem,
            device_id=full(coords), device_id_type=pl.DeviceIdType.MESH,
        )
        copy.start()
        pending.append(copy)
        return copy

    def load_rows(i, carry):
        for k in range(4):
            r = 4 * i + k
            at = pl.multiple_of((r + GHOST) * K, 8)
            X[0][pl.ds(at, R), :] = x_ref[pl.ds(r, R, stride=ROWS), :]
            X[0][pl.ds(at + R, 1), :] = small_ref[pl.ds(r, 1), :]
            X[0][pl.ds(at + R + 1, 1), :] = small_ref[pl.ds(ROWS + r, 1), :]
            X[0][pl.ds(at + R + 2, 1), :] = jnp.zeros((1, LANES), F32)
        return carry

    load.wait()
    lax.fori_loop(0, ROWS // 4, load_rows, 0)
    lane_k = iota((K, LANES), 1)

    def line(rho):
        return pl.ds(pl.multiple_of(rho * K, 8), K)

    def pack(base, n, q):
        def body(b, carry):
            left, right = carry
            for k in range(16):
                i = 16 * b + k
                row = X[0][line(base + i), :]
                here = (lane_k >= 4 * i) & (lane_k < 4 * i + 4)
                left = jnp.where(here, pltpu.roll(row, 4 * i, 1), left)
                right = jnp.where(here, pltpu.roll(row, lax.rem(4 * i + 4, LANES), 1), right)
            return left, right

        zero = jnp.zeros((K, LANES), F32)
        left, right = lax.fori_loop(0, n // 16, body, (zero, zero))
        PL[q, :, :] = left
        PR[q, :, :] = right

    pack(GHOST, 32, 0)
    pack(GHOST + 32, 16, 1)
    pl.semaphore_wait(barrier, count)

    halo = [
        send(X[0].at[pl.ds(GHOST * K, GHOST * K)], X[0].at[pl.ds((GHOST + ROWS) * K, GHOST * K)], hsend.at[0], hrecv.at[0], near(sizes, -1, 0)),
        send(X[0].at[pl.ds(ROWS * K, GHOST * K)], X[0].at[pl.ds(0, GHOST * K)], hsend.at[1], hrecv.at[1], near(sizes, 1, 0)),
        send(PL, RRB.at[pl.ds(1, 2)], hsend.at[2], hrecv.at[2], near(sizes, 0, -1)),
        send(PR, RLB.at[pl.ds(1, 2)], hsend.at[3], hrecv.at[3], near(sizes, 0, 1)),
        send(PL.at[0], RRB.at[3], hsend.at[4], hrecv.at[4], near(sizes, -1, -1)),
        send(PR.at[0], RLB.at[3], hsend.at[5], hrecv.at[5], near(sizes, -1, 1)),
        send(PL.at[1], RRB.at[0], hsend.at[6], hrecv.at[6], near(sizes, 1, -1)),
        send(PR.at[1], RLB.at[0], hsend.at[7], hrecv.at[7], near(sizes, 1, 1)),
    ]

    class Sum:
        def __init__(self, boxes, send_sems, recv_sems):
            self.boxes, self.send_sems, self.recv_sems, self.sem = boxes, send_sems, recv_sems, 0

        def start(self, stage, value):
            me = place(sizes, STAGES[stage])
            box = self.boxes[stage]
            box[me] = value
            self.copies = []
            for off in stage_offsets[stage]:
                to = peer_of(sizes, STAGES[stage], off)
                sems = self.send_sems.at[self.sem], self.recv_sems.at[self.sem]
                self.copies.append(send(box.at[me], box.at[me], *sems, to))
                self.sem += 1

        def finish(self, stage):
            for copy in self.copies:
                copy.wait_recv()
            box = self.boxes[stage]
            total = box[0]
            for i in range(1, len(stage_offsets[stage]) + 1):
                total = total + box[i]
            return total

    early = Sum(slots_early, esend, erecv)
    raw_lines = jnp.concatenate([X[0][line(r + GHOST), :] for r in range(ROWS)], axis=1)
    raw_part = jnp.concatenate([dot3(raw_lines, raw_lines, 1, 1), jnp.zeros((K, LANES - K), F32)], axis=1)
    early.start(0, raw_part)

    blank_half = jnp.zeros((KRYLOV, LANES), F32)
    pt = jnp.zeros((KRYLOV, 256), F32)
    for j in range(4):
        v = small_ref[pl.ds(2 * ROWS + j, KRYLOV, stride=4), :]
        v = jnp.concatenate([v, blank_half], axis=1)
        pt = pt + (pltpu.roll(v, j * K, 1) if j else v)
    pt = jnp.concatenate([pt, jnp.zeros((K - KRYLOV, 256), F32)], axis=0)
    kgram = dot(pt, pt, 1, 1)
    kgram = jnp.concatenate([kgram, jnp.zeros((K, LANES - K), F32)], axis=1)
    kinv = forward_inverse(augmented(kgram, 0.0, KRYLOV), KRYLOV)
    MT[...] = jnp.zeros((LANES, 256), F32)
    MT[pl.ds(0, K), :] = dot(kinv[:, 0:K], pt, 1, 0)
    HS[...] = jnp.zeros((LANES, LANES), F32)
    LB[...] = jnp.zeros((256, 256), F32)
    GS[...] = jnp.zeros((256, 256), F32)
    BIG[...] = jnp.zeros((FIRST, LANES), F32)
    BIG2[...] = jnp.zeros((SECOND, LANES), F32)
    CF[...] = jnp.zeros((10, 64, LANES), F32)
    AHL[pl.ds(PADDED, 256 - PADDED), :] = jnp.zeros((256 - PADDED, (ROWS + 8) * LANES), jnp.bfloat16)
    VW[...] = jnp.zeros((ROWS * 8, LANES), F32)
    UV[...] = jnp.zeros((ROWS * 24, LANES), F32)

    for copy in halo:
        copy.wait_recv()
    for copy in halo[:2]:
        copy.wait_send()
        pending.remove(copy)

    lane1 = iota((1, LANES), 1)
    has_right = (my_col < ncol - 1).astype(F32)
    has_left = (my_col > 0).astype(F32)
    side_mask = jnp.where(lane1 < 4, has_right, jnp.where(lane1 >= 124, has_left, 0.0))
    sub_k = iota((K, LANES), 0)

    def order_zero(base, n, part, first):
        unroll = min(n, 16)

        def body(b, carry):
            stores = []
            for k in range(unroll):
                i = unroll * b + k
                rho = base + i
                g = my_row * ROWS + rho - GHOST
                row_mask = ((g >= 0) & (g < grid_rows)).astype(F32)
                at = 4 * (first + i)
                right = pltpu.roll(RRB[part, :, :], lax.rem(LANES - at, LANES), 1)
                left = pltpu.roll(RLB[part, :, :], lax.rem(2 * LANES - 4 - at, LANES), 1)
                ms = side_mask * row_mask
                side = jnp.where(lane_k < 4, right, left) * ms
                mid = X[0][line(rho), :] * row_mask
                mc = jnp.ones((1, LANES), F32) * row_mask
                stores.append((rho, (mid, mc), (side, ms)))
            for rho, mid, side in stores:
                for half, (v, m) in enumerate((mid, side)):
                    d = v[R : R + 1, :]
                    s = v[R + 1 : R + 2, :]
                    CF[5 * half, pl.ds(rho + 4, 1), :] = 2.0 * d * m
                    CF[5 * half + 1, pl.ds(rho + 4, 1), :] = (2.0 * COUPLING) * m
                    CF[5 * half + 2, pl.ds(rho + 4, 1), :] = 2.0 * (s - COUPLING) * m
                    CF[5 * half + 3, pl.ds(rho + 4, 1), :] = 2.0 * (s + COUPLING) * m
                    CF[5 * half + 4, pl.ds(rho + 4, 1), :] = m
                X[0][line(rho), :] = jnp.where(sub_k < R, mid[0], 0.0)
                SD[0][line(rho), :] = jnp.where(sub_k < R, side[0], 0.0)
            return carry

        lax.fori_loop(0, n // unroll, body, 0)

    order_zero(0, 4, 0, 12)
    order_zero(4, 32, 1, 0)
    order_zero(36, 16, 2, 0)
    order_zero(52, 4, 3, 0)

    def split_tile(t, at, a):
        hi = a.astype(jnp.bfloat16)
        AHL[pl.ds(16 * t, 16), at] = hi
        AHL[pl.ds(256 + 16 * t, 16), at] = (a - hi.astype(F32)).astype(jnp.bfloat16)

    def images(m, n):
        def body(b, carry):
            mids, sides = [], []
            for k in range(n):
                rho = m + n * b + k
                c = X[m - 1][line(rho), :]
                s = SD[m - 1][line(rho), :]
                cu = X[m - 1][line(rho - 1), :] + X[m - 1][line(rho + 1), :]
                cl, sl = pltpu.roll(c, 1, 1), pltpu.roll(s, 1, 1)
                cr, sr = pltpu.roll(c, 127, 1), pltpu.roll(s, 127, 1)

                def row(kind):
                    return CF[kind, pl.ds(rho + 4, 1), :]

                left = jnp.where(lane_k == 0, sl, cl)
                right = jnp.where(lane_k == 127, sr, cr)
                new = row(0) * c - row(1) * cu + row(2) * right - row(3) * left
                mids.append(0.5 * new if m == 1 else new - X[m - 2][line(rho), :])
                if m < 4:
                    su = SD[m - 1][line(rho - 1), :] + SD[m - 1][line(rho + 1), :]
                    left = jnp.where(lane_k == 0, cl, sl)
                    right = jnp.where(lane_k == 127, cr, sr)
                    side = row(5) * s - row(6) * su + row(7) * right - row(8) * left
                    sides.append(0.5 * side if m == 1 else side - SD[m - 2][line(rho), :])
            for k in range(n):
                rho = m + n * b + k
                X[m][line(rho), :] = mids[k]
                if m < 4:
                    SD[m][line(rho), :] = sides[k]
                at = pl.ds(pl.multiple_of(rho * LANES, LANES), LANES)
                new = mids[k]
                if m in (1, 3):
                    ends = jnp.concatenate([X[m - 1][pl.ds(pl.multiple_of(rho * K + 32, 8), 8), :], new[0:8, :]], axis=0)
                    split_tile(5 * (m - 1) // 2 + 2, at, ends)
                    split_tile(5 * (m - 1) // 2 + 3, at, new[8:24, :])
                    split_tile(5 * (m - 1) // 2 + 4, at, new[24:40, :])
                else:
                    split_tile(5 * m // 2, at, new[0:16, :])
                    split_tile(5 * m // 2 + 1, at, new[16:32, :])
                if m == 4:
                    split_tile(12, at, jnp.concatenate([new[32:40, :], jnp.zeros((8, LANES), F32)], axis=0))
                if m == 1:
                    old = X[0][pl.ds(pl.multiple_of(rho * K, 8), 32), :]
                    split_tile(0, at, old[0:16, :])
                    split_tile(1, at, old[16:32, :])
            return carry

        lax.fori_loop(0, (ROWS + 8 - 2 * m) // n, body, 0)

    for m, n in zip(range(1, ORDERS), (18, 26, 25, 24)):
        images(m, n)
        if m == 1:
            early.start(1, early.finish(0))
        if m == 3:
            early.start(2, early.finish(1))


    def bdot(a, b):
        return lax.dot_general(a, b, (((1,), (1,)), ((), ())), preferred_element_type=F32)

    first_rows = jnp.concatenate([AHL[pl.ds(0, 48), CENTRE], AHL[pl.ds(256, 48), CENTRE]], axis=0)
    AC0[:, pl.ds(0, 256 + PADDED)] = bdot(first_rows, AHL[:, CENTRE])
    top = AC0[pl.ds(0, K), pl.ds(0, 256)] + AC0[pl.ds(48, K), pl.ds(0, 256)] + AC0[pl.ds(0, K), pl.ds(256, 256)]
    lane_w = iota((K, 256), 1)
    top = jnp.where(lane_w < FIELDS, top, 0.0)
    BIG[pl.ds(0, K), :] = pltpu.roll(top, 256 - K, 1)[:, 0:LANES]
    tail = pltpu.roll(top, 256 - 168, 1)[:, 0:LANES]
    quarter = iota((8, LANES), 1) // 32
    mixed = tail[0:8, :]
    for t in range(1, 4):
        mixed = jnp.where(quarter == t, pltpu.roll(tail[8 * t : 8 * t + 8, :], 32 * t, 1), mixed)
    BIG[pl.ds(K, 8), :] = mixed
    BIG[pl.ds(K + 8, 8), :] = tail[32:40, :]

    class Reduction:
        def __init__(self, big, whole, boxes, total_rows, send_sems, recv_sems):
            self.big, self.whole, self.boxes = big, whole, boxes
            self.chunk = total_rows // nrow
            self.send_sems, self.recv_sems, self.sem = send_sems, recv_sems, 0
            self.own = pl.ds(pl.multiple_of(my_row * self.chunk, 8), self.chunk)
            self.copies = []

        def emit(self, src, dst, to):
            self.copies.append(send(src, dst, self.send_sems.at[self.sem], self.recv_sems.at[self.sem], to))
            self.sem += 1

        def arrived(self):
            for copy in self.copies:
                copy.wait_recv()
            self.copies = []

        def start(self, stage):
            me = place(sizes, STAGES[stage])
            box = self.boxes[stage]
            if stage == 0:
                box[me] = self.big[self.own, :]
            for off in stage_offsets[stage]:
                to = peer_of(sizes, STAGES[stage], off)
                if stage == 0:
                    at = pl.multiple_of(linear(sizes, ROW, to) * self.chunk, 8)
                    self.emit(self.big.at[pl.ds(at, self.chunk)], box.at[me], to)
                else:
                    self.emit(box.at[me], box.at[me], to)

        def finish(self, stage):
            self.arrived()
            box = self.boxes[stage]
            total = box[0]
            for i in range(1, len(stage_offsets[stage]) + 1):
                total = total + box[i]
            if stage + 1 < len(STAGES):
                self.boxes[stage + 1][place(sizes, STAGES[stage + 1])] = total
            else:
                self.whole[self.own, :] = total * inverse_total

        def gather(self):
            for off in stage_offsets[0]:
                self.emit(self.whole.at[self.own], self.whole.at[self.own], peer_of(sizes, ROW, off))

    one = Reduction(BIG, FULL, slots_big, FIRST, bsend, brecv)
    two = Reduction(BIG2, FULL2, slots_two, SECOND, csend, crecv)
    one.start(0)

    ACC[...] = jnp.zeros((256 + PADDED, 256), F32)

    def gram_rest(g, carry):
        at = pl.ds(pl.multiple_of((GHOST + GROUP * g) * LANES, LANES), GROUP * LANES)
        ACC[:, pl.ds(0, PADDED)] += bdot(AHL[:, at], AHL[pl.ds(0, PADDED), at])
        return carry

    lax.fori_loop(0, ROWS // GROUP, gram_rest, 0)
    cross = jnp.concatenate([ACC[pl.ds(256, PADDED), :], jnp.zeros((256 - PADDED, 256), F32)], axis=0)
    ACC[pl.ds(0, PADDED), :] = ACC[pl.ds(0, PADDED), :] + cross[0:PADDED, :] + jnp.transpose(cross)[0:PADDED, :]

    def strip(a, shift):
        return pltpu.roll(ACC[pl.ds(a * K, K), :], shift % 256, 1)[:, 0:LANES]

    lane_n = iota((K, LANES), 1)
    BIG2[pl.ds(0, K), :] = strip(1, -40)
    BIG2[pl.ds(K, K), :] = strip(2, -80)
    BIG2[pl.ds(2 * K, K), :] = jnp.where(lane_n >= 80, strip(4, -80), strip(3, -120))
    BIG2[pl.ds(3 * K, K), :] = strip(1, -160)

    for stage in range(3):
        one.finish(stage)
        if stage < 2:
            one.start(stage + 1)
        if stage == 0:
            raw_gram = early.finish(2) * inverse_total
            finv = forward_inverse(augmented(raw_gram, GRAM_SHIFT, R), R)
            finv = jnp.where(sub_k < R, finv, 0.0)
            finv_wide = jnp.concatenate([finv, jnp.zeros((K, LANES), F32)], axis=1)
            for a in range(ORDERS):
                LB[pl.ds(a * K, K), :] = pltpu.roll(finv_wide, a * K, 1) if a else finv_wide
    one.gather()
    one.arrived()
    two.start(0)

    mixed = FULL[pl.ds(K, 8), :]
    tail = jnp.concatenate(
        [pltpu.roll(mixed, LANES - 32 * t, 1) if t else mixed for t in range(4)] + [FULL[pl.ds(K + 8, 8), :]],
        axis=0,
    )
    blank = jnp.zeros((K, LANES), F32)
    body = pltpu.roll(jnp.concatenate([FULL[pl.ds(0, K), :], blank], axis=1), K, 1)
    tail = pltpu.roll(jnp.concatenate([tail, blank], axis=1), 168, 1)
    head = jnp.concatenate([jnp.where((sub_k < R) & (lane_k < R), raw_gram, 0.0), blank], axis=1)
    GS[pl.ds(0, K), :] = jnp.where(
        lane_w < K, head, jnp.where(lane_w < 168, body, jnp.where(lane_w < FIELDS, tail, 0.0))
    )
    GC[...] = jnp.transpose(GS[pl.ds(0, LANES), :])

    def assemble_rest():
        def wide(a):
            v = FULL2[pl.ds(a * K, K), :]
            return jnp.concatenate([v, jnp.zeros((K, LANES), F32)], axis=1)

        def moved(v, shift, lo, hi):
            return jnp.where((lane_w >= lo) & (lane_w < hi), pltpu.roll(v, shift, 1), 0.0)

        GS[pl.ds(K, K), :] = moved(wide(0), 40, 40, 160) + moved(wide(3), 160, 160, 200)
        GS[pl.ds(2 * K, K), :] = moved(wide(1), 80, 80, 200)
        GS[pl.ds(3 * K, K), :] = moved(wide(2), 120, 120, 200)
        GS[pl.ds(4 * K, K), :] = moved(wide(2), 80, 160, 200)
        mirrored = jnp.transpose(GS[...])
        for a in range(1, ORDERS):
            GS[pl.ds(a * K, K), :] = jnp.where(
                lane_w >= a * K, GS[pl.ds(a * K, K), :], mirrored[a * K : (a + 1) * K, :]
            )

    square = (iota((LANES, LANES), 0) < K) & (iota((LANES, LANES), 1) < K)
    small = jnp.where(square, LB[pl.ds(0, LANES), pl.ds(0, LANES)], 0.0)
    GB0[...] = dot3(dot3(LB[...], GC[...], 1, 0), small, 1, 1)

    lane_r = iota((1, 256), 1)
    lane8 = iota((8, 256), 1)
    late = [Sum([b.at[s] for b in slots_late], lsend.at[s], lrecv.at[s]) for s in range(STEPS - 1)]

    def paired():
        v = jnp.concatenate([VW[pl.ds(8 * k, 8), :] for k in range(ROWS)], axis=1)
        v_hi = v.astype(jnp.bfloat16).astype(F32)
        return jnp.concatenate([v_hi, v - v_hi], axis=0).astype(jnp.bfloat16)

    def with_old(v):
        old = bdot(v, AHL[:, CENTRE])
        old = old[0:8, :] + old[8:16, :]
        d = old[:, 0:256] + jnp.concatenate([old[:, 256:], jnp.zeros((8, 256 - PADDED), F32)], axis=1)
        return jnp.where(lane8 < FIELDS, d, 0.0)

    def with_first(v):
        first = jnp.concatenate([AHL[pl.ds(0, 48), CENTRE], AHL[pl.ds(256, 48), CENTRE]], axis=0)
        part = bdot(v, first)
        return part[0:8, 0:K] + part[8:16, 0:K] + part[0:8, 48 : 48 + K]

    def with_new(v):
        w = jnp.concatenate([UV[pl.ds(24 * k, 24), :] for k in range(ROWS)], axis=1)
        w_hi = w.astype(jnp.bfloat16).astype(F32)
        w = jnp.concatenate([w_hi, w - w_hi], axis=0).astype(jnp.bfloat16)
        new = bdot(v, w)
        new = new[0:8, :] + new[8:16, :]
        return new[:, 0:24] + new[:, 24:48]

    def keep_late(s, total):
        rows = pl.ds(FIELDS + 8 * s, 8)
        GS[rows, :] = GS[rows, :] + total * inverse_total
    sub8 = iota((8, 256), 0)
    tile_mask = iota((64, LANES), 1)

    for s in range(STEPS):
        column = KRYLOV + s
        r = R + s
        latest = MT[pl.ds(column - 1, 1), :]

        def moved(shift):
            return pltpu.roll(latest, shift % 256, 1)

        cw = jnp.where(lane_r < K, 0.5 * moved(-80), -0.5 * moved(40))
        cw = jnp.where(lane_r < FIELDS, cw, 0.0)
        cw = jnp.broadcast_to(cw, (8, 256))
        h1 = dot3(cw, GB0[...], 1, 0)
        h = 2.0 * h1 - dot3(h1, GB0[pl.ds(0, LANES), :], 1, 0)
        h_wide = jnp.concatenate([h, jnp.zeros((8, LANES), F32)], axis=1)
        raw = dot3(cw - h_wide, LB[...], 1, 0)
        raw_col = jnp.transpose(raw)[0 : FIELDS + 24, 0:1]
        CB[...] = jnp.broadcast_to(raw_col, (FIELDS + 24, LANES))

        def combine(i, carry):
            for k in range(8):
                rho = 8 * i + k + GHOST
                value = CB[pl.ds(0, K), :] * X[0][line(rho), :]
                for m in range(1, ORDERS):
                    value = value + CB[pl.ds(m * K, K), :] * X[m][line(rho), :]
                value = jnp.sum(value, axis=0, keepdims=True)
                if s:
                    at = pl.multiple_of(24 * (8 * i + k), 8)
                    older = CB[pl.ds(FIELDS, 16), :] * UV[pl.ds(at, 16), :]
                    value = value + jnp.sum(older, axis=0, keepdims=True)
                U0[s, pl.ds(8 * i + k, 1), :] = value
            return carry

        lax.fori_loop(0, ROWS // 8, combine, 0)

        lane_t = iota((8, LANES), 1)
        sub_t = iota((8, LANES), 0)
        packed = jnp.zeros((8, LANES), F32)
        for q in range(6):
            tile = U0[s, pl.ds(8 * q, 8), :]
            packed = jnp.where(
                (lane_t >= 4 * q) & (lane_t < 4 * q + 4), pltpu.roll(tile, 4 * q, 1) if q else tile, packed
            )
            packed = jnp.where(
                (lane_t >= 64 + 4 * q) & (lane_t < 68 + 4 * q), pltpu.roll(tile, 68 + 4 * q, 1), packed
            )
        PK[s, :, :] = packed
        edge = [
            send(U0.at[s, pl.ds(0, 8)], HB.at[s], usend.at[s, 0], urecv.at[s, 0], near(sizes, -1, 0)),
            send(U0.at[s, pl.ds(40, 8)], HT.at[s], usend.at[s, 1], urecv.at[s, 1], near(sizes, 1, 0)),
            send(PK.at[s], KRB.at[s, 1], usend.at[s, 2], urecv.at[s, 2], near(sizes, 0, -1)),
            send(PK.at[s], KLB.at[s, 1], usend.at[s, 3], urecv.at[s, 3], near(sizes, 0, 1)),
            send(PK.at[s], KRB.at[s, 2], usend.at[s, 4], urecv.at[s, 4], near(sizes, -1, -1)),
            send(PK.at[s], KLB.at[s, 2], usend.at[s, 5], urecv.at[s, 5], near(sizes, -1, 1)),
            send(PK.at[s], KRB.at[s, 0], usend.at[s, 6], urecv.at[s, 6], near(sizes, 1, -1)),
            send(PK.at[s], KLB.at[s, 0], usend.at[s, 7], urecv.at[s, 7], near(sizes, 1, 1)),
        ]

        if s + 1 < STEPS:
            VW[pl.ds(0, ROWS, stride=8), :] = U0[s]
            d_old = with_old(paired())
        h_row = h_wide[0:1, :]
        e = jnp.where(lane_r < K, moved(-40), 0.5 * (moved(40) + moved(-40)))
        e = jnp.where(lane_r < 3 * K, e, pltpu.roll(h_row, 3 * K, 1))
        e = jnp.where(lane_r < 4 * K, e, 0.0)
        mt = MT[pl.ds(0, K), :]
        g1 = jnp.sum(mt * e, axis=1, keepdims=True)
        e1 = e - jnp.sum(mt * g1, axis=0, keepdims=True)
        g2 = jnp.sum(mt * e1, axis=1, keepdims=True)
        e2 = e1 - jnp.sum(mt * g2, axis=0, keepdims=True)
        e2_square = jnp.sum(e2 * e2, axis=1, keepdims=True)

        if s == 0:
            two.finish(0)
            two.start(1)
        if s == 1:
            two.finish(2)
            two.gather()
            late[0].start(1, late[0].finish(0))
        if s == 2:
            keep_late(0, late[0].finish(2))
            late[1].start(1, late[1].finish(0))
        for copy in edge:
            copy.wait_recv()

        mids = jnp.concatenate([HT[s], U0[s], HB[s]], axis=0) * CF[4]
        sides = []
        for j in range(8):
            part = 0 if j == 0 else (2 if j == 7 else 1)
            q = 5 if j == 0 else (0 if j == 7 else j - 1)
            rt = KRB[s, part]
            lf = pltpu.roll(KLB[s, part], 60 - 4 * q, 1)
            rt = pltpu.roll(rt, LANES - 4 * q, 1) if q else rt
            sides.append(jnp.where(lane_t < 4, rt, lf))
        sds = jnp.concatenate(sides, axis=0) * CF[9]

        def twice_s(c, v):
            cl, sl = pltpu.roll(c, 1, 1), pltpu.roll(v, 1, 1)
            cr, sr = pltpu.roll(c, 127, 1), pltpu.roll(v, 127, 1)
            cu = pltpu.roll(c, 1, 0) + pltpu.roll(c, 63, 0)
            su = pltpu.roll(v, 1, 0) + pltpu.roll(v, 63, 0)
            lo, hi = tile_mask == 0, tile_mask == 127
            mid = CF[0] * c - CF[1] * cu + CF[2] * jnp.where(hi, sr, cr) - CF[3] * jnp.where(lo, sl, cl)
            side = CF[5] * v - CF[6] * su + CF[7] * jnp.where(hi, cr, sr) - CF[8] * jnp.where(lo, cl, sl)
            return mid, side

        before = (mids, sds)
        now = twice_s(*before)
        now = (0.5 * now[0], 0.5 * now[1])
        orders = [before[0], now[0]]
        for m in range(2, ORDERS):
            nxt = twice_s(*now)
            before, now = now, (nxt[0] - before[0], nxt[1] - before[1])
            orders.append(now[0])
        for m in range(ORDERS):
            VB[m, :, :] = orders[m][8:56, :]
            VW[pl.ds(m, ROWS, stride=8), :] = orders[m][8:56, :]
            UV[pl.ds(8 * s + m, ROWS, stride=24), :] = orders[m][8:56, :]

        v = paired()
        if s + 1 < STEPS:
            total_sum = Sum([b.at[s] for b in slots_small], ssend.at[s], srecv.at[s])
            DN[...] = jnp.zeros((8, 256), F32)
            DN[:, pl.ds(0, K)] = with_first(v)
            DN[:, pl.ds(72, 24)] = with_new(v)
            low = pltpu.roll(DN[:, pl.ds(0, LANES)], 1, 0)
            wide_row = d_old[0:1, :]
            packed_new = jnp.where((lane_t >= 72) & (lane_t < 96), DN[0:1, pl.ds(0, LANES)], wide_row[:, LANES:])
            value = jnp.where(sub_t == 0, wide_row[:, 0:LANES], jnp.where(sub_t == 1, packed_new, low))
        else:
            total_sum = Sum(slots_last, ssend.at[s], srecv.at[s])
            DN[...] = with_old(v)
            DN[:, pl.ds(FIELDS, 24)] = with_new(v)
            value = DN[...]
        for stage in range(3):
            total_sum.start(stage, value)
            if stage == 0 and s + 1 < STEPS:
                rest = jnp.where((lane8 >= K) & (sub8 >= 1) & (sub8 < ORDERS), with_old(v), 0.0)
            if s == 0 and stage == 0:
                two.finish(1)
                two.start(2)
            if s == 0 and stage == 2:
                late[0].start(0, rest)
            if s == 1 and stage == 0:
                two.arrived()
                assemble_rest()
            if s == 1 and stage == 0:
                late[0].start(2, late[0].finish(1))
            if s == 1 and stage == 2:
                late[1].start(0, rest)
            if s == 2 and stage == 0:
                late[1].start(2, late[1].finish(1))
            value = total_sum.finish(stage)
        if s + 1 < STEPS:
            up = pltpu.roll(value, 7, 0)
            mid = (lane_t >= 72) & (lane_t < 96)
            left = jnp.where(sub_t == 0, value, jnp.where(lane_t < K, up, 0.0))
            right = jnp.where((sub_t == 0) | mid, up, 0.0)
            value = jnp.concatenate([left, right], axis=1)
        d = value * inverse_total
        d = jnp.where(sub8 < ORDERS, d, 0.0)

        nn = jnp.sum(jnp.where(lane_r == FIELDS + 8 * s, d[0:1, :], 0.0), axis=1, keepdims=True)
        beta = jnp.sqrt(nn + EPSILON)
        ib = 1.0 / beta
        eta = jnp.sqrt(e2_square + beta * beta + EPSILON)
        MT[pl.ds(column, 1), :] = (e2 + jnp.where(lane_r == 3 * K + r, beta, 0.0)) / eta
        sub_col = iota((K, 1), 0)
        g = g1 + g2 + jnp.where(sub_col == column, eta, 0.0)
        lane_h = iota((K, LANES), 1)
        HS[pl.ds(0, K), :] = jnp.where(lane_h == s, g, HS[pl.ds(0, K), :])
        newc_ref[s, :, :] = VB[0] * ib
        newi_ref[s, :, :] = VB[4] * ib
        for m in range(ORDERS):
            at = m * K + r
            LB[pl.ds(at, 1), :] = jnp.where(lane_r == FIELDS + 8 * s + m, ib, 0.0)
        GS[pl.ds(FIELDS + 8 * s, 8), :] = d
        if s + 1 < STEPS:
            db = dot3(d, LB[...], 1, 1) * ib
            dcol = jnp.transpose(db)[:, 0:1]
            lane_g = iota((256, LANES), 1)
            GB0[...] = jnp.where(lane_g == r, dcol, GB0[...])
            for m in range(ORDERS):
                GB0[pl.ds(m * K + r, 1), :] = jnp.where(lane1 < K, db[m : m + 1, 0:LANES], 0.0)

    keep_late(1, late[1].finish(2))
    mirrored = jnp.transpose(GS[...])
    def age(index):
        return sum(((index >= FIELDS + 8 * t).astype(jnp.int32) for t in range(1, STEPS)), (index >= FIELDS).astype(jnp.int32))

    whole_row = age(iota((256, 256), 0))
    whole_col = age(iota((256, 256), 1))
    GS[...] = jnp.where(whole_row >= whole_col, GS[...], mirrored)
    gram = dot3(dot3(LB[...], GS[...], 1, 0), LB[...], 1, 1)
    for a in range(ORDERS):
        for b in range(ORDERS):
            gram_ref[a, b, :, :] = gram[a * K : (a + 1) * K, b * K : (b + 1) * K]
    for j in range(4):
        coef_ref[:, j, :] = MT[pl.ds(0, KRYLOV + STEPS), pl.ds(j * K, K)]
    hess_ref[...] = jnp.transpose(HS[...])[0:STEPS, 0 : KRYLOV + STEPS]

    for copy in pending:
        copy.wait_send()


def handed_out(*refs):
    sources, targets, sems = refs[:5], refs[5:10], refs[10]
    copies = [pltpu.make_async_copy(a, b, sems.at[i]) for i, (a, b) in enumerate(zip(sources, targets))]
    for copy in copies:
        copy.start()
    for copy in copies:
        copy.wait()


def local(sizes, basis_raw, krylov_raw, stiffness, rotation):
    width = KRYLOV + STEPS
    nrow = sizes["x"] * sizes["core"]
    counts = []
    for axes in STAGES:
        n = 1
        for a in axes:
            n *= sizes[a]
        counts.append(n)
    big_copies = sum(n - 1 for n in counts) + counts[0] - 1
    small_copies = sum(n - 1 for n in counts)
    vmem = lambda *shape: pltpu.VMEM(shape, F32)
    half = lambda *shape: pltpu.VMEM(shape, jnp.bfloat16)
    dma = lambda *shape: pltpu.SemaphoreType.DMA(shape)
    scratch = [
        vmem(R * ROWS, LANES), dma(1),
        [vmem((ROWS + 8) * K, LANES) for _ in range(ORDERS)],
        [vmem((ROWS + 8) * K, LANES) for _ in range(ORDERS - 1)],
        vmem(10, 64, LANES), vmem(2, K, LANES), vmem(2, K, LANES), vmem(4, K, LANES), vmem(4, K, LANES),
        half(256 + PADDED, (ROWS + 8) * LANES), vmem(256 + PADDED, 256), vmem(96, 512),
        vmem(FIRST, LANES), vmem(FIRST, LANES), vmem(SECOND, LANES), vmem(SECOND, LANES),
        vmem(256, 256), vmem(256, LANES), vmem(256, 256),
        vmem(256, LANES), vmem(FIELDS + 24, LANES), vmem(LANES, 256), vmem(LANES, LANES),
        vmem(STEPS, ROWS, LANES), vmem(STEPS, 8, LANES), vmem(STEPS, 8, LANES), vmem(STEPS, 8, LANES),
        vmem(STEPS, 3, 8, LANES), vmem(STEPS, 3, 8, LANES), vmem(ORDERS, ROWS, LANES),
        vmem(ROWS * 8, LANES), vmem(ROWS * 24, LANES), vmem(8, 256),
        [vmem(n, FIRST // nrow, LANES) for n in counts],
        [vmem(n, SECOND // nrow, LANES) for n in counts],
        [vmem(STEPS - 1, n, 8, LANES) for n in counts],
        [vmem(n, 8, 256) for n in counts],
        [vmem(STEPS - 1, n, 8, 256) for n in counts],
        [vmem(n, K, LANES) for n in counts],
        dma(8), dma(8), dma(big_copies), dma(big_copies), dma(big_copies), dma(big_copies),
        dma(STEPS, 8), dma(STEPS, 8), dma(STEPS, small_copies), dma(STEPS, small_copies),
        dma(STEPS - 1, small_copies), dma(STEPS - 1, small_copies),
        dma(small_copies), dma(small_copies),
    ]
    shape = lambda *dims: jax.ShapeDtypeStruct(dims, F32)
    shapes = [
        shape(STEPS, ROWS, LANES), shape(width, 4, K), shape(STEPS, width),
        shape(ORDERS, ORDERS, K, K), shape(STEPS, ROWS, LANES),
    ]
    krylov_lines = jnp.transpose(krylov_raw, (2, 0, 1)).reshape(4 * KRYLOV, R)
    krylov_lines = jnp.pad(krylov_lines, ((0, 0), (0, LANES - R)))
    small = jnp.concatenate([stiffness, rotation, krylov_lines], axis=0)
    results = pl.pallas_call(
        functools.partial(kernel, sizes),
        out_shape=shapes,
        in_specs=[pl.BlockSpec(memory_space=pltpu.HBM), pl.BlockSpec(memory_space=pltpu.VMEM)],
        out_specs=[pl.BlockSpec(memory_space=pltpu.VMEM)] * 5,
        scratch_shapes=scratch,
        compiler_params=pltpu.CompilerParams(
            collective_id=0, has_side_effects=True, vmem_limit_bytes=55_000_000
        ),
    )(
        basis_raw.reshape(R * ROWS, LANES), small,
    )
    new_columns, coefficients, hessenberg, gram, new_images = pl.pallas_call(
        handed_out,
        out_shape=shapes,
        in_specs=[pl.BlockSpec(memory_space=pltpu.VMEM)] * 5,
        out_specs=[pl.BlockSpec(memory_space=pltpu.HBM)] * 5,
        scratch_shapes=[pltpu.SemaphoreType.DMA((5,))],
        compiler_params=pltpu.CompilerParams(vmem_limit_bytes=2 * 1024 * 1024),
    )(*results)
    return (
        new_columns, jnp.transpose(coefficients, (1, 2, 0)), hessenberg,
        jnp.transpose(gram, (0, 2, 1, 3)), new_images,
    )


def solution(mesh):
    cores = 2
    columns = mesh.devices.shape[1]
    depth = 8 if columns % 8 == 0 else 2
    sizes = {
        "x": mesh.devices.shape[0] // cores, "core": cores,
        "y": columns // depth, "z": depth,
    }
    split = Mesh(mesh.devices.reshape(*(sizes[a] for a in AXES)), AXES)
    return jax.shard_map(
        functools.partial(local, sizes),
        mesh=split,
        in_specs=(P(None, ROW, COL), P(), P(ROW, COL), P(ROW, COL)),
        out_specs=(P(None, ROW, COL), P(), P(), P(), P(None, ROW, COL)),
        check_vma=False,
    )
```

```python
import functools
import itertools

import jax
import jax.numpy as jnp
from jax import lax
from jax.experimental import pallas as pl
from jax.experimental.pallas import tpu as pltpu
from jax.sharding import Mesh
from jax.sharding import PartitionSpec as P

K = 40
STEPS = 3
R = 37
KRYLOV = 34
ORDERS = 5
FIELDS = ORDERS * K
COUPLING = 0.2
EPSILON = 1e-06
GRAM_SHIFT = 0.05
HIGHEST = lax.Precision.HIGHEST
AXES = ("x", "core", "y", "z")
ROW = ("x", "core")
COL = ("y", "z")
STAGES = (("x", "core"), ("y",), ("z",))
ROWS = 48
LANES = 128
GHOST = 4
PADDED = 208
GROUP = 8
FIRST = 64
SECOND = 192
CENTRE = pl.ds(GHOST * LANES, ROWS * LANES)
F32 = jnp.float32


def dot(a, b, ca, cb):
    return lax.dot_general(
        a, b, (((ca,), (cb,)), ((), ())), precision=HIGHEST, preferred_element_type=F32
    )


def dot3(a, b, ca, cb):
    return lax.dot_general(
        a, b, (((ca,), (cb,)), ((), ())), precision=lax.Precision.HIGH, preferred_element_type=F32
    )


def iota(shape, dim):
    return lax.broadcasted_iota(jnp.int32, shape, dim)


def offsets(sizes, axes):
    ranges = [range(sizes[a]) for a in axes]
    return [o for o in itertools.product(*ranges) if any(o)]


def place(sizes, axes):
    index = 0
    for a in axes:
        index = index * sizes[a] + lax.axis_index(a)
    return index


def peer_of(sizes, axes, off):
    return {a: lax.rem(lax.axis_index(a) + o, sizes[a]) for a, o in zip(axes, off)}


def linear(sizes, axes, coords):
    index = 0
    for a in axes:
        index = index * sizes[a] + coords[a]
    return index


def near(sizes, drow, dcol):
    rows = sizes["x"] * sizes["core"]
    cols = sizes["y"] * sizes["z"]
    r = lax.rem(place(sizes, ROW) + drow + rows, rows)
    c = lax.rem(place(sizes, COL) + dcol + cols, cols)
    return {
        "x": r // sizes["core"],
        "core": lax.rem(r, sizes["core"]),
        "y": c // sizes["z"],
        "z": lax.rem(c, sizes["z"]),
    }


def full(coords):
    return tuple(coords.get(a, lax.axis_index(a)) for a in AXES)


SIDES = [(-1, 0), (1, 0), (0, -1), (0, 1), (-1, -1), (-1, 1), (1, -1), (1, 1)]


def forward_inverse(a, count, block=4):
    sub = iota((K, LANES), 0)
    lane = iota((K, LANES), 1)
    for first in range(0, count, block):
        pivots = range(first, min(first + block, count))
        cols = [jnp.broadcast_to(a[:, j : j + 1], (K, LANES)) for j in pivots]
        rows = [a[j : j + 1, :] for j in pivots]
        for p, j in enumerate(pivots):
            inverse = 1.0 / cols[p][j : j + 1, :]
            factor = jnp.where(sub > j, cols[p] * inverse, 0.0)
            for q in range(p + 1, len(pivots)):
                cols[q] = cols[q] - factor * cols[q][j : j + 1, :]
                rows[q] = rows[q] - factor[pivots[q] : pivots[q] + 1, :] * rows[p]
            a = a - factor * rows[p]
    diag = jnp.sum(jnp.where(lane == sub, a, 0.0), axis=1, keepdims=True)
    scaled = a * (1.0 / jnp.sqrt(diag))
    return jnp.where(lane < K, pltpu.roll(scaled, 64, 1), 0.0)


def augmented(a, shift, count):
    sub = iota((K, LANES), 0)
    lane = iota((K, LANES), 1)
    a = jnp.where((lane < count) & (sub < count), a, 0.0)
    a = a + jnp.where((lane == sub) & (sub < count), shift, 0.0)
    return a + jnp.where(((lane == sub) & (sub >= count)) | (lane == sub + 64), 1.0, 0.0)


def kernel(
    sizes, x_hbm, small_ref,
    newc_ref, coef_ref, hess_ref, gram_ref, newi_ref,
    x_ref, in_sem,
    X, SD, CF, PL, PR, RRB, RLB, AHL, ACC, AC0, BIG, FULL, BIG2, FULL2, GS, GC, LB, GB0, CB, MT, HS,
    U0, PK, HT, HB, KRB, KLB, VB, VW, UV, DN,
    slots_big, slots_two, slots_small, slots_last, slots_late, slots_early,
    hsend, hrecv, bsend, brecv, csend, crecv, usend, urecv, ssend, srecv, lsend, lrecv, esend, erecv,
):
    nrow = sizes["x"] * sizes["core"]
    ncol = sizes["y"] * sizes["z"]
    my_row = place(sizes, ROW)
    my_col = place(sizes, COL)
    grid_rows = nrow * ROWS
    inverse_total = 1.0 / (grid_rows * ncol * LANES)
    stage_offsets = [offsets(sizes, axes) for axes in STAGES]
    pending = []

    load = pltpu.make_async_copy(x_hbm, x_ref.at[pl.ds(0, R * ROWS)], in_sem.at[0])
    load.start()

    barrier = pltpu.get_barrier_semaphore()
    count = 0
    for axes, offs in zip(STAGES, stage_offsets):
        for off in offs:
            pl.semaphore_signal(
                barrier, inc=1, device_id=full(peer_of(sizes, axes, off)),
                device_id_type=pl.DeviceIdType.MESH,
            )
            count += 1
    for side in SIDES:
        pl.semaphore_signal(
            barrier, inc=1, device_id=full(near(sizes, *side)),
            device_id_type=pl.DeviceIdType.MESH,
        )
        count += 1

    def send(src, dst, ssem, rsem, coords):
        copy = pltpu.make_async_remote_copy(
            src_ref=src, dst_ref=dst, send_sem=ssem, recv_sem=rsem,
            device_id=full(coords), device_id_type=pl.DeviceIdType.MESH,
        )
        copy.start()
        pending.append(copy)
        return copy

    def load_rows(i, carry):
        for k in range(4):
            r = 4 * i + k
            at = pl.multiple_of((r + GHOST) * K, 8)
            X[0][pl.ds(at, R), :] = x_ref[pl.ds(r, R, stride=ROWS), :]
            X[0][pl.ds(at + R, 1), :] = small_ref[pl.ds(r, 1), :]
            X[0][pl.ds(at + R + 1, 1), :] = small_ref[pl.ds(ROWS + r, 1), :]
            X[0][pl.ds(at + R + 2, 1), :] = jnp.zeros((1, LANES), F32)
        return carry

    load.wait()
    lax.fori_loop(0, ROWS // 4, load_rows, 0)
    lane_k = iota((K, LANES), 1)

    def line(rho):
        return pl.ds(pl.multiple_of(rho * K, 8), K)

    def pack(base, n, q):
        def body(b, carry):
            left, right = carry
            for k in range(16):
                i = 16 * b + k
                row = X[0][line(base + i), :]
                here = (lane_k >= 4 * i) & (lane_k < 4 * i + 4)
                left = jnp.where(here, pltpu.roll(row, 4 * i, 1), left)
                right = jnp.where(here, pltpu.roll(row, lax.rem(4 * i + 4, LANES), 1), right)
            return left, right

        zero = jnp.zeros((K, LANES), F32)
        left, right = lax.fori_loop(0, n // 16, body, (zero, zero))
        PL[q, :, :] = left
        PR[q, :, :] = right

    pack(GHOST, 32, 0)
    pack(GHOST + 32, 16, 1)
    pl.semaphore_wait(barrier, count)

    halo = [
        send(X[0].at[pl.ds(GHOST * K, GHOST * K)], X[0].at[pl.ds((GHOST + ROWS) * K, GHOST * K)], hsend.at[0], hrecv.at[0], near(sizes, -1, 0)),
        send(X[0].at[pl.ds(ROWS * K, GHOST * K)], X[0].at[pl.ds(0, GHOST * K)], hsend.at[1], hrecv.at[1], near(sizes, 1, 0)),
        send(PL, RRB.at[pl.ds(1, 2)], hsend.at[2], hrecv.at[2], near(sizes, 0, -1)),
        send(PR, RLB.at[pl.ds(1, 2)], hsend.at[3], hrecv.at[3], near(sizes, 0, 1)),
        send(PL.at[0], RRB.at[3], hsend.at[4], hrecv.at[4], near(sizes, -1, -1)),
        send(PR.at[0], RLB.at[3], hsend.at[5], hrecv.at[5], near(sizes, -1, 1)),
        send(PL.at[1], RRB.at[0], hsend.at[6], hrecv.at[6], near(sizes, 1, -1)),
        send(PR.at[1], RLB.at[0], hsend.at[7], hrecv.at[7], near(sizes, 1, 1)),
    ]

    class Sum:
        def __init__(self, boxes, send_sems, recv_sems):
            self.boxes, self.send_sems, self.recv_sems, self.sem = boxes, send_sems, recv_sems, 0

        def start(self, stage, value):
            me = place(sizes, STAGES[stage])
            box = self.boxes[stage]
            box[me] = value
            self.copies = []
            for off in stage_offsets[stage]:
                to = peer_of(sizes, STAGES[stage], off)
                sems = self.send_sems.at[self.sem], self.recv_sems.at[self.sem]
                self.copies.append(send(box.at[me], box.at[me], *sems, to))
                self.sem += 1

        def finish(self, stage):
            for copy in self.copies:
                copy.wait_recv()
            box = self.boxes[stage]
            total = box[0]
            for i in range(1, len(stage_offsets[stage]) + 1):
                total = total + box[i]
            return total

    early = Sum(slots_early, esend, erecv)
    raw_lines = jnp.concatenate([X[0][line(r + GHOST), :] for r in range(ROWS)], axis=1)
    raw_part = jnp.concatenate([dot3(raw_lines, raw_lines, 1, 1), jnp.zeros((K, LANES - K), F32)], axis=1)
    early.start(0, raw_part)

    blank_half = jnp.zeros((KRYLOV, LANES), F32)
    pt = jnp.zeros((KRYLOV, 256), F32)
    for j in range(4):
        v = small_ref[pl.ds(2 * ROWS + j, KRYLOV, stride=4), :]
        v = jnp.concatenate([v, blank_half], axis=1)
        pt = pt + (pltpu.roll(v, j * K, 1) if j else v)
    pt = jnp.concatenate([pt, jnp.zeros((K - KRYLOV, 256), F32)], axis=0)
    kgram = dot(pt, pt, 1, 1)
    kgram = jnp.concatenate([kgram, jnp.zeros((K, LANES - K), F32)], axis=1)
    kinv = forward_inverse(augmented(kgram, 0.0, KRYLOV), KRYLOV)
    MT[...] = jnp.zeros((LANES, 256), F32)
    MT[pl.ds(0, K), :] = dot(kinv[:, 0:K], pt, 1, 0)
    HS[...] = jnp.zeros((LANES, LANES), F32)
    LB[...] = jnp.zeros((256, 256), F32)
    GS[...] = jnp.zeros((256, 256), F32)
    BIG[...] = jnp.zeros((FIRST, LANES), F32)
    BIG2[...] = jnp.zeros((SECOND, LANES), F32)
    CF[...] = jnp.zeros((10, 64, LANES), F32)
    AHL[pl.ds(PADDED, 256 - PADDED), :] = jnp.zeros((256 - PADDED, (ROWS + 8) * LANES), jnp.bfloat16)
    VW[...] = jnp.zeros((ROWS * 8, LANES), F32)
    UV[...] = jnp.zeros((ROWS * 24, LANES), F32)

    for copy in halo:
        copy.wait_recv()
    for copy in halo[:2]:
        copy.wait_send()
        pending.remove(copy)

    lane1 = iota((1, LANES), 1)
    has_right = (my_col < ncol - 1).astype(F32)
    has_left = (my_col > 0).astype(F32)
    side_mask = jnp.where(lane1 < 4, has_right, jnp.where(lane1 >= 124, has_left, 0.0))
    sub_k = iota((K, LANES), 0)

    def order_zero(base, n, part, first):
        unroll = min(n, 16)

        def body(b, carry):
            stores = []
            for k in range(unroll):
                i = unroll * b + k
                rho = base + i
                g = my_row * ROWS + rho - GHOST
                row_mask = ((g >= 0) & (g < grid_rows)).astype(F32)
                at = 4 * (first + i)
                right = pltpu.roll(RRB[part, :, :], lax.rem(LANES - at, LANES), 1)
                left = pltpu.roll(RLB[part, :, :], lax.rem(2 * LANES - 4 - at, LANES), 1)
                ms = side_mask * row_mask
                side = jnp.where(lane_k < 4, right, left) * ms
                mid = X[0][line(rho), :] * row_mask
                mc = jnp.ones((1, LANES), F32) * row_mask
                stores.append((rho, (mid, mc), (side, ms)))
            for rho, mid, side in stores:
                for half, (v, m) in enumerate((mid, side)):
                    d = v[R : R + 1, :]
                    s = v[R + 1 : R + 2, :]
                    CF[5 * half, pl.ds(rho + 4, 1), :] = 2.0 * d * m
                    CF[5 * half + 1, pl.ds(rho + 4, 1), :] = (2.0 * COUPLING) * m
                    CF[5 * half + 2, pl.ds(rho + 4, 1), :] = 2.0 * (s - COUPLING) * m
                    CF[5 * half + 3, pl.ds(rho + 4, 1), :] = 2.0 * (s + COUPLING) * m
                    CF[5 * half + 4, pl.ds(rho + 4, 1), :] = m
                X[0][line(rho), :] = jnp.where(sub_k < R, mid[0], 0.0)
                SD[0][line(rho), :] = jnp.where(sub_k < R, side[0], 0.0)
            return carry

        lax.fori_loop(0, n // unroll, body, 0)

    order_zero(0, 4, 0, 12)
    order_zero(4, 32, 1, 0)
    order_zero(36, 16, 2, 0)
    order_zero(52, 4, 3, 0)

    def split_tile(t, at, a):
        hi = a.astype(jnp.bfloat16)
        AHL[pl.ds(16 * t, 16), at] = hi
        AHL[pl.ds(256 + 16 * t, 16), at] = (a - hi.astype(F32)).astype(jnp.bfloat16)

    def images(m, n):
        def body(b, carry):
            mids, sides = [], []
            for k in range(n):
                rho = m + n * b + k
                c = X[m - 1][line(rho), :]
                s = SD[m - 1][line(rho), :]
                cu = X[m - 1][line(rho - 1), :] + X[m - 1][line(rho + 1), :]
                cl, sl = pltpu.roll(c, 1, 1), pltpu.roll(s, 1, 1)
                cr, sr = pltpu.roll(c, 127, 1), pltpu.roll(s, 127, 1)

                def row(kind):
                    return CF[kind, pl.ds(rho + 4, 1), :]

                left = jnp.where(lane_k == 0, sl, cl)
                right = jnp.where(lane_k == 127, sr, cr)
                new = row(0) * c - row(1) * cu + row(2) * right - row(3) * left
                mids.append(0.5 * new if m == 1 else new - X[m - 2][line(rho), :])
                if m < 4:
                    su = SD[m - 1][line(rho - 1), :] + SD[m - 1][line(rho + 1), :]
                    left = jnp.where(lane_k == 0, cl, sl)
                    right = jnp.where(lane_k == 127, cr, sr)
                    side = row(5) * s - row(6) * su + row(7) * right - row(8) * left
                    sides.append(0.5 * side if m == 1 else side - SD[m - 2][line(rho), :])
            for k in range(n):
                rho = m + n * b + k
                X[m][line(rho), :] = mids[k]
                if m < 4:
                    SD[m][line(rho), :] = sides[k]
                at = pl.ds(pl.multiple_of(rho * LANES, LANES), LANES)
                new = mids[k]
                if m in (1, 3):
                    ends = jnp.concatenate([X[m - 1][pl.ds(pl.multiple_of(rho * K + 32, 8), 8), :], new[0:8, :]], axis=0)
                    split_tile(5 * (m - 1) // 2 + 2, at, ends)
                    split_tile(5 * (m - 1) // 2 + 3, at, new[8:24, :])
                    split_tile(5 * (m - 1) // 2 + 4, at, new[24:40, :])
                else:
                    split_tile(5 * m // 2, at, new[0:16, :])
                    split_tile(5 * m // 2 + 1, at, new[16:32, :])
                if m == 4:
                    split_tile(12, at, jnp.concatenate([new[32:40, :], jnp.zeros((8, LANES), F32)], axis=0))
                if m == 1:
                    old = X[0][pl.ds(pl.multiple_of(rho * K, 8), 32), :]
                    split_tile(0, at, old[0:16, :])
                    split_tile(1, at, old[16:32, :])
            return carry

        lax.fori_loop(0, (ROWS + 8 - 2 * m) // n, body, 0)

    for m, n in zip(range(1, ORDERS), (18, 26, 25, 24)):
        images(m, n)
        if m == 1:
            early.start(1, early.finish(0))
        if m == 3:
            early.start(2, early.finish(1))


    def bdot(a, b):
        return lax.dot_general(a, b, (((1,), (1,)), ((), ())), preferred_element_type=F32)

    first_rows = jnp.concatenate([AHL[pl.ds(0, 48), CENTRE], AHL[pl.ds(256, 48), CENTRE]], axis=0)
    AC0[:, pl.ds(0, 256 + PADDED)] = bdot(first_rows, AHL[:, CENTRE])
    top = AC0[pl.ds(0, K), pl.ds(0, 256)] + AC0[pl.ds(48, K), pl.ds(0, 256)] + AC0[pl.ds(0, K), pl.ds(256, 256)]
    lane_w = iota((K, 256), 1)
    top = jnp.where(lane_w < FIELDS, top, 0.0)
    BIG[pl.ds(0, K), :] = pltpu.roll(top, 256 - K, 1)[:, 0:LANES]
    tail = pltpu.roll(top, 256 - 168, 1)[:, 0:LANES]
    quarter = iota((8, LANES), 1) // 32
    mixed = tail[0:8, :]
    for t in range(1, 4):
        mixed = jnp.where(quarter == t, pltpu.roll(tail[8 * t : 8 * t + 8, :], 32 * t, 1), mixed)
    BIG[pl.ds(K, 8), :] = mixed
    BIG[pl.ds(K + 8, 8), :] = tail[32:40, :]

    class Reduction:
        def __init__(self, big, whole, boxes, total_rows, send_sems, recv_sems):
            self.big, self.whole, self.boxes = big, whole, boxes
            self.chunk = total_rows // nrow
            self.send_sems, self.recv_sems, self.sem = send_sems, recv_sems, 0
            self.own = pl.ds(pl.multiple_of(my_row * self.chunk, 8), self.chunk)
            self.copies = []

        def emit(self, src, dst, to):
            self.copies.append(send(src, dst, self.send_sems.at[self.sem], self.recv_sems.at[self.sem], to))
            self.sem += 1

        def arrived(self):
            for copy in self.copies:
                copy.wait_recv()
            self.copies = []

        def start(self, stage):
            me = place(sizes, STAGES[stage])
            box = self.boxes[stage]
            if stage == 0:
                box[me] = self.big[self.own, :]
            for off in stage_offsets[stage]:
                to = peer_of(sizes, STAGES[stage], off)
                if stage == 0:
                    at = pl.multiple_of(linear(sizes, ROW, to) * self.chunk, 8)
                    self.emit(self.big.at[pl.ds(at, self.chunk)], box.at[me], to)
                else:
                    self.emit(box.at[me], box.at[me], to)

        def finish(self, stage):
            self.arrived()
            box = self.boxes[stage]
            total = box[0]
            for i in range(1, len(stage_offsets[stage]) + 1):
                total = total + box[i]
            if stage + 1 < len(STAGES):
                self.boxes[stage + 1][place(sizes, STAGES[stage + 1])] = total
            else:
                self.whole[self.own, :] = total * inverse_total

        def gather(self):
            for off in stage_offsets[0]:
                self.emit(self.whole.at[self.own], self.whole.at[self.own], peer_of(sizes, ROW, off))

    one = Reduction(BIG, FULL, slots_big, FIRST, bsend, brecv)
    two = Reduction(BIG2, FULL2, slots_two, SECOND, csend, crecv)
    one.start(0)

    ACC[...] = jnp.zeros((256 + PADDED, 256), F32)

    def gram_rest(g, carry):
        at = pl.ds(pl.multiple_of((GHOST + GROUP * g) * LANES, LANES), GROUP * LANES)
        ACC[:, pl.ds(0, PADDED)] += bdot(AHL[:, at], AHL[pl.ds(0, PADDED), at])
        return carry

    lax.fori_loop(0, ROWS // GROUP, gram_rest, 0)
    cross = jnp.concatenate([ACC[pl.ds(256, PADDED), :], jnp.zeros((256 - PADDED, 256), F32)], axis=0)
    ACC[pl.ds(0, PADDED), :] = ACC[pl.ds(0, PADDED), :] + cross[0:PADDED, :] + jnp.transpose(cross)[0:PADDED, :]

    def strip(a, shift):
        return pltpu.roll(ACC[pl.ds(a * K, K), :], shift % 256, 1)[:, 0:LANES]

    lane_n = iota((K, LANES), 1)
    BIG2[pl.ds(0, K), :] = strip(1, -40)
    BIG2[pl.ds(K, K), :] = strip(2, -80)
    BIG2[pl.ds(2 * K, K), :] = jnp.where(lane_n >= 80, strip(4, -80), strip(3, -120))
    BIG2[pl.ds(3 * K, K), :] = strip(1, -160)

    for stage in range(3):
        one.finish(stage)
        if stage < 2:
            one.start(stage + 1)
        if stage == 0:
            raw_gram = early.finish(2) * inverse_total
            finv = forward_inverse(augmented(raw_gram, GRAM_SHIFT, R), R)
            finv = jnp.where(sub_k < R, finv, 0.0)
            finv_wide = jnp.concatenate([finv, jnp.zeros((K, LANES), F32)], axis=1)
            for a in range(ORDERS):
                LB[pl.ds(a * K, K), :] = pltpu.roll(finv_wide, a * K, 1) if a else finv_wide
    one.gather()
    one.arrived()
    two.start(0)

    mixed = FULL[pl.ds(K, 8), :]
    tail = jnp.concatenate(
        [pltpu.roll(mixed, LANES - 32 * t, 1) if t else mixed for t in range(4)] + [FULL[pl.ds(K + 8, 8), :]],
        axis=0,
    )
    blank = jnp.zeros((K, LANES), F32)
    body = pltpu.roll(jnp.concatenate([FULL[pl.ds(0, K), :], blank], axis=1), K, 1)
    tail = pltpu.roll(jnp.concatenate([tail, blank], axis=1), 168, 1)
    head = jnp.concatenate([jnp.where((sub_k < R) & (lane_k < R), raw_gram, 0.0), blank], axis=1)
    GS[pl.ds(0, K), :] = jnp.where(
        lane_w < K, head, jnp.where(lane_w < 168, body, jnp.where(lane_w < FIELDS, tail, 0.0))
    )
    GC[...] = jnp.transpose(GS[pl.ds(0, LANES), :])

    def assemble_rest():
        def wide(a):
            v = FULL2[pl.ds(a * K, K), :]
            return jnp.concatenate([v, jnp.zeros((K, LANES), F32)], axis=1)

        def moved(v, shift, lo, hi):
            return jnp.where((lane_w >= lo) & (lane_w < hi), pltpu.roll(v, shift, 1), 0.0)

        GS[pl.ds(K, K), :] = moved(wide(0), 40, 40, 160) + moved(wide(3), 160, 160, 200)
        GS[pl.ds(2 * K, K), :] = moved(wide(1), 80, 80, 200)
        GS[pl.ds(3 * K, K), :] = moved(wide(2), 120, 120, 200)
        GS[pl.ds(4 * K, K), :] = moved(wide(2), 80, 160, 200)
        mirrored = jnp.transpose(GS[...])
        for a in range(1, ORDERS):
            GS[pl.ds(a * K, K), :] = jnp.where(
                lane_w >= a * K, GS[pl.ds(a * K, K), :], mirrored[a * K : (a + 1) * K, :]
            )

    square = (iota((LANES, LANES), 0) < K) & (iota((LANES, LANES), 1) < K)
    small = jnp.where(square, LB[pl.ds(0, LANES), pl.ds(0, LANES)], 0.0)
    GB0[...] = dot3(dot3(LB[...], GC[...], 1, 0), small, 1, 1)

    lane_r = iota((1, 256), 1)
    lane8 = iota((8, 256), 1)
    late = [Sum([b.at[s] for b in slots_late], lsend.at[s], lrecv.at[s]) for s in range(STEPS - 1)]

    def paired():
        v = jnp.concatenate([VW[pl.ds(8 * k, 8), :] for k in range(ROWS)], axis=1)
        v_hi = v.astype(jnp.bfloat16).astype(F32)
        return jnp.concatenate([v_hi, v - v_hi], axis=0).astype(jnp.bfloat16)

    def with_old(v):
        old = bdot(v, AHL[:, CENTRE])
        old = old[0:8, :] + old[8:16, :]
        d = old[:, 0:256] + jnp.concatenate([old[:, 256:], jnp.zeros((8, 256 - PADDED), F32)], axis=1)
        return jnp.where(lane8 < FIELDS, d, 0.0)

    def with_first(v):
        first = jnp.concatenate([AHL[pl.ds(0, 48), CENTRE], AHL[pl.ds(256, 48), CENTRE]], axis=0)
        part = bdot(v, first)
        return part[0:8, 0:K] + part[8:16, 0:K] + part[0:8, 48 : 48 + K]

    def with_new(v):
        w = jnp.concatenate([UV[pl.ds(24 * k, 24), :] for k in range(ROWS)], axis=1)
        w_hi = w.astype(jnp.bfloat16).astype(F32)
        w = jnp.concatenate([w_hi, w - w_hi], axis=0).astype(jnp.bfloat16)
        new = bdot(v, w)
        new = new[0:8, :] + new[8:16, :]
        return new[:, 0:24] + new[:, 24:48]

    def keep_late(s, total):
        rows = pl.ds(FIELDS + 8 * s, 8)
        GS[rows, :] = GS[rows, :] + total * inverse_total
    sub8 = iota((8, 256), 0)
    tile_mask = iota((64, LANES), 1)

    for s in range(STEPS):
        column = KRYLOV + s
        r = R + s
        latest = MT[pl.ds(column - 1, 1), :]

        def moved(shift):
            return pltpu.roll(latest, shift % 256, 1)

        cw = jnp.where(lane_r < K, 0.5 * moved(-80), -0.5 * moved(40))
        cw = jnp.where(lane_r < FIELDS, cw, 0.0)
        cw = jnp.broadcast_to(cw, (8, 256))
        h1 = dot3(cw, GB0[...], 1, 0)
        h = 2.0 * h1 - dot3(h1, GB0[pl.ds(0, LANES), :], 1, 0)
        h_wide = jnp.concatenate([h, jnp.zeros((8, LANES), F32)], axis=1)
        raw = dot3(cw - h_wide, LB[...], 1, 0)
        raw_col = jnp.transpose(raw)[0 : FIELDS + 24, 0:1]
        CB[...] = jnp.broadcast_to(raw_col, (FIELDS + 24, LANES))

        def combine(i, carry):
            for k in range(8):
                rho = 8 * i + k + GHOST
                value = CB[pl.ds(0, K), :] * X[0][line(rho), :]
                for m in range(1, ORDERS):
                    value = value + CB[pl.ds(m * K, K), :] * X[m][line(rho), :]
                value = jnp.sum(value, axis=0, keepdims=True)
                if s:
                    at = pl.multiple_of(24 * (8 * i + k), 8)
                    older = CB[pl.ds(FIELDS, 16), :] * UV[pl.ds(at, 16), :]
                    value = value + jnp.sum(older, axis=0, keepdims=True)
                U0[s, pl.ds(8 * i + k, 1), :] = value
            return carry

        lax.fori_loop(0, ROWS // 8, combine, 0)

        lane_t = iota((8, LANES), 1)
        sub_t = iota((8, LANES), 0)
        packed = jnp.zeros((8, LANES), F32)
        for q in range(6):
            tile = U0[s, pl.ds(8 * q, 8), :]
            packed = jnp.where(
                (lane_t >= 4 * q) & (lane_t < 4 * q + 4), pltpu.roll(tile, 4 * q, 1) if q else tile, packed
            )
            packed = jnp.where(
                (lane_t >= 64 + 4 * q) & (lane_t < 68 + 4 * q), pltpu.roll(tile, 68 + 4 * q, 1), packed
            )
        PK[s, :, :] = packed
        edge = [
            send(U0.at[s, pl.ds(0, 8)], HB.at[s], usend.at[s, 0], urecv.at[s, 0], near(sizes, -1, 0)),
            send(U0.at[s, pl.ds(40, 8)], HT.at[s], usend.at[s, 1], urecv.at[s, 1], near(sizes, 1, 0)),
            send(PK.at[s], KRB.at[s, 1], usend.at[s, 2], urecv.at[s, 2], near(sizes, 0, -1)),
            send(PK.at[s], KLB.at[s, 1], usend.at[s, 3], urecv.at[s, 3], near(sizes, 0, 1)),
            send(PK.at[s], KRB.at[s, 2], usend.at[s, 4], urecv.at[s, 4], near(sizes, -1, -1)),
            send(PK.at[s], KLB.at[s, 2], usend.at[s, 5], urecv.at[s, 5], near(sizes, -1, 1)),
            send(PK.at[s], KRB.at[s, 0], usend.at[s, 6], urecv.at[s, 6], near(sizes, 1, -1)),
            send(PK.at[s], KLB.at[s, 0], usend.at[s, 7], urecv.at[s, 7], near(sizes, 1, 1)),
        ]

        if s + 1 < STEPS:
            VW[pl.ds(0, ROWS, stride=8), :] = U0[s]
            d_old = with_old(paired())
        h_row = h_wide[0:1, :]
        e = jnp.where(lane_r < K, moved(-40), 0.5 * (moved(40) + moved(-40)))
        e = jnp.where(lane_r < 3 * K, e, pltpu.roll(h_row, 3 * K, 1))
        e = jnp.where(lane_r < 4 * K, e, 0.0)
        mt = MT[pl.ds(0, K), :]
        g1 = jnp.sum(mt * e, axis=1, keepdims=True)
        e1 = e - jnp.sum(mt * g1, axis=0, keepdims=True)
        g2 = jnp.sum(mt * e1, axis=1, keepdims=True)
        e2 = e1 - jnp.sum(mt * g2, axis=0, keepdims=True)
        e2_square = jnp.sum(e2 * e2, axis=1, keepdims=True)

        if s == 0:
            two.finish(0)
            two.start(1)
        if s == 1:
            two.finish(2)
            two.gather()
            late[0].start(1, late[0].finish(0))
        if s == 2:
            keep_late(0, late[0].finish(2))
            late[1].start(1, late[1].finish(0))
        for copy in edge:
            copy.wait_recv()

        mids = jnp.concatenate([HT[s], U0[s], HB[s]], axis=0) * CF[4]
        sides = []
        for j in range(8):
            part = 0 if j == 0 else (2 if j == 7 else 1)
            q = 5 if j == 0 else (0 if j == 7 else j - 1)
            rt = KRB[s, part]
            lf = pltpu.roll(KLB[s, part], 60 - 4 * q, 1)
            rt = pltpu.roll(rt, LANES - 4 * q, 1) if q else rt
            sides.append(jnp.where(lane_t < 4, rt, lf))
        sds = jnp.concatenate(sides, axis=0) * CF[9]

        def twice_s(c, v):
            cl, sl = pltpu.roll(c, 1, 1), pltpu.roll(v, 1, 1)
            cr, sr = pltpu.roll(c, 127, 1), pltpu.roll(v, 127, 1)
            cu = pltpu.roll(c, 1, 0) + pltpu.roll(c, 63, 0)
            su = pltpu.roll(v, 1, 0) + pltpu.roll(v, 63, 0)
            lo, hi = tile_mask == 0, tile_mask == 127
            mid = CF[0] * c - CF[1] * cu + CF[2] * jnp.where(hi, sr, cr) - CF[3] * jnp.where(lo, sl, cl)
            side = CF[5] * v - CF[6] * su + CF[7] * jnp.where(hi, cr, sr) - CF[8] * jnp.where(lo, cl, sl)
            return mid, side

        before = (mids, sds)
        now = twice_s(*before)
        now = (0.5 * now[0], 0.5 * now[1])
        orders = [before[0], now[0]]
        for m in range(2, ORDERS):
            nxt = twice_s(*now)
            before, now = now, (nxt[0] - before[0], nxt[1] - before[1])
            orders.append(now[0])
        for m in range(ORDERS):
            VB[m, :, :] = orders[m][8:56, :]
            VW[pl.ds(m, ROWS, stride=8), :] = orders[m][8:56, :]
            UV[pl.ds(8 * s + m, ROWS, stride=24), :] = orders[m][8:56, :]

        v = paired()
        if s + 1 < STEPS:
            total_sum = Sum([b.at[s] for b in slots_small], ssend.at[s], srecv.at[s])
            DN[...] = jnp.zeros((8, 256), F32)
            DN[:, pl.ds(0, K)] = with_first(v)
            DN[:, pl.ds(72, 24)] = with_new(v)
            low = pltpu.roll(DN[:, pl.ds(0, LANES)], 1, 0)
            wide_row = d_old[0:1, :]
            packed_new = jnp.where((lane_t >= 72) & (lane_t < 96), DN[0:1, pl.ds(0, LANES)], wide_row[:, LANES:])
            value = jnp.where(sub_t == 0, wide_row[:, 0:LANES], jnp.where(sub_t == 1, packed_new, low))
        else:
            total_sum = Sum(slots_last, ssend.at[s], srecv.at[s])
            DN[...] = with_old(v)
            DN[:, pl.ds(FIELDS, 24)] = with_new(v)
            value = DN[...]
        for stage in range(3):
            total_sum.start(stage, value)
            if stage == 0 and s + 1 < STEPS:
                rest = jnp.where((lane8 >= K) & (sub8 >= 1) & (sub8 < ORDERS), with_old(v), 0.0)
            if s == 0 and stage == 0:
                two.finish(1)
                two.start(2)
            if s == 0 and stage == 2:
                late[0].start(0, rest)
            if s == 1 and stage == 0:
                two.arrived()
                assemble_rest()
            if s == 1 and stage == 0:
                late[0].start(2, late[0].finish(1))
            if s == 1 and stage == 2:
                late[1].start(0, rest)
            if s == 2 and stage == 0:
                late[1].start(2, late[1].finish(1))
            value = total_sum.finish(stage)
        if s + 1 < STEPS:
            up = pltpu.roll(value, 7, 0)
            mid = (lane_t >= 72) & (lane_t < 96)
            left = jnp.where(sub_t == 0, value, jnp.where(lane_t < K, up, 0.0))
            right = jnp.where((sub_t == 0) | mid, up, 0.0)
            value = jnp.concatenate([left, right], axis=1)
        d = value * inverse_total
        d = jnp.where(sub8 < ORDERS, d, 0.0)

        nn = jnp.sum(jnp.where(lane_r == FIELDS + 8 * s, d[0:1, :], 0.0), axis=1, keepdims=True)
        beta = jnp.sqrt(nn + EPSILON)
        ib = 1.0 / beta
        eta = jnp.sqrt(e2_square + beta * beta + EPSILON)
        MT[pl.ds(column, 1), :] = (e2 + jnp.where(lane_r == 3 * K + r, beta, 0.0)) / eta
        sub_col = iota((K, 1), 0)
        g = g1 + g2 + jnp.where(sub_col == column, eta, 0.0)
        lane_h = iota((K, LANES), 1)
        HS[pl.ds(0, K), :] = jnp.where(lane_h == s, g, HS[pl.ds(0, K), :])
        newc_ref[s, :, :] = VB[0] * ib
        newi_ref[s, :, :] = VB[4] * ib
        for m in range(ORDERS):
            at = m * K + r
            LB[pl.ds(at, 1), :] = jnp.where(lane_r == FIELDS + 8 * s + m, ib, 0.0)
        GS[pl.ds(FIELDS + 8 * s, 8), :] = d
        if s + 1 < STEPS:
            db = dot3(d, LB[...], 1, 1) * ib
            dcol = jnp.transpose(db)[:, 0:1]
            lane_g = iota((256, LANES), 1)
            GB0[...] = jnp.where(lane_g == r, dcol, GB0[...])
            for m in range(ORDERS):
                GB0[pl.ds(m * K + r, 1), :] = jnp.where(lane1 < K, db[m : m + 1, 0:LANES], 0.0)

    keep_late(1, late[1].finish(2))
    mirrored = jnp.transpose(GS[...])
    def age(index):
        return sum(((index >= FIELDS + 8 * t).astype(jnp.int32) for t in range(1, STEPS)), (index >= FIELDS).astype(jnp.int32))

    whole_row = age(iota((256, 256), 0))
    whole_col = age(iota((256, 256), 1))
    GS[...] = jnp.where(whole_row >= whole_col, GS[...], mirrored)
    gram = dot3(dot3(LB[...], GS[...], 1, 0), LB[...], 1, 1)
    for a in range(ORDERS):
        for b in range(ORDERS):
            gram_ref[a, b, :, :] = gram[a * K : (a + 1) * K, b * K : (b + 1) * K]
    for j in range(4):
        coef_ref[:, j, :] = MT[pl.ds(0, KRYLOV + STEPS), pl.ds(j * K, K)]
    hess_ref[...] = jnp.transpose(HS[...])[0:STEPS, 0 : KRYLOV + STEPS]

    for copy in pending:
        copy.wait_send()


def handed_out(*refs):
    sources, targets, sems = refs[:5], refs[5:10], refs[10]
    copies = [pltpu.make_async_copy(a, b, sems.at[i]) for i, (a, b) in enumerate(zip(sources, targets))]
    for copy in copies:
        copy.start()
    for copy in copies:
        copy.wait()


def local(sizes, basis_raw, krylov_raw, stiffness, rotation):
    width = KRYLOV + STEPS
    nrow = sizes["x"] * sizes["core"]
    counts = []
    for axes in STAGES:
        n = 1
        for a in axes:
            n *= sizes[a]
        counts.append(n)
    big_copies = sum(n - 1 for n in counts) + counts[0] - 1
    small_copies = sum(n - 1 for n in counts)
    vmem = lambda *shape: pltpu.VMEM(shape, F32)
    half = lambda *shape: pltpu.VMEM(shape, jnp.bfloat16)
    dma = lambda *shape: pltpu.SemaphoreType.DMA(shape)
    scratch = [
        vmem(K * ROWS, LANES), dma(1),
        [vmem((ROWS + 8) * K, LANES) for _ in range(ORDERS)],
        [vmem((ROWS + 8) * K, LANES) for _ in range(ORDERS - 1)],
        vmem(10, 64, LANES), vmem(2, K, LANES), vmem(2, K, LANES), vmem(4, K, LANES), vmem(4, K, LANES),
        half(256 + PADDED, (ROWS + 8) * LANES), vmem(256 + PADDED, 256), vmem(96, 512),
        vmem(FIRST, LANES), vmem(FIRST, LANES), vmem(SECOND, LANES), vmem(SECOND, LANES),
        vmem(256, 256), vmem(256, LANES), vmem(256, 256),
        vmem(256, LANES), vmem(FIELDS + 24, LANES), vmem(LANES, 256), vmem(LANES, LANES),
        vmem(STEPS, ROWS, LANES), vmem(STEPS, 8, LANES), vmem(STEPS, 8, LANES), vmem(STEPS, 8, LANES),
        vmem(STEPS, 3, 8, LANES), vmem(STEPS, 3, 8, LANES), vmem(ORDERS, ROWS, LANES),
        vmem(ROWS * 8, LANES), vmem(ROWS * 24, LANES), vmem(8, 256),
        [vmem(n, FIRST // nrow, LANES) for n in counts],
        [vmem(n, SECOND // nrow, LANES) for n in counts],
        [vmem(STEPS - 1, n, 8, LANES) for n in counts],
        [vmem(n, 8, 256) for n in counts],
        [vmem(STEPS - 1, n, 8, 256) for n in counts],
        [vmem(n, K, LANES) for n in counts],
        dma(8), dma(8), dma(big_copies), dma(big_copies), dma(big_copies), dma(big_copies),
        dma(STEPS, 8), dma(STEPS, 8), dma(STEPS, small_copies), dma(STEPS, small_copies),
        dma(STEPS - 1, small_copies), dma(STEPS - 1, small_copies),
        dma(small_copies), dma(small_copies),
    ]
    shape = lambda *dims: jax.ShapeDtypeStruct(dims, F32)
    shapes = [
        shape(STEPS, ROWS, LANES), shape(width, 4, K), shape(STEPS, width),
        shape(ORDERS, ORDERS, K, K), shape(STEPS, ROWS, LANES),
    ]
    krylov_lines = jnp.transpose(krylov_raw, (2, 0, 1)).reshape(4 * KRYLOV, R)
    krylov_lines = jnp.pad(krylov_lines, ((0, 24), (0, LANES - R)))
    small = jnp.concatenate([stiffness, rotation, krylov_lines], axis=0)
    results = pl.pallas_call(
        functools.partial(kernel, sizes),
        out_shape=shapes,
        in_specs=[pl.BlockSpec(memory_space=pltpu.HBM), pl.BlockSpec(memory_space=pltpu.VMEM)],
        out_specs=[pl.BlockSpec(memory_space=pltpu.VMEM)] * 5,
        scratch_shapes=scratch,
        compiler_params=pltpu.CompilerParams(
            collective_id=0, has_side_effects=True, vmem_limit_bytes=55_000_000
        ),
    )(
        basis_raw.reshape(R * ROWS, LANES), small,
    )
    new_columns, coefficients, hessenberg, gram, new_images = pl.pallas_call(
        handed_out,
        out_shape=shapes,
        in_specs=[pl.BlockSpec(memory_space=pltpu.VMEM)] * 5,
        out_specs=[pl.BlockSpec(memory_space=pltpu.HBM)] * 5,
        scratch_shapes=[pltpu.SemaphoreType.DMA((5,))],
        compiler_params=pltpu.CompilerParams(vmem_limit_bytes=2 * 1024 * 1024),
    )(*results)
    return (
        new_columns, jnp.transpose(coefficients, (1, 2, 0)), hessenberg,
        jnp.transpose(gram, (0, 2, 1, 3)), new_images,
    )


def solution(mesh):
    cores = 2
    columns = mesh.devices.shape[1]
    depth = 8 if columns % 8 == 0 else 2
    sizes = {
        "x": mesh.devices.shape[0] // cores, "core": cores,
        "y": columns // depth, "z": depth,
    }
    split = Mesh(mesh.devices.reshape(*(sizes[a] for a in AXES)), AXES)
    return jax.shard_map(
        functools.partial(local, sizes),
        mesh=split,
        in_specs=(P(None, ROW, COL), P(), P(ROW, COL), P(ROW, COL)),
        out_specs=(P(None, ROW, COL), P(), P(), P(), P(None, ROW, COL)),
        check_vma=False,
    )
```
